256 devices in a mesh: row: 16 (over z, core), col: 16 (over x, y).
Axes of the slice: x: 4, y: 4, z: 8, core: 2. Of those that a mesh axis runs over, the one named last changes fastest.
Arguments:
- right_side: float32 [1, 16, 4, 1024], P(None, 'row'), may hold values from -6 to 6
- inverse_t: bfloat16 [1, 16, 1024, 1024], P(None, 'row', 'col'), as said below
- u_factor: bfloat16 [1, 16, 1, 16, 128, 1024], P(None, 'row', None, 'col'), may hold values from -0.25 to 0.25
- v_factor: bfloat16 [1, 16, 1, 16, 128, 1024], P(None, 'row', None, 'col'), may hold values from -0.1875 to 0.1875
- ranks: int32 [1, 16, 1, 16], P(None, 'row', None, 'col'), may hold values from 4 to 128, as said below
Outputs:
- whitened: float32 [1, 16, 4, 1024], P(None, 'row')
- loglik: float32 [1, 16, 4], P(None, 'row')
The draws below stay inside these ranges and needn't reach their ends.
Inputs may be any that keep to these rules, and one draw needn't show every extreme that they name: Tile (i, j) with j < i uses the first ranks of its factor rows. `inverse_t`: upper triangular with a positive diagonal.
All inputs are finite; a program needn't handle non-finite values.
Results may differ from the reference program's by a relative error of at most 0.0085.
Values sent between devices are 32-bit elements; how exact they have to be, the bound alone decides.
A program may use at most 64 MiB of HBM per device.

```python
import math
import jax
import jax.numpy as jnp

NB = 1024
RMAX = 128
NRHS = 4
CYC = 1
SLAB = 16
N_ROW = 16
N_COL = 16


def draw_inverse_t(key, part):
    key_diag, key_off = jax.random.split(jax.random.fold_in(key, 11))
    shape = (CYC, N_ROW, NB, NB)
    diagonal = jnp.exp(jax.random.uniform(key_diag, (CYC, N_ROW, NB), jnp.float32, math.log(0.3), math.log(1.2)))
    spread = jax.random.normal(key_off, shape, jnp.float32)
    upper = jnp.triu(spread * (0.3 / math.sqrt(NB)), 1)
    eye = jnp.eye(NB, dtype=jnp.float32)
    matrix = upper + eye[None, None, :, :] * diagonal[:, :, :, None]
    return matrix.astype(jnp.bfloat16)


def draw_ranks(key, part):
    slab = CYC * N_ROW
    tile_cols = slab // N_COL
    shape = (CYC, N_ROW, tile_cols, N_COL)
    row_ids = jnp.arange(CYC, dtype=jnp.int32)[:, None, None, None] * N_ROW + jnp.arange(N_ROW, dtype=jnp.int32)[None, :, None, None]
    col_ids = jnp.arange(tile_cols, dtype=jnp.int32)[None, None, :, None] * N_COL + jnp.arange(N_COL, dtype=jnp.int32)[None, None, None, :]
    distance = jnp.maximum(row_ids - col_ids, 1)
    lowest = max(RMAX // 32, 1)
    highest = jnp.maximum(RMAX // distance, lowest)
    raw = jax.random.randint(jax.random.fold_in(key, 23), shape, 0, 1 << 20)
    values = lowest + raw % (highest - lowest + 1)
    forced = (row_ids == 1) & (col_ids == 0)
    values = jnp.where(forced, RMAX, values)
    return values.astype(jnp.int32)


def levels(rng, extent, shards, least, top_value):
    def one(position, parts):
        heights = jax.random.uniform(jax.random.fold_in(jax.random.fold_in(rng, 6), position), (parts,), jnp.float32, least / len(shards), top_value / len(shards))
        return jnp.repeat(jnp.exp(heights), extent[position] // parts).reshape((-1,) + (1,) * (len(extent) - position - 1))

    level = one(*shards[0])
    for cut in shards[1:]:
        level = level * one(*cut)
    return level


def scatter_about(own_key, dims, scale, bound, cuts=(), kind=jnp.bfloat16):
    loudness = levels(own_key, dims, cuts, -0.22, 0.18) if cuts else 1.0
    drawn = jax.random.normal(own_key, dims, jnp.float32) * scale * loudness
    return jnp.minimum(jnp.maximum(drawn, -bound), bound).astype(kind)


def setup_inputs(seed: int = 0) -> dict:
    key_of = jax.random.split(jax.random.key(seed), 6)
    return {
        "right_side": scatter_about(key_of[0], (CYC, N_ROW, NRHS, NB), 1.0, 6.0, ((1, 16),), jnp.float32),
        "inverse_t": draw_inverse_t(jax.random.fold_in(key_of[5], 71), 0),
        "u_factor": scatter_about(key_of[2], (CYC, N_ROW, SLAB // N_COL, N_COL, RMAX, NB), (4 * RMAX) ** -0.5, 0.25, ((1, 16), (3, 16))),
        "v_factor": scatter_about(key_of[3], (CYC, N_ROW, SLAB // N_COL, N_COL, RMAX, NB), NB ** -0.5, 0.1875, ((1, 16), (3, 16))),
        "ranks": draw_ranks(jax.random.fold_in(key_of[5], 71), 0),
    }


def reference(right_side, inverse_t, u_factor, v_factor, ranks):
    slab = CYC * N_ROW
    sources = right_side.reshape(slab, NRHS, NB)
    inverse = inverse_t.reshape(slab, NB, NB)
    u_tiles = u_factor.reshape(slab, slab, RMAX, NB)
    v_tiles = v_factor.reshape(slab, slab, RMAX, NB)
    limits = ranks.reshape(slab, slab)
    rank_index = jnp.arange(RMAX, dtype=jnp.int32)
    tile_index = jnp.arange(slab, dtype=jnp.int32)
    solved = jnp.zeros((slab, NRHS, NB), jnp.float32)
    for row in range(slab):
        rounded = solved.astype(jnp.bfloat16).astype(jnp.float32)
        inner = jnp.einsum('jrn,jkn->jrk', v_tiles[row].astype(jnp.float32), rounded)
        keep = (rank_index[None, :] < limits[row][:, None]) & (tile_index < row)[:, None]
        inner = jnp.where(keep[:, :, None], inner, 0.0).astype(jnp.bfloat16)
        partial_value = jnp.einsum('jrk,jrn->kn', inner.astype(jnp.float32), u_tiles[row].astype(jnp.float32))
        reduced = (sources[row] - partial_value).astype(jnp.bfloat16)
        result = jnp.dot(reduced, inverse[row], preferred_element_type=jnp.float32)
        solved = solved.at[row].set(result)
    diagonal = jnp.diagonal(inverse, axis1=1, axis2=2).astype(jnp.float32)
    logdiag = jnp.mean(jnp.log(diagonal), axis=1)
    quadratic = jnp.mean(solved * solved, axis=2)
    loglik = -0.5 * quadratic + logdiag[:, None] - 0.5 * math.log(2.0 * math.pi)
    return solved.reshape(CYC, N_ROW, NRHS, NB), loglik.reshape(CYC, N_ROW, NRHS)
```

```python
import functools
import math

import jax
import jax.numpy as jnp
from jax import lax
from jax.experimental import pallas as pl
from jax.experimental.pallas import tpu as pltpu
from jax.sharding import PartitionSpec as P

MESH = pl.DeviceIdType.MESH
LANES = 128


def kernel(n, rs_ref, inv_ref, u_ref, v_ref, rank_ref, white_ref, lik_ref,
           block, whole, arrived, own_part, parts, result, final, logs, logs_in,
           block_send, block_recv, y_send, y_recv, part_send, part_recv,
           final_send, final_recv, logs_send, logs_recv):
    row = lax.axis_index("row")
    col = lax.axis_index("col")
    piece, width = inv_ref.shape
    rank_max = u_ref.shape[0]
    solver_col = lax.rem(row + n - 1, n)
    is_solver = col == solver_col
    below = col < row

    for tile in range(width // 256):
        whole[pl.ds(tile * 256 + LANES, LANES), pl.ds(tile * 256, LANES)] = jnp.zeros((LANES, LANES), jnp.float32)

    barrier = pltpu.get_barrier_semaphore()
    for step in range(1, n):
        @pl.when(is_solver)
        def _():
            pl.semaphore_signal(barrier, inc=1, device_id=(row, lax.rem(col + step, n)), device_id_type=MESH)
        @pl.when(is_solver & (row + step < n))
        def _():
            pl.semaphore_signal(barrier, inc=1, device_id=(row + step, row), device_id_type=MESH)
    @pl.when(jnp.logical_not(is_solver))
    def _():
        pl.semaphore_signal(barrier, inc=1, device_id=(row, solver_col), device_id_type=MESH)
    @pl.when(below)
    def _():
        source_col = lax.rem(col + n - 1, n)
        pl.semaphore_signal(barrier, inc=1, device_id=(col, source_col), device_id_type=MESH)
    partners = jnp.where(is_solver, 2 * (n - 1) - row, 1) + jnp.where(below, 1, 0)
    pl.semaphore_wait(barrier, partners)

    def block_copy(owner):
        first = owner * piece // LANES * LANES
        return pltpu.make_async_remote_copy(
            src_ref=block.at[:, pl.ds(first, width - first)],
            dst_ref=whole.at[pl.ds(owner * piece, piece), pl.ds(first, width - first)],
            send_sem=block_send,
            recv_sem=block_recv.at[owner],
            device_id=(row, solver_col),
            device_id_type=MESH,
        )

    block[...] = inv_ref[...].astype(jnp.float32)
    for owner in range(n):
        @pl.when((col == owner) & jnp.logical_not(is_solver))
        def _():
            block_copy(owner).start()

    def project(y):
        inner = lax.dot_general(
            y.astype(jnp.bfloat16), v_ref[...], (((1,), (1,)), ((), ())), preferred_element_type=jnp.float32
        )
        keep = lax.broadcasted_iota(jnp.int32, inner.shape, 1) < rank_ref[0, 0]
        inner = jnp.where(keep, inner, 0.0).astype(jnp.bfloat16)
        return jnp.dot(inner, u_ref[...], preferred_element_type=jnp.float32)

    def y_copy(target):
        return pltpu.make_async_remote_copy(
            src_ref=result, dst_ref=arrived, send_sem=y_send.at[target], recv_sem=y_recv,
            device_id=(target, row), device_id_type=MESH,
        )

    def part_copy():
        return pltpu.make_async_remote_copy(
            src_ref=own_part, dst_ref=parts.at[col], send_sem=part_send, recv_sem=part_recv.at[col],
            device_id=(row, solver_col), device_id_type=MESH,
        )

    def final_copy(step):
        return pltpu.make_async_remote_copy(
            src_ref=result, dst_ref=final, send_sem=final_send.at[step], recv_sem=final_recv,
            device_id=(row, lax.rem(col + step, n)), device_id_type=MESH,
        )

    def logs_copy(step):
        return pltpu.make_async_remote_copy(
            src_ref=logs, dst_ref=logs_in, send_sem=logs_send.at[step], recv_sem=logs_recv,
            device_id=(row, lax.rem(col + step, n)), device_id_type=MESH,
        )

    def finish(y, log_mean):
        quadratic = jnp.sum(y * y, axis=1, keepdims=True) * (1.0 / width)
        lik_ref[...] = -0.5 * quadratic + log_mean - 0.5 * math.log(2.0 * math.pi)
        white_ref[...] = y

    @pl.when(is_solver)
    def _():
        whole[pl.ds(pl.multiple_of(col * piece, piece), piece), :] = block[...]
        for owner in range(n):
            @pl.when(col != owner)
            def _():
                block_copy(owner).wait_recv()
        total = jnp.zeros((1, LANES), jnp.float32)
        on_diagonal = (lax.broadcasted_iota(jnp.int32, (LANES, LANES), 0)
                       == lax.broadcasted_iota(jnp.int32, (LANES, LANES), 1))
        for tile in range(width // LANES):
            square = whole[pl.ds(tile * LANES, LANES), pl.ds(tile * LANES, LANES)]
            diagonal = jnp.sum(jnp.where(on_diagonal, square, 0.0), axis=0, keepdims=True)
            total = total + jnp.log(diagonal)
        mean = jnp.sum(total, axis=1, keepdims=True) * (1.0 / width)
        logs[...] = jnp.broadcast_to(mean, logs.shape)
        for step in range(1, n):
            logs_copy(step).start()

        result[...] = rs_ref[...]
        for owner in range(n - 2):
            @pl.when(owner < row - 1)
            def _():
                pltpu.make_async_remote_copy(
                    src_ref=own_part, dst_ref=parts.at[owner], send_sem=part_send, recv_sem=part_recv.at[owner],
                    device_id=(row, solver_col), device_id_type=MESH,
                ).wait_recv()
                result[...] = result[...] - parts[owner]

        @pl.when(row > 0)
        def _():
            y_copy(0).wait_recv()
            result[...] = result[...] - project(arrived[...])

        reduced = result[...].astype(jnp.bfloat16).astype(jnp.float32)
        for right in range(width // 256):
            value = jnp.zeros((reduced.shape[0], 256), jnp.float32)
            for left in range(right + 1):
                value = value + jnp.dot(
                    reduced[:, left * 256:(left + 1) * 256],
                    whole[pl.ds(left * 256, 256), pl.ds(right * 256, 256)],
                    preferred_element_type=jnp.float32,
                )
            result[:, pl.ds(right * 256, 256)] = value
        for target in range(1, n):
            @pl.when(target > row)
            def _():
                y_copy(target).start()
        for step in range(1, n):
            final_copy(step).start()
        finish(result[...], mean)
        for target in range(1, n):
            @pl.when(target > row)
            def _():
                y_copy(target).wait_send()
        for step in range(1, n):
            final_copy(step).wait_send()
            logs_copy(step).wait_send()

    @pl.when(jnp.logical_not(is_solver))
    def _():
        @pl.when(below)
        def _():
            y_copy(0).wait_recv()
            own_part[...] = project(arrived[...])
            part_copy().start()
        for owner in range(n):
            @pl.when(col == owner)
            def _():
                block_copy(owner).wait_send()
        @pl.when(below)
        def _():
            part_copy().wait_send()
        logs_copy(1).wait_recv()
        final_copy(1).wait_recv()
        finish(final[...], logs_in[0:1, 0:1])


def local(n, right_side, inverse_t, u_factor, v_factor, ranks):
    nrhs, width = right_side.shape[2:]
    piece = inverse_t.shape[2]
    rank_max = u_factor.shape[4]
    f32 = jnp.float32
    vmem = pl.BlockSpec(memory_space=pltpu.VMEM)
    dma = pltpu.SemaphoreType.DMA
    white, lik = pl.pallas_call(
        functools.partial(kernel, n),
        out_shape=(jax.ShapeDtypeStruct((nrhs, width), f32), jax.ShapeDtypeStruct((nrhs, 1), f32)),
        in_specs=[vmem, vmem, vmem, vmem, pl.BlockSpec(memory_space=pltpu.SMEM)],
        out_specs=(vmem, vmem),
        scratch_shapes=[
            pltpu.VMEM((piece, width), f32),
            pltpu.VMEM((width, width), f32),
            pltpu.VMEM((nrhs, width), f32),
            pltpu.VMEM((nrhs, width), f32),
            pltpu.VMEM((n, nrhs, width), f32),
            pltpu.VMEM((nrhs, width), f32),
            pltpu.VMEM((nrhs, width), f32),
            pltpu.VMEM((8, LANES), f32),
            pltpu.VMEM((8, LANES), f32),
            dma, dma((n,)), dma((n,)), dma, dma, dma((n,)), dma((n,)), dma, dma((n,)), dma,
        ],
        compiler_params=pltpu.CompilerParams(collective_id=0, has_side_effects=True),
    )(
        right_side.reshape(nrhs, width),
        inverse_t.reshape(piece, width),
        u_factor.reshape(rank_max, width),
        v_factor.reshape(rank_max, width),
        ranks.reshape(1, 1),
    )
    return white.reshape(1, 1, nrhs, width), lik.reshape(1, 1, nrhs)


def solution(mesh):
    return jax.shard_map(
        functools.partial(local, mesh.shape["row"]),
        mesh=mesh,
        in_specs=(
            P(None, "row", None, None),
            P(None, "row", "col", None),
            P(None, "row", None, "col", None, None),
            P(None, "row", None, "col", None, None),
            P(None, "row", None, "col"),
        ),
        out_specs=(P(None, "row", None, None), P(None, "row", None)),
        check_vma=False,
    )
```

```python
import functools
import math

import jax
import jax.numpy as jnp
from jax import lax
from jax.experimental import pallas as pl
from jax.experimental.pallas import tpu as pltpu
from jax.sharding import PartitionSpec as P

MESH = pl.DeviceIdType.MESH
LANES = 128
TILE = 256


def solver_of(row, n):
    return jnp.maximum(row - 1, 0)


def kernel(n, rs_ref, inv_ref, u_ref, v_ref, rank_ref, white_ref, lik_ref,
           block, whole, whole16, folded, padded, arrived, own_part, parts, result, final, logs, logs_parts, logs_in,
           block_send, block_recv, y_send, y_recv, part_send, part_recv,
           final_send, final_recv, log_send, log_recv, logs_send, logs_recv):
    row = lax.axis_index("row")
    col = lax.axis_index("col")
    piece, width = inv_ref.shape
    f32, bf16 = jnp.float32, jnp.bfloat16
    solver_col = solver_of(row, n)
    is_solver = col == solver_col
    first_row = row == 0
    below = col < row

    barrier = pltpu.get_barrier_semaphore()
    for step in range(1, n):
        @pl.when(is_solver)
        def _():
            pl.semaphore_signal(barrier, inc=1, device_id=(row, lax.rem(col + step, n)), device_id_type=MESH)
        @pl.when(is_solver & (row + step < n))
        def _():
            pl.semaphore_signal(barrier, inc=1, device_id=(row + step, row), device_id_type=MESH)
    @pl.when(jnp.logical_not(is_solver))
    def _():
        pl.semaphore_signal(barrier, inc=1, device_id=(row, solver_col), device_id_type=MESH)
    @pl.when(below)
    def _():
        pl.semaphore_signal(barrier, inc=1, device_id=(col, solver_of(col, n)), device_id_type=MESH)

    block[...] = inv_ref[...].astype(f32)
    span = max(piece, LANES)
    base = pl.multiple_of(col * piece // span * span, span)
    offset = col * piece - base
    log_base = pl.multiple_of(col * piece // LANES * LANES, LANES)
    total = jnp.zeros((1, LANES), f32)
    for start in range(0, piece, LANES):
        height = min(LANES, piece - start)
        square = block[pl.ds(start, height), pl.ds(log_base + start, LANES)]
        rows_at = lax.broadcasted_iota(jnp.int32, square.shape, 0) + (col * piece - log_base)
        on_diagonal = rows_at == lax.broadcasted_iota(jnp.int32, square.shape, 1)
        total = total + jnp.sum(jnp.log(jnp.where(on_diagonal, square, 1.0)), axis=0, keepdims=True)
    own_log = jnp.sum(total, axis=1, keepdims=True) * (1.0 / width)
    logs[...] = jnp.broadcast_to(own_log, logs.shape)

    @pl.when(first_row)
    def _():
        padded[...] = jnp.zeros(padded.shape, bf16)
        padded[pl.ds(pl.multiple_of(offset, piece), piece), :] = inv_ref[...]
        own_part[...] = jnp.dot(rs_ref[:, pl.ds(base, span)].astype(bf16), padded[...], preferred_element_type=f32)

    @pl.when(is_solver)
    def _():
        for tile in range(width // TILE):
            whole16[pl.ds(tile * TILE + LANES, LANES), pl.ds(tile * TILE, LANES)] = jnp.zeros((LANES, LANES), bf16)

    partners = jnp.where(is_solver, 2 * (n - 1) - row, 1) + jnp.where(below, 1, 0)
    pl.semaphore_wait(barrier, partners)

    def block_first(owner):
        return owner * piece // LANES * LANES

    def block_copy(owner):
        first = block_first(owner)
        return pltpu.make_async_remote_copy(
            src_ref=block.at[:, pl.ds(first, width - first)],
            dst_ref=whole.at[pl.ds(owner * piece, piece), pl.ds(first, width - first)],
            send_sem=block_send,
            recv_sem=block_recv.at[owner],
            device_id=(row, solver_col),
            device_id_type=MESH,
        )

    def low_rank(y):
        inner = lax.dot_general(y.astype(bf16), v_ref[...], (((1,), (1,)), ((), ())), preferred_element_type=f32)
        keep = lax.broadcasted_iota(jnp.int32, inner.shape, 1) < rank_ref[0, 0]
        return jnp.where(keep, inner, 0.0).astype(bf16)

    def y_copy(target):
        return pltpu.make_async_remote_copy(
            src_ref=result, dst_ref=arrived, send_sem=y_send.at[target], recv_sem=y_recv,
            device_id=(target, row), device_id_type=MESH,
        )

    def part_copy(slot):
        return pltpu.make_async_remote_copy(
            src_ref=own_part, dst_ref=parts.at[slot], send_sem=part_send, recv_sem=part_recv.at[slot],
            device_id=(row, solver_col), device_id_type=MESH,
        )

    def log_copy(slot):
        return pltpu.make_async_remote_copy(
            src_ref=logs, dst_ref=logs_parts.at[slot], send_sem=log_send, recv_sem=log_recv.at[slot],
            device_id=(row, solver_col), device_id_type=MESH,
        )

    def final_copy(step):
        return pltpu.make_async_remote_copy(
            src_ref=result, dst_ref=final, send_sem=final_send.at[step], recv_sem=final_recv,
            device_id=(row, lax.rem(col + step, n)), device_id_type=MESH,
        )

    def logs_copy(step):
        return pltpu.make_async_remote_copy(
            src_ref=logs, dst_ref=logs_in, send_sem=logs_send.at[step], recv_sem=logs_recv,
            device_id=(row, lax.rem(col + step, n)), device_id_type=MESH,
        )

    def finish(y, log_mean):
        quadratic = jnp.sum(y * y, axis=1, keepdims=True) * (1.0 / width)
        lik_ref[...] = -0.5 * quadratic + log_mean - 0.5 * math.log(2.0 * math.pi)
        white_ref[...] = y

    def share_logs():
        for owner in range(n):
            @pl.when(col != owner)
            def _():
                log_copy(owner).wait_recv()
                logs[...] = logs[...] + logs_parts[owner]
        for step in range(1, n):
            logs_copy(step).start()

    def upper(left, right):
        return whole16[pl.ds(left * TILE, TILE), pl.ds(right * TILE, TILE)]

    @pl.when(jnp.logical_not(is_solver))
    def _():
        @pl.when(first_row)
        def _():
            part_copy(col).start()
        for owner in range(n):
            @pl.when((col == owner) & jnp.logical_not(first_row))
            def _():
                block_copy(owner).start()
        log_copy(col).start()

    @pl.when(is_solver)
    def _():
        @pl.when(first_row)
        def _():
            y = own_part[...]
            for owner in range(1, n):
                part_copy(owner).wait_recv()
                y = y + parts[owner]
            result[...] = y

        @pl.when(jnp.logical_not(first_row))
        def _():
            for owner in range(n):
                first = block_first(owner)
                rows = pl.ds(owner * piece, piece)
                columns = pl.ds(first, width - first)
                @pl.when(col != owner)
                def _():
                    block_copy(owner).wait_recv()
                    whole16[rows, columns] = whole[rows, columns].astype(bf16)
                @pl.when(col == owner)
                def _():
                    whole16[rows, columns] = inv_ref[:, columns]
            for right in range(width // TILE):
                value = jnp.zeros((folded.shape[0], TILE), f32)
                for left in range(right + 1):
                    value = value + jnp.dot(
                        u_ref[:, pl.ds(left * TILE, TILE)], upper(left, right), preferred_element_type=f32
                    )
                folded[:, pl.ds(right * TILE, TILE)] = value.astype(bf16)
            share_logs()

            result[...] = rs_ref[...]
            for owner in range(n - 2):
                @pl.when(owner < row - 1)
                def _():
                    part_copy(owner).wait_recv()
                    result[...] = result[...] - parts[owner]
            reduced = result[...].astype(bf16)
            for right in range(width // TILE):
                value = jnp.zeros((reduced.shape[0], TILE), f32)
                for left in range(right + 1):
                    value = value + jnp.dot(
                        reduced[:, left * TILE:(left + 1) * TILE], upper(left, right), preferred_element_type=f32
                    )
                final[:, pl.ds(right * TILE, TILE)] = value

            y_copy(0).wait_recv()
            result[...] = final[...] - jnp.dot(low_rank(arrived[...]), folded[...], preferred_element_type=f32)

        for target in range(1, n):
            @pl.when(target > row)
            def _():
                y_copy(target).start()
        for step in range(1, n):
            final_copy(step).start()
        @pl.when(first_row)
        def _():
            share_logs()
        finish(result[...], logs[0:1, 0:1])
        for target in range(1, n):
            @pl.when(target > row)
            def _():
                y_copy(target).wait_send()
        for step in range(1, n):
            final_copy(step).wait_send()
            logs_copy(step).wait_send()

    @pl.when(jnp.logical_not(is_solver))
    def _():
        @pl.when(below)
        def _():
            y_copy(0).wait_recv()
            own_part[...] = jnp.dot(low_rank(arrived[...]), u_ref[...], preferred_element_type=f32)
            part_copy(col).start()
        for owner in range(n):
            @pl.when((col == owner) & jnp.logical_not(first_row))
            def _():
                block_copy(owner).wait_send()
        log_copy(col).wait_send()
        @pl.when(below | first_row)
        def _():
            part_copy(col).wait_send()
        logs_copy(1).wait_recv()
        final_copy(1).wait_recv()
        finish(final[...], logs_in[0:1, 0:1])


def local(n, right_side, inverse_t, u_factor, v_factor, ranks):
    nrhs, width = right_side.shape[2:]
    piece = inverse_t.shape[2]
    rank_max = u_factor.shape[4]
    f32, bf16 = jnp.float32, jnp.bfloat16
    vmem = pl.BlockSpec(memory_space=pltpu.VMEM)
    dma = pltpu.SemaphoreType.DMA
    rows = pltpu.VMEM((nrhs, width), f32)
    small = pltpu.VMEM((8, LANES), f32)
    white, lik = pl.pallas_call(
        functools.partial(kernel, n),
        out_shape=(jax.ShapeDtypeStruct((nrhs, width), f32), jax.ShapeDtypeStruct((nrhs, 1), f32)),
        in_specs=[vmem, vmem, vmem, vmem, pl.BlockSpec(memory_space=pltpu.SMEM)],
        out_specs=(vmem, vmem),
        scratch_shapes=[
            pltpu.VMEM((piece, width), f32),
            pltpu.VMEM((width, width), f32),
            pltpu.VMEM((width, width), bf16),
            pltpu.VMEM((rank_max, width), bf16),
            pltpu.VMEM((max(piece, LANES), width), bf16),
            rows,
            rows,
            pltpu.VMEM((n, nrhs, width), f32),
            rows,
            rows,
            small,
            pltpu.VMEM((n, 8, LANES), f32),
            small,
            dma, dma((n,)), dma((n,)), dma, dma, dma((n,)), dma((n,)), dma, dma, dma((n,)), dma((n,)), dma,
        ],
        compiler_params=pltpu.CompilerParams(collective_id=0, has_side_effects=True),
    )(
        right_side.reshape(nrhs, width),
        inverse_t.reshape(piece, width),
        u_factor.reshape(rank_max, width),
        v_factor.reshape(rank_max, width),
        ranks.reshape(1, 1),
    )
    return white.reshape(1, 1, nrhs, width), lik.reshape(1, 1, nrhs)


def solution(mesh):
    return jax.shard_map(
        functools.partial(local, mesh.shape["row"]),
        mesh=mesh,
        in_specs=(
            P(None, "row", None, None),
            P(None, "row", "col", None),
            P(None, "row", None, "col", None, None),
            P(None, "row", None, "col", None, None),
            P(None, "row", None, "col"),
        ),
        out_specs=(P(None, "row", None, None), P(None, "row", None)),
        check_vma=False,
    )
```

```python
import functools
import math

import jax
import jax.numpy as jnp
from jax import lax
from jax.experimental import pallas as pl
from jax.experimental.pallas import tpu as pltpu
from jax.sharding import PartitionSpec as P

MESH = pl.DeviceIdType.MESH
LANES = 128
TILE = 256
SECOND = 3


def solver_of(row):
    even = lax.rem(row, 2) == 0
    return jnp.where(even & (row > 0), row + 1, row), jnp.maximum(row - 1, 0)


def kernel(n, rs_ref, inv_ref, u_ref, v_ref, rank_ref, white_ref, lik_ref,
           block, whole, whole16, u32, v32, u16, u_near, v_near, v_pair, u_second, rs_near, folded, padded,
           arrived, own_part, parts, own_inner, inner_second, solved, result, final,
           logs, logs_parts, logs_all, logs_in,
           block_send, block_recv, tile_send, tile_recv, inner_send, inner_recv, y_send, y_recv, part_send, part_recv,
           final_send, final_recv, log_send, log_recv, logs_send, logs_recv):
    row = lax.axis_index("row")
    col = lax.axis_index("col")
    piece, width = inv_ref.shape
    rank_max = u_ref.shape[0]
    f32, bf16 = jnp.float32, jnp.bfloat16

    odd = lax.rem(row, 2) == 1
    for_odd = odd & (col == row - 1)
    for_even = odd & (col == row - 2)
    for_first = (row == 0) & (col == 0)
    is_solver = for_odd | for_even | for_first
    mine = jnp.where(for_even, row - 1, row)
    solver = solver_of(row)
    in_row = for_odd | for_first
    first_row = row == 0
    near = col == row - 1
    moved = near & jnp.logical_not(odd)
    second = (col == row - 2) & (row >= SECOND)
    takes_y = (col < row) & jnp.logical_not(moved)
    sends_part = (col < row - 2) | ((col == row - 2) & (row < SECOND))
    is_worker = takes_y & jnp.logical_not(is_solver)

    def feeds(source, target):
        return (target > source) & (target < n) & jnp.logical_not((target == source + 1) & (lax.rem(target, 2) == 0))

    barrier = pltpu.get_barrier_semaphore()
    fed = 0
    for step in range(n):
        in_my_row = is_solver & jnp.logical_not(in_row & (col == step))
        @pl.when(in_my_row)
        def _():
            pl.semaphore_signal(barrier, inc=1, device_id=(mine, step), device_id_type=MESH)
        feeding = is_solver & feeds(mine, step)
        @pl.when(feeding)
        def _():
            pl.semaphore_signal(barrier, inc=1, device_id=(step, mine), device_id_type=MESH)
        fed = fed + in_my_row.astype(jnp.int32) + feeding.astype(jnp.int32)
    @pl.when(jnp.logical_not(in_row))
    def _():
        pl.semaphore_signal(barrier, inc=1, device_id=solver, device_id_type=MESH)
    @pl.when(takes_y)
    def _():
        pl.semaphore_signal(barrier, inc=1, device_id=solver_of(col), device_id_type=MESH)

    block[...] = inv_ref[...].astype(f32)
    keep = lax.broadcasted_iota(jnp.int32, u_ref.shape, 0) < rank_ref[0, 0]
    u32[...] = jnp.where(keep, u_ref[...].astype(f32), 0.0)
    u16[...] = u32[...].astype(bf16)
    @pl.when(moved)
    def _():
        v32[...] = v_ref[...].astype(f32)

    span = max(piece, LANES)
    base = pl.multiple_of(col * piece // span * span, span)
    offset = col * piece - base
    @pl.when(first_row)
    def _():
        padded[...] = jnp.zeros(padded.shape, bf16)
        padded[pl.ds(pl.multiple_of(offset, piece), piece), :] = inv_ref[...]
        own_part[...] = jnp.dot(rs_ref[:, pl.ds(base, span)].astype(bf16), padded[...], preferred_element_type=f32)

    log_base = pl.multiple_of(col * piece // LANES * LANES, LANES)
    total = jnp.zeros((1, LANES), f32)
    for start in range(0, piece, LANES):
        height = min(LANES, piece - start)
        square = block[pl.ds(start, height), pl.ds(log_base + start, LANES)]
        rows_at = lax.broadcasted_iota(jnp.int32, square.shape, 0) + (col * piece - log_base)
        on_diagonal = rows_at == lax.broadcasted_iota(jnp.int32, square.shape, 1)
        total = total + jnp.sum(jnp.log(jnp.where(on_diagonal, square, 1.0)), axis=0, keepdims=True)
    own_log = jnp.sum(total, axis=1, keepdims=True) * (1.0 / width)
    logs[...] = jnp.broadcast_to(own_log, logs.shape)

    @pl.when(is_solver)
    def _():
        for tile in range(width // TILE):
            whole16[pl.ds(tile * TILE + LANES, LANES), pl.ds(tile * TILE, LANES)] = jnp.zeros((LANES, LANES), bf16)

    waits = fed + jnp.where(in_row, 0, 1) + jnp.where(takes_y, 1, 0)
    pl.semaphore_wait(barrier, waits)

    def block_first(owner):
        return owner * piece // LANES * LANES

    def remote(source, target, send, recv, device):
        return pltpu.make_async_remote_copy(
            src_ref=source, dst_ref=target, send_sem=send, recv_sem=recv, device_id=device, device_id_type=MESH
        )

    def block_copy(owner):
        first = block_first(owner)
        return remote(
            block.at[:, pl.ds(first, width - first)],
            whole.at[pl.ds(owner * piece, piece), pl.ds(first, width - first)],
            block_send, block_recv.at[owner], solver,
        )

    def u_copy():
        return remote(u32, u_near, tile_send.at[0], tile_recv.at[0], solver)

    def v_copy():
        return remote(v32, v_near, tile_send.at[1], tile_recv.at[1], solver)

    def rs_copy():
        return remote(rs_ref, rs_near, tile_send.at[2], tile_recv.at[2], solver)

    def second_copy():
        return remote(u32, u_second, tile_send.at[3], tile_recv.at[3], solver)

    def inner_copy():
        return remote(own_inner, inner_second, inner_send, inner_recv, solver)

    def y_copy(target):
        return remote(result, arrived, y_send.at[target], y_recv, (target, mine))

    def part_copy(slot):
        return remote(own_part, parts.at[slot], part_send, part_recv.at[slot], solver)

    def log_copy(slot):
        return remote(logs, logs_parts.at[slot], log_send, log_recv.at[slot], solver)

    def final_copy(target):
        return remote(result, final, final_send.at[target], final_recv, (mine, target))

    def logs_copy(target):
        return remote(logs_all, logs_in, logs_send.at[target], logs_recv, (mine, target))

    def inner_of(y, v):
        return lax.dot_general(y.astype(bf16), v, (((1,), (1,)), ((), ())), preferred_element_type=f32)

    def finish(y, log_mean):
        quadratic = jnp.sum(y * y, axis=1, keepdims=True) * (1.0 / width)
        lik_ref[...] = -0.5 * quadratic + log_mean - 0.5 * math.log(2.0 * math.pi)
        white_ref[...] = y

    def others():
        for target in range(n):
            yield target, jnp.logical_not(in_row & (col == target))

    def share_logs():
        logs_all[...] = jnp.where(in_row, logs[...], 0.0)
        for owner, other in others():
            @pl.when(other)
            def _():
                log_copy(owner).wait_recv()
                logs_all[...] = logs_all[...] + logs_parts[owner]
        for target, other in others():
            @pl.when(other)
            def _():
                logs_copy(target).start()

    def upper(left, right):
        return whole16[pl.ds(left * TILE, TILE), pl.ds(right * TILE, TILE)]

    def times_upper(lhs, right):
        value = jnp.zeros((lhs.shape[0], TILE), f32)
        for left in range(right + 1):
            value = value + jnp.dot(
                lhs[:, left * TILE:(left + 1) * TILE], upper(left, right), preferred_element_type=f32
            )
        return value

    @pl.when(first_row & jnp.logical_not(in_row))
    def _():
        part_copy(col).start()
    for owner in range(n):
        @pl.when((col == owner) & jnp.logical_not(first_row | in_row))
        def _():
            block_copy(owner).start()
    @pl.when(moved)
    def _():
        rs_copy().start()
        v_copy().start()
        u_copy().start()
    @pl.when(second)
    def _():
        second_copy().start()
    @pl.when(jnp.logical_not(in_row))
    def _():
        log_copy(col).start()

    @pl.when(is_solver)
    def _():
        @pl.when(for_first)
        def _():
            y = own_part[...]
            for owner in range(1, n):
                part_copy(owner).wait_recv()
                y = y + parts[owner]
            result[...] = y

        @pl.when(jnp.logical_not(for_first))
        def _():
            @pl.when(for_even)
            def _():
                rs_copy().wait_recv()
                v_copy().wait_recv()
                u_copy().wait_recv()
                u16[...] = u_near[...].astype(bf16)
                v_pair[pl.ds(0, rank_max), :] = v_near[...].astype(bf16)
                v_pair[pl.ds(rank_max, rank_max), :] = v_ref[...]
            @pl.when(for_odd)
            def _():
                rs_near[...] = rs_ref[...]
                v_pair[pl.ds(0, rank_max), :] = v_ref[...]
                v_pair[pl.ds(rank_max, rank_max), :] = v_ref[...]
            for owner in range(n):
                first = block_first(owner)
                rows = pl.ds(owner * piece, piece)
                columns = pl.ds(first, width - first)
                @pl.when(jnp.logical_not(in_row & (col == owner)))
                def _():
                    block_copy(owner).wait_recv()
                    whole16[rows, columns] = whole[rows, columns].astype(bf16)
                @pl.when(in_row & (col == owner))
                def _():
                    whole16[rows, columns] = inv_ref[:, columns]
            for right in range(width // TILE):
                folded[pl.ds(0, rank_max), pl.ds(right * TILE, TILE)] = times_upper(u16, right).astype(bf16)
            @pl.when(mine >= SECOND)
            def _():
                second_copy().wait_recv()
                u16[...] = u_second[...].astype(bf16)
                for right in range(width // TILE):
                    folded[pl.ds(rank_max, rank_max), pl.ds(right * TILE, TILE)] = times_upper(u16, right).astype(bf16)
            @pl.when(mine < SECOND)
            def _():
                folded[pl.ds(rank_max, rank_max), :] = jnp.zeros((rank_max, width), bf16)
            share_logs()

            result[...] = rs_near[...]
            for owner in range(n - 2):
                @pl.when((owner < mine - 2) | ((owner < mine - 1) & (mine < SECOND)))
                def _():
                    part_copy(owner).wait_recv()
                    result[...] = result[...] - parts[owner]
            reduced = result[...].astype(bf16)
            for right in range(width // TILE):
                solved[:, pl.ds(right * TILE, TILE)] = times_upper(reduced, right)

            y_copy(0).wait_recv()
            inner = inner_of(arrived[...], v_pair[...])
            @pl.when(for_even & second)
            def _():
                own_inner[...] = inner[:, rank_max:]
                inner_copy().start()
            @pl.when(for_even & sends_part)
            def _():
                own_part[...] = jnp.dot(inner[:, rank_max:].astype(bf16), u32[...].astype(bf16), preferred_element_type=f32)
                part_copy(col).start()
            @pl.when(mine >= SECOND)
            def _():
                inner_copy().wait_recv()
            @pl.when(mine < SECOND)
            def _():
                inner_second[...] = jnp.zeros(inner_second.shape, f32)
            result[...] = solved[...] - jnp.dot(
                jnp.concatenate([inner[:, :rank_max], inner_second[...]], axis=1).astype(bf16),
                folded[...], preferred_element_type=f32,
            )

        for target in range(1, n):
            @pl.when(feeds(mine, target))
            def _():
                y_copy(target).start()
        for target, other in others():
            @pl.when(other)
            def _():
                final_copy(target).start()
        @pl.when(for_first)
        def _():
            share_logs()

    @pl.when(is_worker)
    def _():
        y_copy(0).wait_recv()
        inner = inner_of(arrived[...], v_ref[...])
        @pl.when(second)
        def _():
            own_inner[...] = inner
            inner_copy().start()
        @pl.when(sends_part)
        def _():
            own_part[...] = jnp.dot(inner.astype(bf16), u16[...], preferred_element_type=f32)
            part_copy(col).start()

    @pl.when(in_row)
    def _():
        finish(result[...], logs_all[0:1, 0:1])
    @pl.when(jnp.logical_not(in_row))
    def _():
        logs_copy(0).wait_recv()
        final_copy(0).wait_recv()
        finish(final[...], logs_in[0:1, 0:1])

    for owner in range(n):
        @pl.when((col == owner) & jnp.logical_not(first_row | in_row))
        def _():
            block_copy(owner).wait_send()
    @pl.when(moved)
    def _():
        rs_copy().wait_send()
        v_copy().wait_send()
        u_copy().wait_send()
    @pl.when(second)
    def _():
        second_copy().wait_send()
        inner_copy().wait_send()
    @pl.when(jnp.logical_not(in_row))
    def _():
        log_copy(col).wait_send()
    @pl.when(sends_part | (first_row & jnp.logical_not(in_row)))
    def _():
        part_copy(col).wait_send()
    @pl.when(is_solver)
    def _():
        for target in range(1, n):
            @pl.when(feeds(mine, target))
            def _():
                y_copy(target).wait_send()
        for target, other in others():
            @pl.when(other)
            def _():
                final_copy(target).wait_send()
                logs_copy(target).wait_send()


def local(n, right_side, inverse_t, u_factor, v_factor, ranks):
    nrhs, width = right_side.shape[2:]
    piece = inverse_t.shape[2]
    rank_max = u_factor.shape[4]
    f32, bf16 = jnp.float32, jnp.bfloat16
    vmem = pl.BlockSpec(memory_space=pltpu.VMEM)
    dma = pltpu.SemaphoreType.DMA
    rows = pltpu.VMEM((nrhs, width), f32)
    small = pltpu.VMEM((8, LANES), f32)
    factor32 = pltpu.VMEM((rank_max, width), f32)
    factor16 = pltpu.VMEM((rank_max, width), bf16)
    inner = pltpu.VMEM((nrhs, rank_max), f32)
    white, lik = pl.pallas_call(
        functools.partial(kernel, n),
        out_shape=(jax.ShapeDtypeStruct((nrhs, width), f32), jax.ShapeDtypeStruct((nrhs, 1), f32)),
        in_specs=[vmem, vmem, vmem, vmem, pl.BlockSpec(memory_space=pltpu.SMEM)],
        out_specs=(vmem, vmem),
        scratch_shapes=[
            pltpu.VMEM((piece, width), f32),
            pltpu.VMEM((width, width), f32),
            pltpu.VMEM((width, width), bf16),
            factor32,
            factor32,
            factor16,
            factor32,
            factor32,
            pltpu.VMEM((2 * rank_max, width), bf16),
            factor32,
            rows,
            pltpu.VMEM((2 * rank_max, width), bf16),
            pltpu.VMEM((max(piece, LANES), width), bf16),
            rows,
            rows,
            pltpu.VMEM((n, nrhs, width), f32),
            inner,
            inner,
            rows,
            rows,
            rows,
            small,
            pltpu.VMEM((n, 8, LANES), f32),
            small,
            small,
            dma, dma((n,)), dma((4,)), dma((4,)), dma, dma, dma((n,)), dma, dma, dma((n,)),
            dma((n,)), dma, dma, dma((n,)), dma((n,)), dma,
        ],
        compiler_params=pltpu.CompilerParams(collective_id=0, has_side_effects=True),
    )(
        right_side.reshape(nrhs, width),
        inverse_t.reshape(piece, width),
        u_factor.reshape(rank_max, width),
        v_factor.reshape(rank_max, width),
        ranks.reshape(1, 1),
    )
    return white.reshape(1, 1, nrhs, width), lik.reshape(1, 1, nrhs)


def solution(mesh):
    return jax.shard_map(
        functools.partial(local, mesh.shape["row"]),
        mesh=mesh,
        in_specs=(
            P(None, "row", None, None),
            P(None, "row", "col", None),
            P(None, "row", None, "col", None, None),
            P(None, "row", None, "col", None, None),
            P(None, "row", None, "col"),
        ),
        out_specs=(P(None, "row", None, None), P(None, "row", None)),
        check_vma=False,
    )
```

```python
import functools
import math

import jax
import jax.numpy as jnp
from jax import lax
from jax.experimental import pallas as pl
from jax.experimental.pallas import tpu as pltpu
from jax.sharding import PartitionSpec as P

MESH = pl.DeviceIdType.MESH
LANES = 128
TILE = 256
SECOND = 4


def solver_of(row):
    even = lax.rem(row, 2) == 0
    return jnp.where(even & (row > 0), row + 1, row), jnp.maximum(row - 1, 0)


def kernel(n, rs_ref, inv_ref, u_ref, v_ref, rank_ref, white_ref, lik_ref,
           block, whole, whole16, u32, v32, u16, u_near, v_near, v_pair, u_second, rs_near, folded, padded,
           lhs, products, arrived, own_part, parts, own_inner, inner_second, solved, result, final,
           logs, logs_parts, logs_all, logs_in,
           block_send, block_recv, tile_send, tile_recv, inner_send, inner_recv, y_send, y_recv, part_send, part_recv,
           final_send, final_recv, log_send, log_recv, logs_send, logs_recv):
    row = lax.axis_index("row")
    col = lax.axis_index("col")
    piece, width = inv_ref.shape
    rank_max = u_ref.shape[0]
    nrhs = rs_ref.shape[0]
    f32, bf16 = jnp.float32, jnp.bfloat16

    odd = lax.rem(row, 2) == 1
    for_odd = odd & (col == row - 1)
    for_even = odd & (col == row - 2)
    for_first = (row == 0) & (col == 0)
    is_solver = for_odd | for_even | for_first
    mine = jnp.where(for_even, row - 1, row)
    solver = solver_of(row)
    in_row = for_odd | for_first
    first_row = row == 0
    near = col == row - 1
    moved = near & jnp.logical_not(odd)
    second = (col == row - 2) & (row >= SECOND)
    takes_y = (col < row) & jnp.logical_not(moved)
    sends_part = (col < row - 2) | ((col == row - 2) & (row < SECOND))
    is_worker = takes_y & jnp.logical_not(is_solver)

    def feeds(source, target):
        return (target > source) & (target < n) & jnp.logical_not((target == source + 1) & (lax.rem(target, 2) == 0))

    barrier = pltpu.get_barrier_semaphore()
    fed = 0
    for step in range(n):
        in_my_row = is_solver & jnp.logical_not(in_row & (col == step))
        @pl.when(in_my_row)
        def _():
            pl.semaphore_signal(barrier, inc=1, device_id=(mine, step), device_id_type=MESH)
        feeding = is_solver & feeds(mine, step)
        @pl.when(feeding)
        def _():
            pl.semaphore_signal(barrier, inc=1, device_id=(step, mine), device_id_type=MESH)
        fed = fed + in_my_row.astype(jnp.int32) + feeding.astype(jnp.int32)
    @pl.when(jnp.logical_not(in_row))
    def _():
        pl.semaphore_signal(barrier, inc=1, device_id=solver, device_id_type=MESH)
    @pl.when(takes_y)
    def _():
        pl.semaphore_signal(barrier, inc=1, device_id=solver_of(col), device_id_type=MESH)

    block[...] = inv_ref[...].astype(f32)
    keep = lax.broadcasted_iota(jnp.int32, u_ref.shape, 0) < rank_ref[0, 0]
    u32[...] = jnp.where(keep, u_ref[...].astype(f32), 0.0)
    u16[...] = u32[...].astype(bf16)
    @pl.when(moved)
    def _():
        v32[...] = v_ref[...].astype(f32)

    span = max(piece, LANES)
    base = pl.multiple_of(col * piece // span * span, span)
    offset = col * piece - base
    @pl.when(first_row)
    def _():
        padded[...] = jnp.zeros(padded.shape, bf16)
        padded[pl.ds(pl.multiple_of(offset, piece), piece), :] = inv_ref[...]
        own_part[...] = jnp.dot(rs_ref[:, pl.ds(base, span)].astype(bf16), padded[...], preferred_element_type=f32)

    log_base = pl.multiple_of(col * piece // LANES * LANES, LANES)
    total = jnp.zeros((1, LANES), f32)
    for start in range(0, piece, LANES):
        height = min(LANES, piece - start)
        square = block[pl.ds(start, height), pl.ds(log_base + start, LANES)]
        rows_at = lax.broadcasted_iota(jnp.int32, square.shape, 0) + (col * piece - log_base)
        on_diagonal = rows_at == lax.broadcasted_iota(jnp.int32, square.shape, 1)
        total = total + jnp.sum(jnp.log(jnp.where(on_diagonal, square, 1.0)), axis=0, keepdims=True)
    own_log = jnp.sum(total, axis=1, keepdims=True) * (1.0 / width)
    logs[...] = jnp.broadcast_to(own_log, logs.shape)

    @pl.when(is_solver)
    def _():
        for tile in range(width // TILE):
            whole16[pl.ds(tile * TILE + LANES, LANES), pl.ds(tile * TILE, LANES)] = jnp.zeros((LANES, LANES), bf16)

    waits = fed + jnp.where(in_row, 0, 1) + jnp.where(takes_y, 1, 0)
    pl.semaphore_wait(barrier, waits)

    def block_first(owner):
        return owner * piece // LANES * LANES

    def remote(source, target, send, recv, device):
        return pltpu.make_async_remote_copy(
            src_ref=source, dst_ref=target, send_sem=send, recv_sem=recv, device_id=device, device_id_type=MESH
        )

    def block_copy(owner):
        first = block_first(owner)
        return remote(
            block.at[:, pl.ds(first, width - first)],
            whole.at[pl.ds(owner * piece, piece), pl.ds(first, width - first)],
            block_send, block_recv.at[owner], solver,
        )

    def u_copy():
        return remote(u32, u_near, tile_send.at[0], tile_recv.at[0], solver)

    def v_copy():
        return remote(v32, v_near, tile_send.at[1], tile_recv.at[1], solver)

    def rs_copy():
        return remote(rs_ref, rs_near, tile_send.at[2], tile_recv.at[2], solver)

    def second_copy():
        return remote(u32, u_second, tile_send.at[3], tile_recv.at[3], solver)

    def inner_copy():
        return remote(own_inner, inner_second, inner_send, inner_recv, solver)

    def y_copy(step):
        return remote(result, arrived, y_send.at[step], y_recv, (mine + step, mine))

    def part_copy(slot):
        return remote(own_part, parts.at[slot], part_send, part_recv.at[slot], solver)

    def log_copy(slot):
        return remote(logs, logs_parts.at[slot], log_send, log_recv.at[slot], solver)

    def final_copy(target):
        return remote(result, final, final_send.at[target], final_recv, (mine, target))

    def logs_copy(target):
        return remote(logs_all, logs_in, logs_send.at[target], logs_recv, (mine, target))

    def inner_of(y, v):
        return lax.dot_general(y.astype(bf16), v, (((1,), (1,)), ((), ())), preferred_element_type=f32)

    def finish(y, log_mean):
        lik_ref[...] = log_mean
        white_ref[...] = y

    def update(inner, depth):
        result[...] = solved[...] - jnp.dot(inner, folded[pl.ds(0, depth), :], preferred_element_type=f32)

    def others():
        for target in range(n):
            yield target, jnp.logical_not(in_row & (col == target))

    def share_logs():
        logs_all[...] = jnp.where(in_row, logs[...], 0.0)
        for owner, other in others():
            @pl.when(other)
            def _():
                log_copy(owner).wait_recv()
                logs_all[...] = logs_all[...] + logs_parts[owner]
        for target, other in others():
            @pl.when(other)
            def _():
                logs_copy(target).start()

    def upper(left, right):
        return whole16[pl.ds(left * TILE, TILE), pl.ds(right * TILE, TILE)]

    def times_upper(lhs, right):
        value = jnp.zeros((lhs.shape[0], TILE), f32)
        for left in range(right + 1):
            value = value + jnp.dot(
                lhs[:, left * TILE:(left + 1) * TILE], upper(left, right), preferred_element_type=f32
            )
        return value

    @pl.when(first_row & jnp.logical_not(in_row))
    def _():
        part_copy(col).start()
    for owner in range(n):
        @pl.when((col == owner) & jnp.logical_not(first_row | in_row))
        def _():
            block_copy(owner).start()
    @pl.when(moved)
    def _():
        rs_copy().start()
        v_copy().start()
        u_copy().start()
    @pl.when(second)
    def _():
        second_copy().start()
    @pl.when(jnp.logical_not(in_row))
    def _():
        log_copy(col).start()

    @pl.when(is_solver)
    def _():
        @pl.when(for_first)
        def _():
            y = own_part[...]
            for owner in range(1, n):
                part_copy(owner).wait_recv()
                y = y + parts[owner]
            result[...] = y

        @pl.when(jnp.logical_not(for_first))
        def _():
            @pl.when(for_even)
            def _():
                rs_copy().wait_recv()
                v_copy().wait_recv()
                u_copy().wait_recv()
                u16[...] = u_near[...].astype(bf16)
                v_pair[:, pl.ds(0, rank_max)] = v_near[...].T.astype(bf16)
                v_pair[:, pl.ds(rank_max, rank_max)] = v_ref[...].astype(f32).T.astype(bf16)
            @pl.when(for_odd)
            def _():
                rs_near[...] = rs_ref[...]
                v_pair[:, pl.ds(0, rank_max)] = v_ref[...].astype(f32).T.astype(bf16)
            lhs[pl.ds(0, rank_max), :] = u16[...]
            lhs[pl.ds(rank_max, 16), :] = jnp.concatenate([rs_near[...]] * (16 // nrhs), axis=0).astype(bf16)
            for left in range(width // TILE):
                for owner in range(left * TILE // piece, (left + 1) * TILE // piece):
                    first = block_first(owner)
                    rows = pl.ds(owner * piece, piece)
                    columns = pl.ds(first, width - first)
                    @pl.when(jnp.logical_not(in_row & (col == owner)))
                    def _():
                        block_copy(owner).wait_recv()
                        whole16[rows, columns] = whole[rows, columns].astype(bf16)
                    @pl.when(in_row & (col == owner))
                    def _():
                        whole16[rows, columns] = inv_ref[:, columns]
                for right in range(left, width // TILE):
                    value = jnp.dot(lhs[:, pl.ds(left * TILE, TILE)], upper(left, right), preferred_element_type=f32)
                    columns = pl.ds(right * TILE, TILE)
                    if left:
                        value = value + products[:, columns]
                    products[:, columns] = value
            folded[pl.ds(0, rank_max), :] = products[pl.ds(0, rank_max), :].astype(bf16)
            @pl.when(mine >= SECOND)
            def _():
                second_copy().wait_recv()
                u16[...] = u_second[...].astype(bf16)
                for right in range(width // TILE):
                    folded[pl.ds(rank_max, rank_max), pl.ds(right * TILE, TILE)] = times_upper(u16, right).astype(bf16)

            @pl.when(mine == 1)
            def _():
                solved[...] = products[pl.ds(rank_max, nrhs), :]
            @pl.when(mine > 1)
            def _():
                share_logs()
                result[...] = rs_near[...]
                for owner in range(n - 2):
                    @pl.when((owner < mine - 2) | ((owner < mine - 1) & (mine < SECOND)))
                    def _():
                        part_copy(owner).wait_recv()
                        result[...] = result[...] - parts[owner]
                reduced = result[...].astype(bf16)
                for right in range(width // TILE):
                    solved[:, pl.ds(right * TILE, TILE)] = times_upper(reduced, right)

            two = mine >= SECOND
            @pl.when(for_odd & jnp.logical_not(two))
            def _():
                y_copy(0).wait_recv()
                inner = jnp.dot(arrived[...].astype(bf16), v_pair[:, pl.ds(0, rank_max)], preferred_element_type=f32)
                update(inner.astype(bf16), rank_max)
            @pl.when(for_even & jnp.logical_not(two))
            def _():
                y_copy(0).wait_recv()
                inner = jnp.dot(arrived[...].astype(bf16), v_pair[...], preferred_element_type=f32)
                own_inner[...] = inner[:, rank_max:]
                update(inner[:, :rank_max].astype(bf16), rank_max)
            @pl.when(for_odd & two)
            def _():
                y_copy(0).wait_recv()
                inner_copy().wait_recv()
                inner = jnp.dot(arrived[...].astype(bf16), v_pair[:, pl.ds(0, rank_max)], preferred_element_type=f32)
                update(jnp.concatenate([inner, inner_second[...]], axis=1).astype(bf16), 2 * rank_max)
            @pl.when(for_even & two)
            def _():
                y_copy(0).wait_recv()
                inner = jnp.dot(arrived[...].astype(bf16), v_pair[...], preferred_element_type=f32)
                own_inner[...] = inner[:, rank_max:]
                inner_copy().start()
                inner_copy().wait_recv()
                update(jnp.concatenate([inner[:, :rank_max], inner_second[...]], axis=1).astype(bf16), 2 * rank_max)

        for step in range(1, n):
            @pl.when(feeds(mine, mine + step))
            def _():
                y_copy(step).start()
        for target, other in others():
            @pl.when(other)
            def _():
                final_copy(target).start()
        @pl.when(for_even & sends_part)
        def _():
            own_part[...] = jnp.dot(own_inner[...].astype(bf16), u32[...].astype(bf16), preferred_element_type=f32)
            part_copy(col).start()
        @pl.when(mine <= 1)
        def _():
            share_logs()

    @pl.when(is_worker)
    def _():
        y_copy(0).wait_recv()
        inner = inner_of(arrived[...], v_ref[...])
        @pl.when(second)
        def _():
            own_inner[...] = inner
            inner_copy().start()
        @pl.when(sends_part)
        def _():
            own_part[...] = jnp.dot(inner.astype(bf16), u16[...], preferred_element_type=f32)
            part_copy(col).start()

    @pl.when(in_row)
    def _():
        finish(result[...], logs_all[...])
    @pl.when(jnp.logical_not(in_row))
    def _():
        logs_copy(0).wait_recv()
        final_copy(0).wait_recv()
        finish(final[...], logs_in[...])

    for owner in range(n):
        @pl.when((col == owner) & jnp.logical_not(first_row | in_row))
        def _():
            block_copy(owner).wait_send()
    @pl.when(moved)
    def _():
        rs_copy().wait_send()
        v_copy().wait_send()
        u_copy().wait_send()
    @pl.when(second)
    def _():
        second_copy().wait_send()
        inner_copy().wait_send()
    @pl.when(jnp.logical_not(in_row))
    def _():
        log_copy(col).wait_send()
    @pl.when(sends_part | (first_row & jnp.logical_not(in_row)))
    def _():
        part_copy(col).wait_send()
    @pl.when(is_solver)
    def _():
        for step in range(1, n):
            @pl.when(feeds(mine, mine + step))
            def _():
                y_copy(step).wait_send()
        for target, other in others():
            @pl.when(other)
            def _():
                final_copy(target).wait_send()
                logs_copy(target).wait_send()


def outputs(y_ref, log_ref, white_ref, lik_ref):
    y = y_ref[...]
    nrhs, width = y.shape
    lik = -0.5 * jnp.sum(y * y, axis=1, keepdims=True) * (1.0 / width) + log_ref[0:1, 0:1] - 0.5 * math.log(2.0 * math.pi)
    diagonal = lax.broadcasted_iota(jnp.int32, (nrhs, nrhs), 0) == lax.broadcasted_iota(jnp.int32, (nrhs, nrhs), 1)
    lik_ref[...] = jnp.sum(jnp.where(diagonal, lik, 0.0), axis=0, keepdims=True)
    white_ref[...] = y


def local(n, right_side, inverse_t, u_factor, v_factor, ranks):
    nrhs, width = right_side.shape[2:]
    piece = inverse_t.shape[2]
    rank_max = u_factor.shape[4]
    f32, bf16 = jnp.float32, jnp.bfloat16
    vmem = pl.BlockSpec(memory_space=pltpu.VMEM)
    dma = pltpu.SemaphoreType.DMA
    rows = pltpu.VMEM((nrhs, width), f32)
    small = pltpu.VMEM((8, LANES), f32)
    factor32 = pltpu.VMEM((rank_max, width), f32)
    factor16 = pltpu.VMEM((rank_max, width), bf16)
    inner = pltpu.VMEM((nrhs, rank_max), f32)
    y, log_mean = pl.pallas_call(
        functools.partial(kernel, n),
        out_shape=(jax.ShapeDtypeStruct((nrhs, width), f32), jax.ShapeDtypeStruct((8, LANES), f32)),
        in_specs=[vmem, vmem, vmem, vmem, pl.BlockSpec(memory_space=pltpu.SMEM)],
        out_specs=(vmem, vmem),
        scratch_shapes=[
            pltpu.VMEM((piece, width), f32),
            pltpu.VMEM((width, width), f32),
            pltpu.VMEM((width, width), bf16),
            factor32,
            factor32,
            factor16,
            factor32,
            factor32,
            pltpu.VMEM((width, 2 * rank_max), bf16),
            factor32,
            rows,
            pltpu.VMEM((2 * rank_max, width), bf16),
            pltpu.VMEM((max(piece, LANES), width), bf16),
            pltpu.VMEM((rank_max + 16, width), bf16),
            pltpu.VMEM((rank_max + 16, width), f32),
            rows,
            rows,
            pltpu.VMEM((n, nrhs, width), f32),
            inner,
            inner,
            rows,
            rows,
            rows,
            small,
            pltpu.VMEM((n, 8, LANES), f32),
            small,
            small,
            dma, dma((n,)), dma((4,)), dma((4,)), dma, dma, dma((n,)), dma, dma, dma((n,)),
            dma((n,)), dma, dma, dma((n,)), dma((n,)), dma,
        ],
        compiler_params=pltpu.CompilerParams(collective_id=0, has_side_effects=True),
    )(
        right_side.reshape(nrhs, width),
        inverse_t.reshape(piece, width),
        u_factor.reshape(rank_max, width),
        v_factor.reshape(rank_max, width),
        ranks.reshape(1, 1),
    )
    white, lik = pl.pallas_call(
        outputs,
        out_shape=(jax.ShapeDtypeStruct((nrhs, width), f32), jax.ShapeDtypeStruct((1, nrhs), f32)),
        in_specs=[vmem, vmem],
        out_specs=(vmem, vmem),
    )(y, log_mean)
    return white.reshape(1, 1, nrhs, width), lik.reshape(1, 1, nrhs)


def solution(mesh):
    return jax.shard_map(
        functools.partial(local, mesh.shape["row"]),
        mesh=mesh,
        in_specs=(
            P(None, "row", None, None),
            P(None, "row", "col", None),
            P(None, "row", None, "col", None, None),
            P(None, "row", None, "col", None, None),
            P(None, "row", None, "col"),
        ),
        out_specs=(P(None, "row", None, None), P(None, "row", None)),
        check_vma=False,
    )
```

```python
import functools
import math

import jax
import jax.numpy as jnp
from jax import lax
from jax.experimental import pallas as pl
from jax.experimental.pallas import tpu as pltpu
from jax.sharding import PartitionSpec as P

MESH = pl.DeviceIdType.MESH
LANES = 128
TILE = 256
SECOND = 4


def first_pair(n):
    return 10 if n == 16 else 2


def lean(base, n):
    return 2 - lax.rem(base // 2, 2) if n == 16 else LEAN


LEAN = 1


def solver_of(row, n):
    parity = lax.rem(row, 2)
    base = row - parity
    paired = row >= first_pair(n)
    return (jnp.where((parity == 0) & (row > 0), row + 1, row),
            jnp.where(paired, base - lean(base, n), jnp.maximum(row - 1, 0)))


def kernel(n, rs_ref, inv_ref, u_ref, v_ref, rank_ref, white_ref, lik_ref,
           block, whole, whole16, u32, v32, u16, u_near, v_near, v_pair, v_pair2, v_last, factors, sums, u_second, rs_near,
           tiles, relay, folded, folded2, padded, lhs, products,
           arrived, arrived2, own_part, low_part, parts, own_inner, inner_second, held, solved, result, final,
           logs, logs_parts, logs_all, logs_in,
           block_send, block_recv, tile_send, tile_recv, inner_send, inner_recv, y_send, y_recv, extra_send, extra_recv,
           part_send, part_recv, final_send, final_recv, log_send, log_recv, logs_send, logs_recv,
           relay_send, relay_recv, tiles_send, tiles_recv):
    row = lax.axis_index("row")
    col = lax.axis_index("col")
    piece, width = inv_ref.shape
    rank_max = u_ref.shape[0]
    nrhs = rs_ref.shape[0]
    f32, bf16 = jnp.float32, jnp.bfloat16
    start_pairs = first_pair(n)
    shift = 4 if n == 16 else LEAN + 1

    parity = lax.rem(row, 2)
    odd = parity == 1
    paired = row >= start_pairs
    single = jnp.logical_not(paired)
    pair_row = row - parity
    own_col = pair_row - lean(pair_row, n)
    other_col = pair_row - 3 + lean(pair_row, n)
    pair = odd & (col == own_col) & paired
    for_odd = odd & (col == row - 1) & single
    for_even = odd & (col == row - 2) & single
    for_first = (row == 0) & (col == 0)
    is_single = for_odd | for_even | for_first
    is_solver = is_single | pair
    mine = jnp.where(for_even | pair, row - 1, row)
    kind = lax.rem(mine, 2)
    served = ((0, mine, is_solver), (1, row, pair))
    solver = solver_of(row, n)
    in_row = for_odd | for_first | pair
    first_row = row == 0
    near = col == row - 1
    moved = jnp.where(paired, col == own_col, near) & jnp.logical_not(odd)
    second = (col == row - 2) & (row >= SECOND) & single
    by_x = paired & odd & near
    by_up = paired & jnp.logical_not(odd) & (col == other_col)
    by_down = paired & odd & (col == other_col)
    by_relay = by_x | by_up | by_down
    far = paired & (col <= pair_row - 3)
    lent = far & jnp.logical_not(odd)
    double = far & odd
    takes_y = jnp.where(paired, double | pair, (col < row) & jnp.logical_not(moved))
    sends_part = single & ((col < row - 2) | ((col == row - 2) & (row < SECOND)))
    is_worker = takes_y & single & jnp.logical_not(is_solver)
    relay_row = jnp.where(by_x, row, jnp.where(by_up, lax.rem(row + 2, n), row - 2))
    relay_col = jnp.where(by_x, lax.rem(own_col + shift, n), own_col)
    up_row = lax.rem(row + n - 2, n)
    x_relay = paired & odd & (col == lax.rem(own_col + shift, n))
    up_relay = jnp.logical_not(odd) & (up_row >= start_pairs) & (col == up_row - lean(up_row, n))
    down_relay = odd & (row + 2 > start_pairs) & (row + 2 < n) & (col == row + 1 - lean(row + 1, n))
    is_relay = x_relay | up_relay | down_relay
    from_row = jnp.where(x_relay, row, jnp.where(up_relay, up_row, row + 2))
    from_col = jnp.where(
        x_relay, row - 1, jnp.where(up_relay, up_row - 3 + lean(up_row, n), row - 2 + lean(row + 1, n))
    )
    onto_slot = jnp.where(x_relay, 0, jnp.where(up_relay, 1, 2))

    def feeds(source, target):
        base = target - lax.rem(target, 2)
        early = jnp.logical_not((target == source + 1) & (lax.rem(target, 2) == 0))
        late = ((source <= base - 3) | (source == base - lean(base, n))) & (lax.rem(target, 2) == 1)
        return (target > source) & (target < n) & jnp.where(target >= start_pairs, late, early)

    def next_base(source):
        return source + 2 - lax.rem(source, 2)

    def feeds_extra(source):
        base = next_base(source)
        return (base >= start_pairs) & (base < n) & (source != base - lean(base, n))

    def extra_target(source):
        base = next_base(source)
        return base + 1, base - lean(base, n)

    barrier = pltpu.get_barrier_semaphore()

    def greet(condition, device):
        @pl.when(condition)
        def _():
            pl.semaphore_signal(barrier, inc=1, device_id=device, device_id_type=MESH)
        return condition.astype(jnp.int32)

    waits = 0
    for slot, source, active in served:
        @pl.when(active)
        def _():
            for step in range(n):
                greet(jnp.logical_not((source == row) & (col == step)), (source, step))
            for step in range(1, n):
                greet(feeds(source, source + step), (source + step, source))
            greet(feeds_extra(source), extra_target(source))
        met = n - (source == row).astype(jnp.int32) + feeds_extra(source).astype(jnp.int32)
        for step in range(1, n):
            met = met + feeds(source, source + step).astype(jnp.int32)
        waits = waits + jnp.where(active, met, 0)
    waits = waits + greet(jnp.logical_not(in_row), solver)
    waits = waits + greet(takes_y, solver_of(col, n))
    @pl.when(paired)
    def _():
        greet(pair, solver_of(other_col, n))
        greet(by_relay, (relay_row, relay_col))
        greet(lent, (row + 1, col))
        greet(double, (row - 1, col))
        greet(pair, (row, lax.rem(own_col + shift, n)))
        greet(pair, (lax.rem(row + 1, n), col))
        greet(pair, (row - 2, col))
    @pl.when(is_relay)
    def _():
        greet(is_relay, (from_row, from_col))
        greet(is_relay, solver_of(from_row, n))
    for count, condition in ((4, pair), (1, by_relay), (1, lent), (1, double), (2, is_relay)):
        waits = waits + jnp.where(condition, count, 0)

    block[...] = inv_ref[...].astype(f32)
    keep = lax.broadcasted_iota(jnp.int32, u_ref.shape, 0) < rank_ref[0, 0]
    u32[...] = jnp.where(keep, u_ref[...].astype(f32), 0.0)
    u16[...] = u32[...].astype(bf16)
    @pl.when(moved | by_relay | lent)
    def _():
        v32[...] = v_ref[...].astype(f32)

    span = max(piece, LANES)
    base = pl.multiple_of(col * piece // span * span, span)
    offset = col * piece - base
    @pl.when(first_row)
    def _():
        padded[...] = jnp.zeros(padded.shape, bf16)
        padded[pl.ds(pl.multiple_of(offset, piece), piece), :] = inv_ref[...]
        own_part[...] = jnp.dot(rs_ref[:, pl.ds(base, span)].astype(bf16), padded[...], preferred_element_type=f32)

    log_base = pl.multiple_of(col * piece // LANES * LANES, LANES)
    total = jnp.zeros((1, LANES), f32)
    for start in range(0, piece, LANES):
        height = min(LANES, piece - start)
        square = block[pl.ds(start, height), pl.ds(log_base + start, LANES)]
        rows_at = lax.broadcasted_iota(jnp.int32, square.shape, 0) + (col * piece - log_base)
        on_diagonal = rows_at == lax.broadcasted_iota(jnp.int32, square.shape, 1)
        total = total + jnp.sum(jnp.log(jnp.where(on_diagonal, square, 1.0)), axis=0, keepdims=True)
    own_log = jnp.sum(total, axis=1, keepdims=True) * (1.0 / width)
    logs[...] = jnp.broadcast_to(own_log, logs.shape)

    @pl.when(is_solver)
    def _():
        for half in range(2):
            for tile in range(width // TILE):
                whole16[half, pl.ds(tile * TILE + LANES, LANES), pl.ds(tile * TILE, LANES)] = jnp.zeros(
                    (LANES, LANES), bf16
                )

    pl.semaphore_wait(barrier, waits)

    def block_first(owner):
        return owner * piece // LANES * LANES

    def remote(source, target, send, recv, device):
        return pltpu.make_async_remote_copy(
            src_ref=source, dst_ref=target, send_sem=send, recv_sem=recv, device_id=device, device_id_type=MESH
        )

    def block_copy(owner, half):
        first = block_first(owner)
        return remote(
            block.at[:, pl.ds(first, width - first)],
            whole.at[half, pl.ds(owner * piece, piece), pl.ds(first, width - first)],
            block_send, block_recv.at[half, owner], solver,
        )

    tile_device = (jnp.where(lent, row + 1, solver[0]), jnp.where(lent, col, solver[1]))

    def u_copy():
        return remote(u32, u_near, tile_send.at[0], tile_recv.at[0], tile_device)

    def v_copy():
        return remote(v32, v_near, tile_send.at[1], tile_recv.at[1], tile_device)

    def rs_copy():
        return remote(rs_ref, rs_near, tile_send.at[2], tile_recv.at[2], solver)

    def second_copy():
        return remote(u32, u_second, tile_send.at[3], tile_recv.at[3], solver)

    def relay_copy(which):
        return remote(
            (u32, v32)[which], relay.at[which], relay_send.at[which], relay_recv.at[which], (relay_row, relay_col)
        )

    def onward_copy(which, slot):
        return remote(
            relay.at[which], tiles.at[slot, which], tiles_send.at[which], tiles_recv.at[slot, which],
            solver_of(from_row, n),
        )

    def inner_copy():
        return remote(own_inner, inner_second, inner_send, inner_recv, solver)

    def y_copy(slot, source, step):
        return remote(result.at[slot], arrived, y_send.at[slot, step], y_recv, (source + step, source))

    def extra_copy(slot, source):
        return remote(result.at[slot], arrived2, extra_send.at[slot], extra_recv, extra_target(source))

    def part_copy(owner, half):
        return remote(own_part, parts.at[half, owner], part_send.at[0], part_recv.at[half, owner], solver)

    def low_part_copy(owner):
        return remote(low_part, parts.at[0, owner], part_send.at[1], part_recv.at[0, owner], solver)

    def log_copy(owner, half):
        return remote(logs, logs_parts.at[half, owner], log_send, log_recv.at[half, owner], solver)

    def final_copy(slot, source, target):
        return remote(result.at[slot], final, final_send.at[slot, target], final_recv, (source, target))

    def logs_copy(slot, source, target):
        return remote(logs_all.at[slot], logs_in, logs_send.at[slot, target], logs_recv, (source, target))

    def inner_of(y, v):
        return lax.dot_general(y.astype(bf16), v, (((1,), (1,)), ((), ())), preferred_element_type=f32)

    def finish(y, log_mean):
        lik_ref[...] = log_mean
        white_ref[...] = y

    def update(inner, depth):
        result[0] = solved[0] - jnp.dot(inner, folded[pl.ds(0, depth), :], preferred_element_type=f32)

    def others(source):
        for target in range(n):
            yield target, jnp.logical_not((source == row) & (col == target))

    def share_logs(slot, source, half):
        logs_all[slot] = jnp.where(source == row, logs[...], 0.0)
        for owner, other in others(source):
            @pl.when(other)
            def _():
                log_copy(owner, half).wait_recv()
                logs_all[slot] = logs_all[slot] + logs_parts[half, owner]
        for target, other in others(source):
            @pl.when(other)
            def _():
                logs_copy(slot, source, target).start()

    def upper(half, left, right):
        return whole16[half, pl.ds(left * TILE, TILE), pl.ds(right * TILE, TILE)]

    def times_upper(lhs, half, right):
        value = jnp.zeros((lhs.shape[0], TILE), f32)
        for left in range(right + 1):
            value = value + jnp.dot(
                lhs[:, left * TILE:(left + 1) * TILE], upper(half, left, right), preferred_element_type=f32
            )
        return value

    def fold(factor, half, into, at):
        for right in range(width // TILE):
            into[pl.ds(at, rank_max), pl.ds(right * TILE, TILE)] = times_upper(factor, half, right).astype(bf16)

    def solve_far(slot, source, half, right_side, needed):
        solved[slot] = right_side
        for owner in range(n - 2):
            @pl.when(needed(owner))
            def _():
                part_copy(owner, half).wait_recv()
                solved[slot] = solved[slot] - parts[half, owner]
        reduced = solved[slot].astype(bf16)
        for right in range(width // TILE):
            solved[slot, :, pl.ds(right * TILE, TILE)] = times_upper(reduced, half, right)

    def take_block(owner, half, own):
        first = block_first(owner)
        rows = pl.ds(owner * piece, piece)
        columns = pl.ds(first, width - first)
        @pl.when(jnp.logical_not(own & (col == owner)))
        def _():
            block_copy(owner, half).wait_recv()
            whole16[half, rows, columns] = whole[half, rows, columns].astype(bf16)
        @pl.when(own & (col == owner))
        def _():
            whole16[half, rows, columns] = inv_ref[:, columns]

    def onward_copy_in(slot, which):
        return remote(relay.at[which], tiles.at[slot, which], tiles_send.at[which], tiles_recv.at[slot, which], solver)

    def send_y(slot, source, without=0):
        for step in range(1, n):
            if step == without:
                continue
            @pl.when(feeds(source, source + step))
            def _():
                y_copy(slot, source, step).start()

    def send_final(slot, source):
        for target, other in others(source):
            @pl.when(other)
            def _():
                final_copy(slot, source, target).start()

    def transposed(value):
        return value.astype(f32).T.astype(bf16)

    @pl.when(first_row & jnp.logical_not(in_row))
    def _():
        part_copy(col, parity).start()
    for owner in range(n):
        @pl.when((col == owner) & jnp.logical_not(first_row | in_row))
        def _():
            block_copy(owner, parity).start()
    @pl.when(by_relay)
    def _():
        for which in range(2):
            relay_copy(which).start()
    @pl.when(moved)
    def _():
        rs_copy().start()
        v_copy().start()
        u_copy().start()
    @pl.when(lent)
    def _():
        v_copy().start()
        u_copy().start()
    @pl.when(second)
    def _():
        second_copy().start()
    @pl.when(jnp.logical_not(in_row))
    def _():
        log_copy(col, parity).start()
    @pl.when(is_relay)
    def _():
        for which in range(2):
            relay_copy(which).wait_recv()
            onward_copy(which, onto_slot).start()

    @pl.when(is_single)
    def _():
        @pl.when(for_first)
        def _():
            y = own_part[...]
            for owner in range(1, n):
                part_copy(owner, 0).wait_recv()
                y = y + parts[0, owner]
            result[0] = y

        @pl.when(jnp.logical_not(for_first))
        def _():
            @pl.when(for_even)
            def _():
                rs_copy().wait_recv()
                v_copy().wait_recv()
                u_copy().wait_recv()
                u16[...] = u_near[...].astype(bf16)
                v_pair[:, pl.ds(0, rank_max)] = transposed(v_near[...])
                v_pair[:, pl.ds(rank_max, rank_max)] = transposed(v_ref[...])
            @pl.when(for_odd)
            def _():
                rs_near[...] = rs_ref[...]
                v_pair[:, pl.ds(0, rank_max)] = transposed(v_ref[...])
            lhs[pl.ds(0, rank_max), :] = u16[...]
            lhs[pl.ds(rank_max, 16), :] = jnp.concatenate([rs_near[...]] * (16 // nrhs), axis=0).astype(bf16)
            for left in range(width // TILE):
                for owner in range(left * TILE // piece, (left + 1) * TILE // piece):
                    take_block(owner, kind, in_row)
                for right in range(left, width // TILE):
                    value = jnp.dot(lhs[:, pl.ds(left * TILE, TILE)], upper(kind, left, right), preferred_element_type=f32)
                    columns = pl.ds(right * TILE, TILE)
                    if left:
                        value = value + products[:, columns]
                    products[:, columns] = value
            folded[pl.ds(0, rank_max), :] = products[pl.ds(0, rank_max), :].astype(bf16)
            @pl.when(mine >= SECOND)
            def _():
                second_copy().wait_recv()
                u16[...] = u_second[...].astype(bf16)
                fold(u16, kind, folded, rank_max)

            @pl.when(mine == 1)
            def _():
                solved[0] = products[pl.ds(rank_max, nrhs), :]
            @pl.when(mine > 1)
            def _():
                share_logs(0, mine, kind)
                solve_far(0, mine, kind, rs_near[...],
                          lambda owner: (owner < mine - 2) | ((owner < mine - 1) & (mine < SECOND)))

            two = mine >= SECOND
            @pl.when(for_odd & jnp.logical_not(two))
            def _():
                y_copy(0, mine, 0).wait_recv()
                inner = jnp.dot(arrived[...].astype(bf16), v_pair[:, pl.ds(0, rank_max)], preferred_element_type=f32)
                update(inner.astype(bf16), rank_max)
            @pl.when(for_even & jnp.logical_not(two))
            def _():
                y_copy(0, mine, 0).wait_recv()
                inner = jnp.dot(arrived[...].astype(bf16), v_pair[...], preferred_element_type=f32)
                own_inner[...] = inner[:, rank_max:]
                update(inner[:, :rank_max].astype(bf16), rank_max)
            @pl.when(for_odd & two)
            def _():
                y_copy(0, mine, 0).wait_recv()
                inner_copy().wait_recv()
                inner = jnp.dot(arrived[...].astype(bf16), v_pair[:, pl.ds(0, rank_max)], preferred_element_type=f32)
                update(jnp.concatenate([inner, inner_second[...]], axis=1).astype(bf16), 2 * rank_max)
            @pl.when(for_even & two)
            def _():
                y_copy(0, mine, 0).wait_recv()
                inner = jnp.dot(arrived[...].astype(bf16), v_pair[...], preferred_element_type=f32)
                own_inner[...] = inner[:, rank_max:]
                inner_copy().start()
                inner_copy().wait_recv()
                update(jnp.concatenate([inner[:, :rank_max], inner_second[...]], axis=1).astype(bf16), 2 * rank_max)

        @pl.when(feeds_extra(mine))
        def _():
            extra_copy(0, mine).start()
        send_y(0, mine)
        send_final(0, mine)
        @pl.when(for_even & sends_part)
        def _():
            own_part[...] = jnp.dot(own_inner[...].astype(bf16), u32[...].astype(bf16), preferred_element_type=f32)
            part_copy(col, parity).start()
        @pl.when(mine <= 1)
        def _():
            share_logs(0, mine, kind)

    @pl.when(pair)
    def _():
        lower, upper_row = row - 1, row
        rs_copy().wait_recv()
        v_copy().wait_recv()
        v_pair[:, pl.ds(0, rank_max)] = transposed(v_near[...])
        v_pair[:, pl.ds(rank_max, rank_max)] = transposed(v_ref[...])
        u_copy().wait_recv()
        factors[pl.ds(0, rank_max), :] = u_near[...].astype(bf16)
        factors[pl.ds(2 * rank_max, rank_max), :] = u16[...]
        for slot in range(3):
            for which in range(2):
                onward_copy_in(slot, which).wait_recv()
        factors[pl.ds(rank_max, rank_max), :] = tiles[1, 0].astype(bf16)
        factors[pl.ds(3 * rank_max, rank_max), :] = tiles[2, 0].astype(bf16)
        factors[pl.ds(4 * rank_max, rank_max), :] = tiles[0, 0].astype(bf16)
        v_pair2[:, pl.ds(0, rank_max)] = transposed(tiles[1, 1])
        v_pair2[:, pl.ds(rank_max, rank_max)] = transposed(tiles[2, 1])
        v_last[...] = transposed(tiles[0, 1])
        for left in reversed(range(width // TILE)):
            for half, at in ((0, pl.ds(0, 2 * rank_max)), (1, pl.ds(2 * rank_max, 3 * rank_max))):
                for owner in reversed(range(left * TILE // piece, (left + 1) * TILE // piece)):
                    take_block(owner, half, half == 1)
                for right in range(left, width // TILE):
                    columns = pl.ds(right * TILE, TILE)
                    value = jnp.dot(
                        factors[at, pl.ds(left * TILE, TILE)], upper(half, left, right), preferred_element_type=f32
                    )
                    if left < right:
                        value = value + sums[at, columns]
                    if left:
                        sums[at, columns] = value
                    elif half == 0:
                        folded[:, columns] = value.astype(bf16)
                    else:
                        folded2[:, columns] = value.astype(bf16)
        share_logs(0, lower, 0)
        share_logs(1, upper_row, 1)
        solved[0] = rs_near[...]
        solved[1] = rs_ref[...]
        for owner in range(n - 2):
            @pl.when(owner <= row - 6)
            def _():
                for half in range(2):
                    part_copy(owner, half).wait_recv()
                    solved[half] = solved[half] - parts[half, owner]
        own_part_of = pl.ds(0, rank_max)
        other_part_of = pl.ds(rank_max, rank_max)

        def near_products(y, v, part, first):
            inner = jnp.dot(y.astype(bf16), v, preferred_element_type=f32).astype(bf16)
            low = jnp.dot(inner[:, :rank_max], folded[part, :], preferred_element_type=f32)
            high = jnp.dot(inner[:, rank_max:], folded2[part, :], preferred_element_type=f32)
            held[0] = low if first else held[0] + low
            held[1] = high if first else held[1] + high

        @pl.when(lean(lower, n) == 1)
        def _():
            extra_copy(0, 0).wait_recv()
            near_products(arrived2[...], v_pair2[...], other_part_of, True)
            y_copy(0, mine, 0).wait_recv()
            near_products(arrived[...], v_pair[...], own_part_of, False)
        @pl.when(lean(lower, n) == 2)
        def _():
            y_copy(0, mine, 0).wait_recv()
            near_products(arrived[...], v_pair[...], own_part_of, True)
            extra_copy(0, 0).wait_recv()
            near_products(arrived2[...], v_pair2[...], other_part_of, False)
        for owner in (row - 5, row - 4):
            @pl.when(owner >= 0)
            def _():
                for half in range(2):
                    part_copy(owner, half).wait_recv()
                    solved[half] = solved[half] - parts[half, owner]
        reduced = solved[0].astype(bf16)
        y_low = jnp.concatenate(
            [times_upper(reduced, 0, right) for right in range(width // TILE)], axis=1
        ) - held[0]
        result[0] = y_low
        @pl.when(feeds_extra(lower))
        def _():
            extra_copy(0, lower).start()
        @pl.when(feeds(lower, lower + 3))
        def _():
            y_copy(0, lower, 3).start()
        last = jnp.dot(y_low.astype(bf16), v_last[...], preferred_element_type=f32).astype(bf16)
        reduced = solved[1].astype(bf16)
        result[1] = (
            jnp.concatenate([times_upper(reduced, 1, right) for right in range(width // TILE)], axis=1)
            - held[1]
            - jnp.dot(last, folded2[pl.ds(2 * rank_max, rank_max), :], preferred_element_type=f32)
        )
        @pl.when(feeds_extra(upper_row))
        def _():
            extra_copy(1, upper_row).start()
        send_y(1, upper_row)
        send_y(0, lower, without=3)
        send_final(1, upper_row)
        send_final(0, lower)

    @pl.when(double)
    def _():
        v_copy().wait_recv()
        v_pair[:, pl.ds(0, rank_max)] = transposed(v_near[...])
        v_pair[:, pl.ds(rank_max, rank_max)] = transposed(v_ref[...])
        u_copy().wait_recv()
        folded[pl.ds(0, rank_max), :] = u_near[...].astype(bf16)
        y_copy(0, mine, 0).wait_recv()
        inner = jnp.dot(arrived[...].astype(bf16), v_pair[...], preferred_element_type=f32).astype(bf16)
        low_part[...] = jnp.dot(inner[:, :rank_max], folded[pl.ds(0, rank_max), :], preferred_element_type=f32)
        own_part[...] = jnp.dot(inner[:, rank_max:], u16[...], preferred_element_type=f32)
        low_part_copy(col).start()
        part_copy(col, 1).start()

    @pl.when(is_worker)
    def _():
        y_copy(0, mine, 0).wait_recv()
        inner = inner_of(arrived[...], v_ref[...])
        @pl.when(second)
        def _():
            own_inner[...] = inner
            inner_copy().start()
        @pl.when(sends_part)
        def _():
            own_part[...] = jnp.dot(inner.astype(bf16), u16[...], preferred_element_type=f32)
            part_copy(col, parity).start()

    @pl.when(pair)
    def _():
        finish(result[1], logs_all[1])
    @pl.when(in_row & jnp.logical_not(pair))
    def _():
        finish(result[0], logs_all[0])
    @pl.when(jnp.logical_not(in_row))
    def _():
        logs_copy(0, mine, 0).wait_recv()
        final_copy(0, mine, 0).wait_recv()
        finish(final[...], logs_in[...])

    for owner in range(n):
        @pl.when((col == owner) & jnp.logical_not(first_row | in_row))
        def _():
            block_copy(owner, parity).wait_send()
    @pl.when(moved)
    def _():
        rs_copy().wait_send()
        v_copy().wait_send()
        u_copy().wait_send()
    @pl.when(lent)
    def _():
        v_copy().wait_send()
        u_copy().wait_send()
    @pl.when(double)
    def _():
        low_part_copy(col).wait_send()
        part_copy(col, 1).wait_send()
    @pl.when(second)
    def _():
        second_copy().wait_send()
        inner_copy().wait_send()
    @pl.when(by_relay)
    def _():
        for which in range(2):
            relay_copy(which).wait_send()
    @pl.when(is_relay)
    def _():
        for which in range(2):
            onward_copy(which, onto_slot).wait_send()
    @pl.when(jnp.logical_not(in_row))
    def _():
        log_copy(col, parity).wait_send()
    @pl.when(sends_part | (first_row & jnp.logical_not(in_row)))
    def _():
        part_copy(col, parity).wait_send()
    for slot, source, active in served:
        @pl.when(active)
        def _():
            @pl.when(feeds_extra(source))
            def _():
                extra_copy(slot, source).wait_send()
            for step in range(1, n):
                @pl.when(feeds(source, source + step))
                def _():
                    y_copy(slot, source, step).wait_send()
            for target, other in others(source):
                @pl.when(other)
                def _():
                    final_copy(slot, source, target).wait_send()
                    logs_copy(slot, source, target).wait_send()


def outputs(y_ref, log_ref, white_ref, lik_ref):
    y = y_ref[...]
    nrhs, width = y.shape
    lik = -0.5 * jnp.sum(y * y, axis=1, keepdims=True) * (1.0 / width) + log_ref[0:1, 0:1] - 0.5 * math.log(2.0 * math.pi)
    diagonal = lax.broadcasted_iota(jnp.int32, (nrhs, nrhs), 0) == lax.broadcasted_iota(jnp.int32, (nrhs, nrhs), 1)
    lik_ref[...] = jnp.sum(jnp.where(diagonal, lik, 0.0), axis=0, keepdims=True)
    white_ref[...] = y


def local(n, right_side, inverse_t, u_factor, v_factor, ranks):
    nrhs, width = right_side.shape[2:]
    piece = inverse_t.shape[2]
    rank_max = u_factor.shape[4]
    f32, bf16 = jnp.float32, jnp.bfloat16
    vmem = pl.BlockSpec(memory_space=pltpu.VMEM)
    dma = pltpu.SemaphoreType.DMA
    rows = pltpu.VMEM((nrhs, width), f32)
    two_rows = pltpu.VMEM((2, nrhs, width), f32)
    small = pltpu.VMEM((8, LANES), f32)
    factor32 = pltpu.VMEM((rank_max, width), f32)
    factor16 = pltpu.VMEM((rank_max, width), bf16)
    inner = pltpu.VMEM((nrhs, rank_max), f32)
    y, log_mean = pl.pallas_call(
        functools.partial(kernel, n),
        out_shape=(jax.ShapeDtypeStruct((nrhs, width), f32), jax.ShapeDtypeStruct((8, LANES), f32)),
        in_specs=[vmem, vmem, vmem, vmem, pl.BlockSpec(memory_space=pltpu.SMEM)],
        out_specs=(vmem, vmem),
        scratch_shapes=[
            pltpu.VMEM((piece, width), f32),
            pltpu.VMEM((2, width, width), f32),
            pltpu.VMEM((2, width, width), bf16),
            factor32,
            factor32,
            factor16,
            factor32,
            factor32,
            pltpu.VMEM((width, 2 * rank_max), bf16),
            pltpu.VMEM((width, 2 * rank_max), bf16),
            pltpu.VMEM((width, rank_max), bf16),
            pltpu.VMEM((5 * rank_max, width), bf16),
            pltpu.VMEM((5 * rank_max, width), f32),
            factor32,
            rows,
            pltpu.VMEM((3, 2, rank_max, width), f32),
            pltpu.VMEM((2, rank_max, width), f32),
            pltpu.VMEM((2 * rank_max, width), bf16),
            pltpu.VMEM((3 * rank_max, width), bf16),
            pltpu.VMEM((max(piece, LANES), width), bf16),
            pltpu.VMEM((rank_max + 16, width), bf16),
            pltpu.VMEM((rank_max + 16, width), f32),
            rows,
            rows,
            rows,
            rows,
            pltpu.VMEM((2, n, nrhs, width), f32),
            inner,
            inner,
            two_rows,
            two_rows,
            two_rows,
            rows,
            small,
            pltpu.VMEM((2, n, 8, LANES), f32),
            pltpu.VMEM((2, 8, LANES), f32),
            small,
            dma, dma((2, n)), dma((4,)), dma((4,)), dma, dma, dma((2, n)), dma, dma((2,)), dma,
            dma((2,)), dma((2, n)), dma((2, n)), dma, dma, dma((2, n)), dma((2, n)), dma,
            dma((2,)), dma((2,)), dma((2,)), dma((3, 2)),
        ],
        compiler_params=pltpu.CompilerParams(collective_id=0, has_side_effects=True),
    )(
        right_side.reshape(nrhs, width),
        inverse_t.reshape(piece, width),
        u_factor.reshape(rank_max, width),
        v_factor.reshape(rank_max, width),
        ranks.reshape(1, 1),
    )
    white, lik = pl.pallas_call(
        outputs,
        out_shape=(jax.ShapeDtypeStruct((nrhs, width), f32), jax.ShapeDtypeStruct((1, nrhs), f32)),
        in_specs=[vmem, vmem],
        out_specs=(vmem, vmem),
    )(y, log_mean)
    return white.reshape(1, 1, nrhs, width), lik.reshape(1, 1, nrhs)


def solution(mesh):
    return jax.shard_map(
        functools.partial(local, mesh.shape["row"]),
        mesh=mesh,
        in_specs=(
            P(None, "row", None, None),
            P(None, "row", "col", None),
            P(None, "row", None, "col", None, None),
            P(None, "row", None, "col", None, None),
            P(None, "row", None, "col"),
        ),
        out_specs=(P(None, "row", None, None), P(None, "row", None)),
        check_vma=False,
    )
```

```python
import functools
import math

import jax
import jax.numpy as jnp
from jax import lax
from jax.experimental import pallas as pl
from jax.experimental.pallas import tpu as pltpu
from jax.sharding import PartitionSpec as P

MESH = pl.DeviceIdType.MESH
LANES = 128
TILE = 256
SECOND = 4


def first_pair(n):
    return 6 if n == 16 else 2


def lean(base, n):
    return 2 - lax.rem(base // 2, 2) if n == 16 else LEAN


LEAN = 1


def solver_of(row, n):
    parity = lax.rem(row, 2)
    base = row - parity
    paired = row >= first_pair(n)
    return (jnp.where((parity == 0) & (row > 0), row + 1, row),
            jnp.where(paired, base - lean(base, n), jnp.maximum(row - 1, 0)))


def kernel(n, rs_ref, inv_ref, u_ref, v_ref, rank_ref, white_ref, lik_ref,
           block, block_in, whole, whole16, u32, v32, u16, u_near, v_near, v_pair, v_pair2, v_last, factors, sums, u_second, rs_near,
           tiles, relay, folded, folded2, padded, lhs, products,
           arrived, arrived2, own_part, low_part, parts, own_inner, inner_second, held, solved, result, final,
           logs, logs_parts, logs_all, logs_in,
           block_send, block_recv, tile_send, tile_recv, inner_send, inner_recv, y_send, y_recv, extra_send, extra_recv,
           part_send, part_recv, final_send, final_recv, log_send, log_recv, logs_send, logs_recv,
           relay_send, relay_recv, tiles_send, tiles_recv, detour_send, detour_recv):
    row = lax.axis_index("row")
    col = lax.axis_index("col")
    piece, width = inv_ref.shape
    rank_max = u_ref.shape[0]
    nrhs = rs_ref.shape[0]
    f32, bf16 = jnp.float32, jnp.bfloat16
    start_pairs = first_pair(n)
    shift = 4 if n == 16 else LEAN + 1

    parity = lax.rem(row, 2)
    odd = parity == 1
    paired = row >= start_pairs
    single = jnp.logical_not(paired)
    pair_row = row - parity
    own_col = pair_row - lean(pair_row, n)
    other_col = pair_row - 3 + lean(pair_row, n)
    pair = odd & (col == own_col) & paired
    for_odd = odd & (col == row - 1) & single
    for_even = odd & (col == row - 2) & single
    for_first = (row == 0) & (col == 0)
    is_single = for_odd | for_even | for_first
    is_solver = is_single | pair
    mine = jnp.where(for_even | pair, row - 1, row)
    kind = lax.rem(mine, 2)
    served = ((0, mine, is_solver), (1, row, pair))
    solver = solver_of(row, n)
    in_row = for_odd | for_first | pair
    first_row = row == 0
    near = col == row - 1
    moved = jnp.where(paired, col == own_col, near) & jnp.logical_not(odd)
    second = (col == row - 2) & (row >= SECOND) & single
    by_x = paired & odd & near
    by_up = paired & jnp.logical_not(odd) & (col == other_col)
    by_down = paired & odd & (col == other_col)
    by_relay = by_x | by_up | by_down
    far = paired & (col <= pair_row - 3)
    lent = far & jnp.logical_not(odd)
    double = far & odd
    takes_y = jnp.where(paired, double | pair, (col < row) & jnp.logical_not(moved))
    sends_part = single & ((col < row - 2) | ((col == row - 2) & (row < SECOND)))
    is_worker = takes_y & single & jnp.logical_not(is_solver)
    west_row, west_col = (row, lax.rem(own_col + n - shift, n)) if n == 16 else (row - 2, own_col)
    def goes_up(base):
        return (lean(base, n) == 2) | (base > start_pairs)

    z_row = jnp.where(goes_up(pair_row), lax.rem(row + 2, n), row - 2)
    relay_row = jnp.where(by_x, row, jnp.where(by_up, z_row, west_row))
    relay_col = jnp.where(by_x, lax.rem(own_col + shift, n), jnp.where(by_up, own_col, west_col))
    x_relay = paired & odd & (col == lax.rem(own_col + shift, n))
    below_row, above_row = lax.rem(row + n - 2, n), row + 2
    from_below = (below_row >= start_pairs) & goes_up(below_row) & (col == below_row - lean(below_row, n))
    from_above = (
        (above_row < n) & (above_row >= start_pairs) & jnp.logical_not(goes_up(above_row)) & (col == above_row - 1)
    )
    up_relay = jnp.logical_not(odd) & (from_below | from_above)
    up_row = jnp.where(from_below, below_row, above_row)
    if n == 16:
        west_relay = paired & odd & (col == west_col)
        west_from = row
    else:
        west_relay = odd & (row + 2 > start_pairs) & (row + 2 < n) & (col == row + 1 - lean(row + 1, n))
        west_from = row + 2
    is_relay = x_relay | up_relay | west_relay
    from_row = jnp.where(x_relay, row, jnp.where(up_relay, up_row, west_from))
    from_col = jnp.where(
        x_relay, row - 1,
        jnp.where(up_relay, up_row - 3 + lean(up_row, n), west_from - 4 + lean(west_from - 1, n))
    )
    onto_slot = jnp.where(x_relay, 0, jnp.where(up_relay, 1, 2))

    detours = [(2, 1, row == 1)]
    if n == 16:
        detours += [(0, 3, paired & (lean(pair_row, n) == 2)), (4, 7, paired & (lean(pair_row, n) == 2))]
    takes_detour, detour_col, serves_detour, detour_from = False, 0, False, 0
    for owner, third, condition in detours:
        takes_detour = takes_detour | (condition & (col == owner))
        detour_col = jnp.where(col == owner, third, detour_col)
        serves_detour = serves_detour | (condition & (col == third))
        detour_from = jnp.where(col == third, owner, detour_from)

    def feeds(source, target):
        base = target - lax.rem(target, 2)
        early = jnp.logical_not((target == source + 1) & (lax.rem(target, 2) == 0))
        late = ((source <= base - 3) | (source == base - lean(base, n))) & (lax.rem(target, 2) == 1)
        return (target > source) & (target < n) & jnp.where(target >= start_pairs, late, early)

    def next_base(source):
        return source + 2 - lax.rem(source, 2)

    def feeds_extra(source):
        base = next_base(source)
        return (base >= start_pairs) & (base < n) & (source != base - lean(base, n))

    def extra_target(source):
        base = next_base(source)
        return base + 1, base - lean(base, n)

    barrier = pltpu.get_barrier_semaphore()

    def greet(condition, device):
        @pl.when(condition)
        def _():
            pl.semaphore_signal(barrier, inc=1, device_id=device, device_id_type=MESH)
        return condition.astype(jnp.int32)

    waits = 0
    for slot, source, active in served:
        @pl.when(active)
        def _():
            for step in range(n):
                greet(jnp.logical_not((source == row) & (col == step)), (source, step))
            for step in range(1, n):
                greet(feeds(source, source + step), (source + step, source))
            greet(feeds_extra(source), extra_target(source))
        met = n - (source == row).astype(jnp.int32) + feeds_extra(source).astype(jnp.int32)
        for step in range(1, n):
            met = met + feeds(source, source + step).astype(jnp.int32)
        waits = waits + jnp.where(active, met, 0)
    waits = waits + greet(jnp.logical_not(in_row), solver)
    waits = waits + greet(takes_y, solver_of(col, n))
    greet(takes_detour, (row, detour_col))
    greet(serves_detour, (row, detour_from))
    waits = waits + takes_detour.astype(jnp.int32) + serves_detour.astype(jnp.int32)

    @pl.when(paired)
    def _():
        greet(pair, solver_of(other_col, n))
        greet(by_relay, (relay_row, relay_col))
        greet(lent, (row + 1, col))
        greet(double, (row - 1, col))
        greet(pair, (row, lax.rem(own_col + shift, n)))
        greet(pair, (jnp.where(goes_up(pair_row), lax.rem(row + 1, n), row - 3), col))
        greet(pair, (west_row, west_col))
    @pl.when(is_relay)
    def _():
        greet(is_relay, (from_row, from_col))
        greet(is_relay, solver_of(from_row, n))
    for count, condition in ((4, pair), (1, by_relay), (1, lent), (1, double), (2, is_relay)):
        waits = waits + jnp.where(condition, count, 0)

    block[...] = inv_ref[...].astype(f32)
    keep = lax.broadcasted_iota(jnp.int32, u_ref.shape, 0) < rank_ref[0, 0]
    u32[...] = jnp.where(keep, u_ref[...].astype(f32), 0.0)
    u16[...] = u32[...].astype(bf16)
    @pl.when(moved | by_relay | lent)
    def _():
        v32[...] = v_ref[...].astype(f32)

    span = max(piece, LANES)
    base = pl.multiple_of(col * piece // span * span, span)
    offset = col * piece - base
    @pl.when(first_row)
    def _():
        padded[...] = jnp.zeros(padded.shape, bf16)
        padded[pl.ds(pl.multiple_of(offset, piece), piece), :] = inv_ref[...]
        own_part[...] = jnp.dot(rs_ref[:, pl.ds(base, span)].astype(bf16), padded[...], preferred_element_type=f32)

    log_base = pl.multiple_of(col * piece // LANES * LANES, LANES)
    total = jnp.zeros((1, LANES), f32)
    for start in range(0, piece, LANES):
        height = min(LANES, piece - start)
        square = block[pl.ds(start, height), pl.ds(log_base + start, LANES)]
        rows_at = lax.broadcasted_iota(jnp.int32, square.shape, 0) + (col * piece - log_base)
        on_diagonal = rows_at == lax.broadcasted_iota(jnp.int32, square.shape, 1)
        total = total + jnp.sum(jnp.log(jnp.where(on_diagonal, square, 1.0)), axis=0, keepdims=True)
    own_log = jnp.sum(total, axis=1, keepdims=True) * (1.0 / width)
    logs[...] = jnp.broadcast_to(own_log, logs.shape)

    @pl.when(is_solver)
    def _():
        for half in range(2):
            for tile in range(width // TILE):
                whole16[half, pl.ds(tile * TILE + LANES, LANES), pl.ds(tile * TILE, LANES)] = jnp.zeros(
                    (LANES, LANES), bf16
                )

    pl.semaphore_wait(barrier, waits)

    def block_first(owner):
        return owner * piece // LANES * LANES

    def remote(source, target, send, recv, device):
        return pltpu.make_async_remote_copy(
            src_ref=source, dst_ref=target, send_sem=send, recv_sem=recv, device_id=device, device_id_type=MESH
        )

    def block_copy(owner, half):
        first = block_first(owner)
        return remote(
            block.at[:, pl.ds(first, width - first)],
            whole.at[half, pl.ds(owner * piece, piece), pl.ds(first, width - first)],
            block_send, block_recv.at[half, owner], solver,
        )

    tile_device = (jnp.where(lent, row + 1, solver[0]), jnp.where(lent, col, solver[1]))

    def detour_copy():
        return remote(block, block_in, block_send, detour_recv, (row, detour_col))

    def detour_onward(owner):
        first = block_first(owner)
        return remote(
            block_in.at[:, pl.ds(first, width - first)],
            whole.at[parity, pl.ds(owner * piece, piece), pl.ds(first, width - first)],
            detour_send, block_recv.at[parity, owner], solver,
        )

    def u_copy():
        return remote(u32, u_near, tile_send.at[0], tile_recv.at[0], tile_device)

    def v_copy():
        return remote(v32, v_near, tile_send.at[1], tile_recv.at[1], tile_device)

    def rs_copy():
        return remote(rs_ref, rs_near, tile_send.at[2], tile_recv.at[2], solver)

    def second_copy():
        return remote(u32, u_second, tile_send.at[3], tile_recv.at[3], solver)

    def relay_copy(which):
        return remote(
            (u32, v32)[which], relay.at[which], relay_send.at[which], relay_recv.at[which], (relay_row, relay_col)
        )

    def onward_copy(which, slot):
        return remote(
            relay.at[which], tiles.at[slot, which], tiles_send.at[which], tiles_recv.at[slot, which],
            solver_of(from_row, n),
        )

    def inner_copy():
        return remote(own_inner, inner_second, inner_send, inner_recv, solver)

    def y_copy(slot, source, step):
        return remote(result.at[slot], arrived, y_send.at[slot, step], y_recv, (source + step, source))

    def extra_copy(slot, source):
        return remote(result.at[slot], arrived2, extra_send.at[slot], extra_recv, extra_target(source))

    def part_copy(owner, half):
        return remote(own_part, parts.at[half, owner], part_send.at[0], part_recv.at[half, owner], solver)

    def low_part_copy(owner):
        return remote(low_part, parts.at[0, owner], part_send.at[1], part_recv.at[0, owner], solver)

    def log_copy(owner, half):
        return remote(logs, logs_parts.at[half, owner], log_send, log_recv.at[half, owner], solver)

    def final_copy(slot, source, target):
        return remote(result.at[slot], final, final_send.at[slot, target], final_recv, (source, target))

    def logs_copy(slot, source, target):
        return remote(logs_all.at[slot], logs_in, logs_send.at[slot, target], logs_recv, (source, target))

    def inner_of(y, v):
        return lax.dot_general(y.astype(bf16), v, (((1,), (1,)), ((), ())), preferred_element_type=f32)

    def finish(y, log_mean):
        lik_ref[...] = log_mean
        white_ref[...] = y

    def update(inner, depth):
        result[0] = solved[0] - jnp.dot(inner, folded[pl.ds(0, depth), :], preferred_element_type=f32)

    def others(source):
        for target in range(n):
            yield target, jnp.logical_not((source == row) & (col == target))

    def share_logs(slot, source, half):
        logs_all[slot] = jnp.where(source == row, logs[...], 0.0)
        for owner, other in others(source):
            @pl.when(other)
            def _():
                log_copy(owner, half).wait_recv()
                logs_all[slot] = logs_all[slot] + logs_parts[half, owner]
        for target, other in others(source):
            @pl.when(other)
            def _():
                logs_copy(slot, source, target).start()

    def upper(half, left, right):
        return whole16[half, pl.ds(left * TILE, TILE), pl.ds(right * TILE, TILE)]

    def times_upper(lhs, half, right):
        value = jnp.zeros((lhs.shape[0], TILE), f32)
        for left in range(right + 1):
            value = value + jnp.dot(
                lhs[:, left * TILE:(left + 1) * TILE], upper(half, left, right), preferred_element_type=f32
            )
        return value

    def fold(factor, half, into, at):
        for right in range(width // TILE):
            into[pl.ds(at, rank_max), pl.ds(right * TILE, TILE)] = times_upper(factor, half, right).astype(bf16)

    def solve_far(slot, source, half, right_side, needed):
        solved[slot] = right_side
        for owner in range(n - 2):
            @pl.when(needed(owner))
            def _():
                part_copy(owner, half).wait_recv()
                solved[slot] = solved[slot] - parts[half, owner]
        reduced = solved[slot].astype(bf16)
        for right in range(width // TILE):
            solved[slot, :, pl.ds(right * TILE, TILE)] = times_upper(reduced, half, right)

    def take_block(owner, half, own):
        first = block_first(owner)
        rows = pl.ds(owner * piece, piece)
        columns = pl.ds(first, width - first)
        @pl.when(jnp.logical_not(own & (col == owner)))
        def _():
            block_copy(owner, half).wait_recv()
            whole16[half, rows, columns] = whole[half, rows, columns].astype(bf16)
        @pl.when(own & (col == owner))
        def _():
            whole16[half, rows, columns] = inv_ref[:, columns]

    def onward_copy_in(slot, which):
        return remote(relay.at[which], tiles.at[slot, which], tiles_send.at[which], tiles_recv.at[slot, which], solver)

    def send_y(slot, source, without=0):
        for step in range(1, n):
            if step == without:
                continue
            @pl.when(feeds(source, source + step))
            def _():
                y_copy(slot, source, step).start()

    def send_final(slot, source):
        for target, other in others(source):
            @pl.when(other)
            def _():
                final_copy(slot, source, target).start()

    def transposed(value):
        return value.astype(f32).T.astype(bf16)

    @pl.when(first_row & jnp.logical_not(in_row))
    def _():
        part_copy(col, parity).start()
    for owner in range(n):
        @pl.when((col == owner) & jnp.logical_not(first_row | in_row | takes_detour))
        def _():
            block_copy(owner, parity).start()
    @pl.when(takes_detour)
    def _():
        detour_copy().start()
    @pl.when(by_relay)
    def _():
        for which in range(2):
            relay_copy(which).start()
    @pl.when(moved)
    def _():
        rs_copy().start()
        v_copy().start()
        u_copy().start()
    @pl.when(lent)
    def _():
        v_copy().start()
        u_copy().start()
    @pl.when(second)
    def _():
        second_copy().start()
    @pl.when(jnp.logical_not(in_row))
    def _():
        log_copy(col, parity).start()
    for owner, third, condition in detours:
        @pl.when(condition & (col == third))
        def _():
            detour_copy().wait_recv()
            detour_onward(owner).start()
    @pl.when(is_relay)
    def _():
        for which in range(2):
            relay_copy(which).wait_recv()
            onward_copy(which, onto_slot).start()

    @pl.when(is_single)
    def _():
        @pl.when(for_first)
        def _():
            y = own_part[...]
            for owner in range(1, n):
                part_copy(owner, 0).wait_recv()
                y = y + parts[0, owner]
            result[0] = y

        @pl.when(jnp.logical_not(for_first))
        def _():
            @pl.when(for_even)
            def _():
                rs_copy().wait_recv()
                v_copy().wait_recv()
                u_copy().wait_recv()
                u16[...] = u_near[...].astype(bf16)
                v_pair[:, pl.ds(0, rank_max)] = transposed(v_near[...])
                v_pair[:, pl.ds(rank_max, rank_max)] = transposed(v_ref[...])
            @pl.when(for_odd)
            def _():
                rs_near[...] = rs_ref[...]
                v_pair[:, pl.ds(0, rank_max)] = transposed(v_ref[...])
            lhs[pl.ds(0, rank_max), :] = u16[...]
            lhs[pl.ds(rank_max, 16), :] = jnp.concatenate([rs_near[...]] * (16 // nrhs), axis=0).astype(bf16)
            for left in range(width // TILE):
                for owner in range(left * TILE // piece, (left + 1) * TILE // piece):
                    take_block(owner, kind, in_row)
                for right in range(left, width // TILE):
                    value = jnp.dot(lhs[:, pl.ds(left * TILE, TILE)], upper(kind, left, right), preferred_element_type=f32)
                    columns = pl.ds(right * TILE, TILE)
                    if left:
                        value = value + products[:, columns]
                    products[:, columns] = value
            folded[pl.ds(0, rank_max), :] = products[pl.ds(0, rank_max), :].astype(bf16)
            @pl.when(mine >= SECOND)
            def _():
                second_copy().wait_recv()
                u16[...] = u_second[...].astype(bf16)
                fold(u16, kind, folded, rank_max)

            @pl.when(mine == 1)
            def _():
                solved[0] = products[pl.ds(rank_max, nrhs), :]
            @pl.when(mine > 1)
            def _():
                share_logs(0, mine, kind)
                solve_far(0, mine, kind, rs_near[...],
                          lambda owner: (owner < mine - 2) | ((owner < mine - 1) & (mine < SECOND)))

            two = mine >= SECOND
            @pl.when(for_odd & jnp.logical_not(two))
            def _():
                y_copy(0, mine, 0).wait_recv()
                inner = jnp.dot(arrived[...].astype(bf16), v_pair[:, pl.ds(0, rank_max)], preferred_element_type=f32)
                update(inner.astype(bf16), rank_max)
            @pl.when(for_even & jnp.logical_not(two))
            def _():
                y_copy(0, mine, 0).wait_recv()
                inner = jnp.dot(arrived[...].astype(bf16), v_pair[...], preferred_element_type=f32)
                own_inner[...] = inner[:, rank_max:]
                update(inner[:, :rank_max].astype(bf16), rank_max)
            @pl.when(for_odd & two)
            def _():
                y_copy(0, mine, 0).wait_recv()
                inner_copy().wait_recv()
                inner = jnp.dot(arrived[...].astype(bf16), v_pair[:, pl.ds(0, rank_max)], preferred_element_type=f32)
                update(jnp.concatenate([inner, inner_second[...]], axis=1).astype(bf16), 2 * rank_max)
            @pl.when(for_even & two)
            def _():
                y_copy(0, mine, 0).wait_recv()
                inner = jnp.dot(arrived[...].astype(bf16), v_pair[...], preferred_element_type=f32)
                own_inner[...] = inner[:, rank_max:]
                inner_copy().start()
                inner_copy().wait_recv()
                update(jnp.concatenate([inner[:, :rank_max], inner_second[...]], axis=1).astype(bf16), 2 * rank_max)

        @pl.when(feeds_extra(mine))
        def _():
            extra_copy(0, mine).start()
        send_y(0, mine)
        send_final(0, mine)
        @pl.when(for_even & sends_part)
        def _():
            own_part[...] = jnp.dot(own_inner[...].astype(bf16), u32[...].astype(bf16), preferred_element_type=f32)
            part_copy(col, parity).start()
        @pl.when(mine <= 1)
        def _():
            share_logs(0, mine, kind)

    @pl.when(pair)
    def _():
        lower, upper_row = row - 1, row
        rs_copy().wait_recv()
        v_copy().wait_recv()
        v_pair[:, pl.ds(0, rank_max)] = transposed(v_near[...])
        v_pair[:, pl.ds(rank_max, rank_max)] = transposed(v_ref[...])
        u_copy().wait_recv()
        factors[pl.ds(0, rank_max), :] = u_near[...].astype(bf16)
        factors[pl.ds(2 * rank_max, rank_max), :] = u16[...]
        for slot in range(3):
            for which in range(2):
                onward_copy_in(slot, which).wait_recv()
        factors[pl.ds(rank_max, rank_max), :] = tiles[1, 0].astype(bf16)
        factors[pl.ds(3 * rank_max, rank_max), :] = tiles[2, 0].astype(bf16)
        factors[pl.ds(4 * rank_max, rank_max), :] = tiles[0, 0].astype(bf16)
        v_pair2[:, pl.ds(0, rank_max)] = transposed(tiles[1, 1])
        v_pair2[:, pl.ds(rank_max, rank_max)] = transposed(tiles[2, 1])
        v_last[...] = transposed(tiles[0, 1])
        for left in reversed(range(width // TILE)):
            for half, at in ((0, pl.ds(0, 2 * rank_max)), (1, pl.ds(2 * rank_max, 3 * rank_max))):
                for owner in reversed(range(left * TILE // piece, (left + 1) * TILE // piece)):
                    take_block(owner, half, half == 1)
                for right in range(left, width // TILE):
                    columns = pl.ds(right * TILE, TILE)
                    value = jnp.dot(
                        factors[at, pl.ds(left * TILE, TILE)], upper(half, left, right), preferred_element_type=f32
                    )
                    if left < right:
                        value = value + sums[at, columns]
                    if left:
                        sums[at, columns] = value
                    elif half == 0:
                        folded[:, columns] = value.astype(bf16)
                    else:
                        folded2[:, columns] = value.astype(bf16)
        share_logs(0, lower, 0)
        share_logs(1, upper_row, 1)
        solved[0] = rs_near[...]
        solved[1] = rs_ref[...]
        for owner in range(n - 2):
            @pl.when(owner <= row - 6)
            def _():
                for half in range(2):
                    part_copy(owner, half).wait_recv()
                    solved[half] = solved[half] - parts[half, owner]
        own_part_of = pl.ds(0, rank_max)
        other_part_of = pl.ds(rank_max, rank_max)

        def near_products(y, v, part, first):
            inner = jnp.dot(y.astype(bf16), v, preferred_element_type=f32).astype(bf16)
            low = jnp.dot(inner[:, :rank_max], folded[part, :], preferred_element_type=f32)
            high = jnp.dot(inner[:, rank_max:], folded2[part, :], preferred_element_type=f32)
            held[0] = low if first else held[0] + low
            held[1] = high if first else held[1] + high

        @pl.when(lean(lower, n) == 1)
        def _():
            extra_copy(0, 0).wait_recv()
            near_products(arrived2[...], v_pair2[...], other_part_of, True)
            y_copy(0, mine, 0).wait_recv()
            near_products(arrived[...], v_pair[...], own_part_of, False)
        @pl.when(lean(lower, n) == 2)
        def _():
            y_copy(0, mine, 0).wait_recv()
            near_products(arrived[...], v_pair[...], own_part_of, True)
            extra_copy(0, 0).wait_recv()
            near_products(arrived2[...], v_pair2[...], other_part_of, False)
        for owner in (row - 5, row - 4):
            @pl.when(owner >= 0)
            def _():
                for half in range(2):
                    part_copy(owner, half).wait_recv()
                    solved[half] = solved[half] - parts[half, owner]
        reduced = solved[0].astype(bf16)
        y_low = jnp.concatenate(
            [times_upper(reduced, 0, right) for right in range(width // TILE)], axis=1
        ) - held[0]
        result[0] = y_low
        @pl.when(feeds_extra(lower))
        def _():
            extra_copy(0, lower).start()
        @pl.when(feeds(lower, lower + 3))
        def _():
            y_copy(0, lower, 3).start()
        last = jnp.dot(y_low.astype(bf16), v_last[...], preferred_element_type=f32).astype(bf16)
        reduced = solved[1].astype(bf16)
        result[1] = (
            jnp.concatenate([times_upper(reduced, 1, right) for right in range(width // TILE)], axis=1)
            - held[1]
            - jnp.dot(last, folded2[pl.ds(2 * rank_max, rank_max), :], preferred_element_type=f32)
        )
        @pl.when(feeds_extra(upper_row))
        def _():
            extra_copy(1, upper_row).start()
        send_y(1, upper_row)
        send_y(0, lower, without=3)
        send_final(1, upper_row)
        send_final(0, lower)

    @pl.when(double)
    def _():
        v_copy().wait_recv()
        v_pair[:, pl.ds(0, rank_max)] = transposed(v_near[...])
        v_pair[:, pl.ds(rank_max, rank_max)] = transposed(v_ref[...])
        u_copy().wait_recv()
        folded[pl.ds(0, rank_max), :] = u_near[...].astype(bf16)
        y_copy(0, mine, 0).wait_recv()
        inner = jnp.dot(arrived[...].astype(bf16), v_pair[...], preferred_element_type=f32).astype(bf16)
        low_part[...] = jnp.dot(inner[:, :rank_max], folded[pl.ds(0, rank_max), :], preferred_element_type=f32)
        own_part[...] = jnp.dot(inner[:, rank_max:], u16[...], preferred_element_type=f32)
        low_part_copy(col).start()
        part_copy(col, 1).start()

    @pl.when(is_worker)
    def _():
        y_copy(0, mine, 0).wait_recv()
        inner = inner_of(arrived[...], v_ref[...])
        @pl.when(second)
        def _():
            own_inner[...] = inner
            inner_copy().start()
        @pl.when(sends_part)
        def _():
            own_part[...] = jnp.dot(inner.astype(bf16), u16[...], preferred_element_type=f32)
            part_copy(col, parity).start()

    @pl.when(pair)
    def _():
        finish(result[1], logs_all[1])
    @pl.when(in_row & jnp.logical_not(pair))
    def _():
        finish(result[0], logs_all[0])
    @pl.when(jnp.logical_not(in_row))
    def _():
        logs_copy(0, mine, 0).wait_recv()
        final_copy(0, mine, 0).wait_recv()
        finish(final[...], logs_in[...])

    for owner in range(n):
        @pl.when((col == owner) & jnp.logical_not(first_row | in_row | takes_detour))
        def _():
            block_copy(owner, parity).wait_send()
    @pl.when(takes_detour)
    def _():
        detour_copy().wait_send()
    for owner, third, condition in detours:
        @pl.when(condition & (col == third))
        def _():
            detour_onward(owner).wait_send()
    @pl.when(moved)
    def _():
        rs_copy().wait_send()
        v_copy().wait_send()
        u_copy().wait_send()
    @pl.when(lent)
    def _():
        v_copy().wait_send()
        u_copy().wait_send()
    @pl.when(double)
    def _():
        low_part_copy(col).wait_send()
        part_copy(col, 1).wait_send()
    @pl.when(second)
    def _():
        second_copy().wait_send()
        inner_copy().wait_send()
    @pl.when(by_relay)
    def _():
        for which in range(2):
            relay_copy(which).wait_send()
    @pl.when(is_relay)
    def _():
        for which in range(2):
            onward_copy(which, onto_slot).wait_send()
    @pl.when(jnp.logical_not(in_row))
    def _():
        log_copy(col, parity).wait_send()
    @pl.when(sends_part | (first_row & jnp.logical_not(in_row)))
    def _():
        part_copy(col, parity).wait_send()
    for slot, source, active in served:
        @pl.when(active)
        def _():
            @pl.when(feeds_extra(source))
            def _():
                extra_copy(slot, source).wait_send()
            for step in range(1, n):
                @pl.when(feeds(source, source + step))
                def _():
                    y_copy(slot, source, step).wait_send()
            for target, other in others(source):
                @pl.when(other)
                def _():
                    final_copy(slot, source, target).wait_send()
                    logs_copy(slot, source, target).wait_send()


def outputs(y_ref, log_ref, white_ref, lik_ref):
    y = y_ref[...]
    nrhs, width = y.shape
    lik = -0.5 * jnp.sum(y * y, axis=1, keepdims=True) * (1.0 / width) + log_ref[0:1, 0:1] - 0.5 * math.log(2.0 * math.pi)
    diagonal = lax.broadcasted_iota(jnp.int32, (nrhs, nrhs), 0) == lax.broadcasted_iota(jnp.int32, (nrhs, nrhs), 1)
    lik_ref[...] = jnp.sum(jnp.where(diagonal, lik, 0.0), axis=0, keepdims=True)
    white_ref[...] = y


def local(n, right_side, inverse_t, u_factor, v_factor, ranks):
    nrhs, width = right_side.shape[2:]
    piece = inverse_t.shape[2]
    rank_max = u_factor.shape[4]
    f32, bf16 = jnp.float32, jnp.bfloat16
    vmem = pl.BlockSpec(memory_space=pltpu.VMEM)
    dma = pltpu.SemaphoreType.DMA
    rows = pltpu.VMEM((nrhs, width), f32)
    two_rows = pltpu.VMEM((2, nrhs, width), f32)
    small = pltpu.VMEM((8, LANES), f32)
    factor32 = pltpu.VMEM((rank_max, width), f32)
    factor16 = pltpu.VMEM((rank_max, width), bf16)
    inner = pltpu.VMEM((nrhs, rank_max), f32)
    y, log_mean = pl.pallas_call(
        functools.partial(kernel, n),
        out_shape=(jax.ShapeDtypeStruct((nrhs, width), f32), jax.ShapeDtypeStruct((8, LANES), f32)),
        in_specs=[vmem, vmem, vmem, vmem, pl.BlockSpec(memory_space=pltpu.SMEM)],
        out_specs=(vmem, vmem),
        scratch_shapes=[
            pltpu.VMEM((piece, width), f32),
            pltpu.VMEM((piece, width), f32),
            pltpu.VMEM((2, width, width), f32),
            pltpu.VMEM((2, width, width), bf16),
            factor32,
            factor32,
            factor16,
            factor32,
            factor32,
            pltpu.VMEM((width, 2 * rank_max), bf16),
            pltpu.VMEM((width, 2 * rank_max), bf16),
            pltpu.VMEM((width, rank_max), bf16),
            pltpu.VMEM((5 * rank_max, width), bf16),
            pltpu.VMEM((5 * rank_max, width), f32),
            factor32,
            rows,
            pltpu.VMEM((3, 2, rank_max, width), f32),
            pltpu.VMEM((2, rank_max, width), f32),
            pltpu.VMEM((2 * rank_max, width), bf16),
            pltpu.VMEM((3 * rank_max, width), bf16),
            pltpu.VMEM((max(piece, LANES), width), bf16),
            pltpu.VMEM((rank_max + 16, width), bf16),
            pltpu.VMEM((rank_max + 16, width), f32),
            rows,
            rows,
            rows,
            rows,
            pltpu.VMEM((2, n, nrhs, width), f32),
            inner,
            inner,
            two_rows,
            two_rows,
            two_rows,
            rows,
            small,
            pltpu.VMEM((2, n, 8, LANES), f32),
            pltpu.VMEM((2, 8, LANES), f32),
            small,
            dma, dma((2, n)), dma((4,)), dma((4,)), dma, dma, dma((2, n)), dma, dma((2,)), dma,
            dma((2,)), dma((2, n)), dma((2, n)), dma, dma, dma((2, n)), dma((2, n)), dma,
            dma((2,)), dma((2,)), dma((2,)), dma((3, 2)), dma, dma,
        ],
        compiler_params=pltpu.CompilerParams(collective_id=0, has_side_effects=True),
    )(
        right_side.reshape(nrhs, width),
        inverse_t.reshape(piece, width),
        u_factor.reshape(rank_max, width),
        v_factor.reshape(rank_max, width),
        ranks.reshape(1, 1),
    )
    white, lik = pl.pallas_call(
        outputs,
        out_shape=(jax.ShapeDtypeStruct((nrhs, width), f32), jax.ShapeDtypeStruct((1, nrhs), f32)),
        in_specs=[vmem, vmem],
        out_specs=(vmem, vmem),
    )(y, log_mean)
    return white.reshape(1, 1, nrhs, width), lik.reshape(1, 1, nrhs)


def solution(mesh):
    return jax.shard_map(
        functools.partial(local, mesh.shape["row"]),
        mesh=mesh,
        in_specs=(
            P(None, "row", None, None),
            P(None, "row", "col", None),
            P(None, "row", None, "col", None, None),
            P(None, "row", None, "col", None, None),
            P(None, "row", None, "col"),
        ),
        out_specs=(P(None, "row", None, None), P(None, "row", None)),
        check_vma=False,
    )
```

```python
import functools
import math

import jax
import jax.numpy as jnp
from jax import lax
from jax.experimental import pallas as pl
from jax.experimental.pallas import tpu as pltpu
from jax.sharding import PartitionSpec as P

MESH = pl.DeviceIdType.MESH
LANES = 128
TILE = 256
SECOND = 4


def first_pair(n):
    return 6 if n == 16 else 2


def lean(base, n):
    return 2 - lax.rem(base // 2, 2) if n == 16 else LEAN


LEAN = 1


def solver_of(row, n):
    parity = lax.rem(row, 2)
    base = row - parity
    paired = row >= first_pair(n)
    return (jnp.where((parity == 0) & (row > 0), row + 1, row),
            jnp.where(paired, base - lean(base, n), jnp.maximum(row - 1, 0)))


def kernel(n, rs_ref, inv_ref, u_ref, v_ref, rank_ref, white_ref, lik_ref,
           block, block_in, whole, whole16, u32, v32, u16, u_near, v_near, v_pair, v_pair2, v_last, factors, sums, u_second, rs_near,
           tiles, relay, folded, folded2, padded, lhs, products,
           arrived, arrived2, own_part, low_part, parts, own_inner, inner_second, held, solved, result, final,
           logs, logs_parts, logs_all, logs_in,
           block_send, block_recv, tile_send, tile_recv, inner_send, inner_recv, y_send, y_recv, extra_send, extra_recv,
           part_send, part_recv, final_send, final_recv, log_send, log_recv, logs_send, logs_recv,
           relay_send, relay_recv, tiles_send, tiles_recv, detour_send, detour_recv):
    row = lax.axis_index("row")
    col = lax.axis_index("col")
    piece, width = inv_ref.shape
    rank_max = u_ref.shape[0]
    nrhs = rs_ref.shape[0]
    f32, bf16 = jnp.float32, jnp.bfloat16
    start_pairs = first_pair(n)
    shift = 4 if n == 16 else LEAN + 1

    parity = lax.rem(row, 2)
    odd = parity == 1
    paired = row >= start_pairs
    single = jnp.logical_not(paired)
    pair_row = row - parity
    own_col = pair_row - lean(pair_row, n)
    other_col = pair_row - 3 + lean(pair_row, n)
    pair = odd & (col == own_col) & paired
    for_odd = odd & (col == row - 1) & single
    for_even = odd & (col == row - 2) & single
    for_first = (row == 0) & (col == 0)
    is_single = for_odd | for_even | for_first
    is_solver = is_single | pair
    mine = jnp.where(for_even | pair, row - 1, row)
    kind = lax.rem(mine, 2)
    served = ((0, mine, is_solver), (1, row, pair))
    solver = solver_of(row, n)
    in_row = for_odd | for_first | pair
    first_row = row == 0
    near = col == row - 1
    moved = jnp.where(paired, col == own_col, near) & jnp.logical_not(odd)
    second = (col == row - 2) & (row >= SECOND) & single
    by_x = paired & odd & near
    by_up = paired & jnp.logical_not(odd) & (col == other_col)
    by_down = paired & odd & (col == other_col)
    by_relay = by_x | by_up | by_down
    far = paired & (col <= pair_row - 3)
    lent = far & jnp.logical_not(odd)
    double = far & odd
    takes_y = jnp.where(paired, double | pair, (col < row) & jnp.logical_not(moved))
    sends_part = single & ((col < row - 2) | ((col == row - 2) & (row < SECOND)))
    is_worker = takes_y & single & jnp.logical_not(is_solver)
    west_row, west_col = (row, lax.rem(own_col + n - shift, n)) if n == 16 else (row - 2, own_col)
    def goes_up(base):
        return (lean(base, n) == 2) | (base > start_pairs)

    z_row = jnp.where(goes_up(pair_row), lax.rem(row + 2, n), row - 2)
    relay_row = jnp.where(by_x, row, jnp.where(by_up, z_row, west_row))
    relay_col = jnp.where(by_x, lax.rem(own_col + shift, n), jnp.where(by_up, own_col, west_col))
    x_relay = paired & odd & (col == lax.rem(own_col + shift, n))
    below_row, above_row = lax.rem(row + n - 2, n), row + 2
    from_below = (below_row >= start_pairs) & goes_up(below_row) & (col == below_row - lean(below_row, n))
    from_above = (
        (above_row < n) & (above_row >= start_pairs) & jnp.logical_not(goes_up(above_row)) & (col == above_row - 1)
    )
    up_relay = jnp.logical_not(odd) & (from_below | from_above)
    up_row = jnp.where(from_below, below_row, above_row)
    if n == 16:
        west_relay = paired & odd & (col == west_col)
        west_from = row
    else:
        west_relay = odd & (row + 2 > start_pairs) & (row + 2 < n) & (col == row + 1 - lean(row + 1, n))
        west_from = row + 2
    is_relay = x_relay | up_relay | west_relay
    from_row = jnp.where(x_relay, row, jnp.where(up_relay, up_row, west_from))
    from_col = jnp.where(
        x_relay, row - 1,
        jnp.where(up_relay, up_row - 3 + lean(up_row, n), west_from - 4 + lean(west_from - 1, n))
    )
    onto_slot = jnp.where(x_relay, 0, jnp.where(up_relay, 1, 2))

    even_out = paired & (lean(pair_row, n) == 2)
    if n == 16:
        detours = [
            (6, 4, 0, row == 1), (7, 4, 1, row == 1),
            (4, 5, 0, row == 2), (6, 5, 1, row == 2),
            (4, 6, 0, row == 3), (5, 6, 1, row == 3),
            (0, 3, 0, even_out), (4, 7, 0, even_out),
            (7, 4, 0, pair_row == start_pairs),
        ]
    else:
        detours = [(2, 1, 0, row == 1), (3, 1, 1, row == 1)]
    takes_detour, detour_col, detour_slot = False, 0, 0
    for owner, third, slot, condition in detours:
        takes = condition & (col == owner)
        takes_detour = takes_detour | takes
        detour_col = jnp.where(takes, third, detour_col)
        detour_slot = jnp.where(takes, slot, detour_slot)

    def feeds(source, target):
        base = target - lax.rem(target, 2)
        early = jnp.logical_not((target == source + 1) & (lax.rem(target, 2) == 0))
        late = ((source <= base - 3) | (source == base - lean(base, n))) & (lax.rem(target, 2) == 1)
        return (target > source) & (target < n) & jnp.where(target >= start_pairs, late, early)

    def next_base(source):
        return source + 2 - lax.rem(source, 2)

    def feeds_extra(source):
        base = next_base(source)
        return (base >= start_pairs) & (base < n) & (source != base - lean(base, n))

    def extra_target(source):
        base = next_base(source)
        return base + 1, base - lean(base, n)

    barrier = pltpu.get_barrier_semaphore()

    def greet(condition, device):
        @pl.when(condition)
        def _():
            pl.semaphore_signal(barrier, inc=1, device_id=device, device_id_type=MESH)
        return condition.astype(jnp.int32)

    waits = 0
    for slot, source, active in served:
        @pl.when(active)
        def _():
            for step in range(n):
                greet(jnp.logical_not((source == row) & (col == step)), (source, step))
            for step in range(1, n):
                greet(feeds(source, source + step), (source + step, source))
            greet(feeds_extra(source), extra_target(source))
        met = n - (source == row).astype(jnp.int32) + feeds_extra(source).astype(jnp.int32)
        for step in range(1, n):
            met = met + feeds(source, source + step).astype(jnp.int32)
        waits = waits + jnp.where(active, met, 0)
    waits = waits + greet(jnp.logical_not(in_row), solver)
    waits = waits + greet(takes_y, solver_of(col, n))
    greet(takes_detour, (row, detour_col))
    waits = waits + takes_detour.astype(jnp.int32)
    for owner, third, slot, condition in detours:
        waits = waits + greet(condition & (col == third), (row, owner))

    @pl.when(paired)
    def _():
        greet(pair, solver_of(other_col, n))
        greet(by_relay, (relay_row, relay_col))
        greet(lent, (row + 1, col))
        greet(double, (row - 1, col))
        greet(pair, (row, lax.rem(own_col + shift, n)))
        greet(pair, (jnp.where(goes_up(pair_row), lax.rem(row + 1, n), row - 3), col))
        greet(pair, (west_row, west_col))
    @pl.when(is_relay)
    def _():
        greet(is_relay, (from_row, from_col))
        greet(is_relay, solver_of(from_row, n))
    for count, condition in ((4, pair), (1, by_relay), (1, lent), (1, double), (2, is_relay)):
        waits = waits + jnp.where(condition, count, 0)

    block[...] = inv_ref[...].astype(f32)
    keep = lax.broadcasted_iota(jnp.int32, u_ref.shape, 0) < rank_ref[0, 0]
    u32[...] = jnp.where(keep, u_ref[...].astype(f32), 0.0)
    u16[...] = u32[...].astype(bf16)
    @pl.when(moved | by_relay | lent)
    def _():
        v32[...] = v_ref[...].astype(f32)

    span = max(piece, LANES)
    base = pl.multiple_of(col * piece // span * span, span)
    offset = col * piece - base
    @pl.when(first_row)
    def _():
        padded[...] = jnp.zeros(padded.shape, bf16)
        padded[pl.ds(pl.multiple_of(offset, piece), piece), :] = inv_ref[...]
        own_part[...] = jnp.dot(rs_ref[:, pl.ds(base, span)].astype(bf16), padded[...], preferred_element_type=f32)

    log_base = pl.multiple_of(col * piece // LANES * LANES, LANES)
    total = jnp.zeros((1, LANES), f32)
    for start in range(0, piece, LANES):
        height = min(LANES, piece - start)
        square = block[pl.ds(start, height), pl.ds(log_base + start, LANES)]
        rows_at = lax.broadcasted_iota(jnp.int32, square.shape, 0) + (col * piece - log_base)
        on_diagonal = rows_at == lax.broadcasted_iota(jnp.int32, square.shape, 1)
        total = total + jnp.sum(jnp.log(jnp.where(on_diagonal, square, 1.0)), axis=0, keepdims=True)
    own_log = jnp.sum(total, axis=1, keepdims=True) * (1.0 / width)
    logs[...] = jnp.broadcast_to(own_log, logs.shape)

    @pl.when(is_solver)
    def _():
        for half in range(2):
            for tile in range(width // TILE):
                whole16[half, pl.ds(tile * TILE + LANES, LANES), pl.ds(tile * TILE, LANES)] = jnp.zeros(
                    (LANES, LANES), bf16
                )

    pl.semaphore_wait(barrier, waits)

    def block_first(owner):
        return owner * piece // LANES * LANES

    def remote(source, target, send, recv, device):
        return pltpu.make_async_remote_copy(
            src_ref=source, dst_ref=target, send_sem=send, recv_sem=recv, device_id=device, device_id_type=MESH
        )

    def block_copy(owner, half):
        first = block_first(owner)
        return remote(
            block.at[:, pl.ds(first, width - first)],
            whole.at[half, pl.ds(owner * piece, piece), pl.ds(first, width - first)],
            block_send, block_recv.at[half, owner], solver,
        )

    tile_device = (jnp.where(lent, row + 1, solver[0]), jnp.where(lent, col, solver[1]))

    def detour_copy(slot):
        return remote(block, block_in.at[slot], block_send, detour_recv.at[slot], (row, detour_col))

    def detour_onward(owner, slot):
        first = block_first(owner)
        return remote(
            block_in.at[slot, :, pl.ds(first, width - first)],
            whole.at[parity, pl.ds(owner * piece, piece), pl.ds(first, width - first)],
            detour_send.at[slot], block_recv.at[parity, owner], solver,
        )

    def u_copy():
        return remote(u32, u_near, tile_send.at[0], tile_recv.at[0], tile_device)

    def v_copy():
        return remote(v32, v_near, tile_send.at[1], tile_recv.at[1], tile_device)

    def rs_copy():
        return remote(rs_ref, rs_near, tile_send.at[2], tile_recv.at[2], solver)

    def second_copy():
        return remote(u32, u_second, tile_send.at[3], tile_recv.at[3], solver)

    def relay_copy(which):
        return remote(
            (u32, v32)[which], relay.at[which], relay_send.at[which], relay_recv.at[which], (relay_row, relay_col)
        )

    def onward_copy(which, slot):
        return remote(
            relay.at[which], tiles.at[slot, which], tiles_send.at[which], tiles_recv.at[slot, which],
            solver_of(from_row, n),
        )

    def inner_copy():
        return remote(own_inner, inner_second, inner_send, inner_recv, solver)

    def y_copy(slot, source, step):
        return remote(result.at[slot], arrived, y_send.at[slot, step], y_recv, (source + step, source))

    def extra_copy(slot, source):
        return remote(result.at[slot], arrived2, extra_send.at[slot], extra_recv, extra_target(source))

    def part_copy(owner, half):
        return remote(own_part, parts.at[half, owner], part_send.at[0], part_recv.at[half, owner], solver)

    def low_part_copy(owner):
        return remote(low_part, parts.at[0, owner], part_send.at[1], part_recv.at[0, owner], solver)

    def log_copy(owner, half):
        return remote(logs, logs_parts.at[half, owner], log_send, log_recv.at[half, owner], solver)

    def final_copy(slot, source, target):
        return remote(result.at[slot], final, final_send.at[slot, target], final_recv, (source, target))

    def logs_copy(slot, source, target):
        return remote(logs_all.at[slot], logs_in, logs_send.at[slot, target], logs_recv, (source, target))

    def inner_of(y, v):
        return lax.dot_general(y.astype(bf16), v, (((1,), (1,)), ((), ())), preferred_element_type=f32)

    def finish(y, log_mean):
        lik_ref[...] = log_mean
        white_ref[...] = y

    def update(inner, depth):
        result[0] = solved[0] - jnp.dot(inner, folded[pl.ds(0, depth), :], preferred_element_type=f32)

    def others(source):
        for target in range(n):
            yield target, jnp.logical_not((source == row) & (col == target))

    def share_logs(slot, source, half):
        logs_all[slot] = jnp.where(source == row, logs[...], 0.0)
        for owner, other in others(source):
            @pl.when(other)
            def _():
                log_copy(owner, half).wait_recv()
                logs_all[slot] = logs_all[slot] + logs_parts[half, owner]
        for target, other in others(source):
            @pl.when(other)
            def _():
                logs_copy(slot, source, target).start()

    def upper(half, left, right):
        return whole16[half, pl.ds(left * TILE, TILE), pl.ds(right * TILE, TILE)]

    def times_upper(lhs, half, right):
        value = jnp.zeros((lhs.shape[0], TILE), f32)
        for left in range(right + 1):
            value = value + jnp.dot(
                lhs[:, left * TILE:(left + 1) * TILE], upper(half, left, right), preferred_element_type=f32
            )
        return value

    def fold(factor, half, into, at):
        for right in range(width // TILE):
            into[pl.ds(at, rank_max), pl.ds(right * TILE, TILE)] = times_upper(factor, half, right).astype(bf16)

    def solve_far(slot, source, half, right_side, needed):
        solved[slot] = right_side
        for owner in range(n - 2):
            @pl.when(needed(owner))
            def _():
                part_copy(owner, half).wait_recv()
                solved[slot] = solved[slot] - parts[half, owner]
        reduced = solved[slot].astype(bf16)
        for right in range(width // TILE):
            solved[slot, :, pl.ds(right * TILE, TILE)] = times_upper(reduced, half, right)

    def take_block(owner, half, own):
        first = block_first(owner)
        rows = pl.ds(owner * piece, piece)
        columns = pl.ds(first, width - first)
        @pl.when(jnp.logical_not(own & (col == owner)))
        def _():
            block_copy(owner, half).wait_recv()
            whole16[half, rows, columns] = whole[half, rows, columns].astype(bf16)
        @pl.when(own & (col == owner))
        def _():
            whole16[half, rows, columns] = inv_ref[:, columns]

    def onward_copy_in(slot, which):
        return remote(relay.at[which], tiles.at[slot, which], tiles_send.at[which], tiles_recv.at[slot, which], solver)

    def send_y(slot, source, without=0):
        for step in range(1, n):
            if step == without:
                continue
            @pl.when(feeds(source, source + step))
            def _():
                y_copy(slot, source, step).start()

    def send_final(slot, source):
        for target, other in others(source):
            @pl.when(other)
            def _():
                final_copy(slot, source, target).start()

    def transposed(value):
        return value.astype(f32).T.astype(bf16)

    @pl.when(first_row & jnp.logical_not(in_row))
    def _():
        part_copy(col, parity).start()
    for owner in range(n):
        @pl.when((col == owner) & jnp.logical_not(first_row | in_row | takes_detour))
        def _():
            block_copy(owner, parity).start()
    @pl.when(takes_detour)
    def _():
        detour_copy(detour_slot).start()
    @pl.when(by_relay)
    def _():
        for which in range(2):
            relay_copy(which).start()
    @pl.when(moved)
    def _():
        rs_copy().start()
        v_copy().start()
        u_copy().start()
    @pl.when(lent)
    def _():
        v_copy().start()
        u_copy().start()
    @pl.when(second)
    def _():
        second_copy().start()
    @pl.when(jnp.logical_not(in_row))
    def _():
        log_copy(col, parity).start()
    for owner, third, slot, condition in detours:
        @pl.when(condition & (col == third))
        def _():
            detour_copy(slot).wait_recv()
            detour_onward(owner, slot).start()
    @pl.when(is_relay)
    def _():
        for which in range(2):
            relay_copy(which).wait_recv()
            onward_copy(which, onto_slot).start()

    @pl.when(is_single)
    def _():
        @pl.when(for_first)
        def _():
            y = own_part[...]
            for owner in range(1, n):
                part_copy(owner, 0).wait_recv()
                y = y + parts[0, owner]
            result[0] = y

        @pl.when(jnp.logical_not(for_first))
        def _():
            @pl.when(for_even)
            def _():
                rs_copy().wait_recv()
                v_copy().wait_recv()
                u_copy().wait_recv()
                u16[...] = u_near[...].astype(bf16)
                v_pair[:, pl.ds(0, rank_max)] = transposed(v_near[...])
                v_pair[:, pl.ds(rank_max, rank_max)] = transposed(v_ref[...])
            @pl.when(for_odd)
            def _():
                rs_near[...] = rs_ref[...]
                v_pair[:, pl.ds(0, rank_max)] = transposed(v_ref[...])
            lhs[pl.ds(0, rank_max), :] = u16[...]
            lhs[pl.ds(rank_max, 16), :] = jnp.concatenate([rs_near[...]] * (16 // nrhs), axis=0).astype(bf16)
            for left in range(width // TILE):
                for owner in range(left * TILE // piece, (left + 1) * TILE // piece):
                    take_block(owner, kind, in_row)
                for right in range(left, width // TILE):
                    value = jnp.dot(lhs[:, pl.ds(left * TILE, TILE)], upper(kind, left, right), preferred_element_type=f32)
                    columns = pl.ds(right * TILE, TILE)
                    if left:
                        value = value + products[:, columns]
                    products[:, columns] = value
            folded[pl.ds(0, rank_max), :] = products[pl.ds(0, rank_max), :].astype(bf16)
            @pl.when(mine >= SECOND)
            def _():
                second_copy().wait_recv()
                u16[...] = u_second[...].astype(bf16)
                fold(u16, kind, folded, rank_max)

            @pl.when(mine == 1)
            def _():
                solved[0] = products[pl.ds(rank_max, nrhs), :]
            @pl.when(mine > 1)
            def _():
                share_logs(0, mine, kind)
                solve_far(0, mine, kind, rs_near[...],
                          lambda owner: (owner < mine - 2) | ((owner < mine - 1) & (mine < SECOND)))

            two = mine >= SECOND
            @pl.when(for_odd & jnp.logical_not(two))
            def _():
                y_copy(0, mine, 0).wait_recv()
                inner = jnp.dot(arrived[...].astype(bf16), v_pair[:, pl.ds(0, rank_max)], preferred_element_type=f32)
                update(inner.astype(bf16), rank_max)
            @pl.when(for_even & jnp.logical_not(two))
            def _():
                y_copy(0, mine, 0).wait_recv()
                inner = jnp.dot(arrived[...].astype(bf16), v_pair[...], preferred_element_type=f32)
                own_inner[...] = inner[:, rank_max:]
                update(inner[:, :rank_max].astype(bf16), rank_max)
            @pl.when(for_odd & two)
            def _():
                y_copy(0, mine, 0).wait_recv()
                inner_copy().wait_recv()
                inner = jnp.dot(arrived[...].astype(bf16), v_pair[:, pl.ds(0, rank_max)], preferred_element_type=f32)
                update(jnp.concatenate([inner, inner_second[...]], axis=1).astype(bf16), 2 * rank_max)
            @pl.when(for_even & two)
            def _():
                y_copy(0, mine, 0).wait_recv()
                inner = jnp.dot(arrived[...].astype(bf16), v_pair[...], preferred_element_type=f32)
                own_inner[...] = inner[:, rank_max:]
                inner_copy().start()
                inner_copy().wait_recv()
                update(jnp.concatenate([inner[:, :rank_max], inner_second[...]], axis=1).astype(bf16), 2 * rank_max)

        @pl.when(feeds_extra(mine))
        def _():
            extra_copy(0, mine).start()
        send_y(0, mine)
        send_final(0, mine)
        @pl.when(for_even & sends_part)
        def _():
            own_part[...] = jnp.dot(own_inner[...].astype(bf16), u32[...].astype(bf16), preferred_element_type=f32)
            part_copy(col, parity).start()
        @pl.when(mine <= 1)
        def _():
            share_logs(0, mine, kind)

    @pl.when(pair)
    def _():
        lower, upper_row = row - 1, row
        rs_copy().wait_recv()
        v_copy().wait_recv()
        v_pair[:, pl.ds(0, rank_max)] = transposed(v_near[...])
        v_pair[:, pl.ds(rank_max, rank_max)] = transposed(v_ref[...])
        u_copy().wait_recv()
        factors[pl.ds(0, rank_max), :] = u_near[...].astype(bf16)
        factors[pl.ds(2 * rank_max, rank_max), :] = u16[...]
        for slot in range(3):
            for which in range(2):
                onward_copy_in(slot, which).wait_recv()
        factors[pl.ds(rank_max, rank_max), :] = tiles[1, 0].astype(bf16)
        factors[pl.ds(3 * rank_max, rank_max), :] = tiles[2, 0].astype(bf16)
        factors[pl.ds(4 * rank_max, rank_max), :] = tiles[0, 0].astype(bf16)
        v_pair2[:, pl.ds(0, rank_max)] = transposed(tiles[1, 1])
        v_pair2[:, pl.ds(rank_max, rank_max)] = transposed(tiles[2, 1])
        v_last[...] = transposed(tiles[0, 1])
        for left in reversed(range(width // TILE)):
            for half, at in ((0, pl.ds(0, 2 * rank_max)), (1, pl.ds(2 * rank_max, 3 * rank_max))):
                for owner in reversed(range(left * TILE // piece, (left + 1) * TILE // piece)):
                    take_block(owner, half, half == 1)
                for right in range(left, width // TILE):
                    columns = pl.ds(right * TILE, TILE)
                    value = jnp.dot(
                        factors[at, pl.ds(left * TILE, TILE)], upper(half, left, right), preferred_element_type=f32
                    )
                    if left < right:
                        value = value + sums[at, columns]
                    if left:
                        sums[at, columns] = value
                    elif half == 0:
                        folded[:, columns] = value.astype(bf16)
                    else:
                        folded2[:, columns] = value.astype(bf16)
        share_logs(0, lower, 0)
        share_logs(1, upper_row, 1)
        solved[0] = rs_near[...]
        solved[1] = rs_ref[...]
        for owner in range(n - 2):
            @pl.when(owner <= row - 6)
            def _():
                for half in range(2):
                    part_copy(owner, half).wait_recv()
                    solved[half] = solved[half] - parts[half, owner]
        own_part_of = pl.ds(0, rank_max)
        other_part_of = pl.ds(rank_max, rank_max)

        def near_products(y, v, part, first):
            inner = jnp.dot(y.astype(bf16), v, preferred_element_type=f32).astype(bf16)
            low = jnp.dot(inner[:, :rank_max], folded[part, :], preferred_element_type=f32)
            high = jnp.dot(inner[:, rank_max:], folded2[part, :], preferred_element_type=f32)
            held[0] = low if first else held[0] + low
            held[1] = high if first else held[1] + high

        @pl.when(lean(lower, n) == 1)
        def _():
            extra_copy(0, 0).wait_recv()
            near_products(arrived2[...], v_pair2[...], other_part_of, True)
            y_copy(0, mine, 0).wait_recv()
            near_products(arrived[...], v_pair[...], own_part_of, False)
        @pl.when(lean(lower, n) == 2)
        def _():
            y_copy(0, mine, 0).wait_recv()
            near_products(arrived[...], v_pair[...], own_part_of, True)
            extra_copy(0, 0).wait_recv()
            near_products(arrived2[...], v_pair2[...], other_part_of, False)
        for owner in (row - 5, row - 4):
            @pl.when(owner >= 0)
            def _():
                for half in range(2):
                    part_copy(owner, half).wait_recv()
                    solved[half] = solved[half] - parts[half, owner]
        reduced = solved[0].astype(bf16)
        y_low = jnp.concatenate(
            [times_upper(reduced, 0, right) for right in range(width // TILE)], axis=1
        ) - held[0]
        result[0] = y_low
        @pl.when(feeds_extra(lower))
        def _():
            extra_copy(0, lower).start()
        @pl.when(feeds(lower, lower + 3))
        def _():
            y_copy(0, lower, 3).start()
        @pl.when(row == n - 1)
        def _():
            send_final(0, lower)
        last = jnp.dot(y_low.astype(bf16), v_last[...], preferred_element_type=f32).astype(bf16)
        reduced = solved[1].astype(bf16)
        result[1] = (
            jnp.concatenate([times_upper(reduced, 1, right) for right in range(width // TILE)], axis=1)
            - held[1]
            - jnp.dot(last, folded2[pl.ds(2 * rank_max, rank_max), :], preferred_element_type=f32)
        )
        @pl.when(feeds_extra(upper_row))
        def _():
            extra_copy(1, upper_row).start()
        send_y(1, upper_row)
        send_y(0, lower, without=3)
        send_final(1, upper_row)
        @pl.when(row < n - 1)
        def _():
            send_final(0, lower)

    @pl.when(double)
    def _():
        v_copy().wait_recv()
        v_pair[:, pl.ds(0, rank_max)] = transposed(v_near[...])
        v_pair[:, pl.ds(rank_max, rank_max)] = transposed(v_ref[...])
        u_copy().wait_recv()
        folded[pl.ds(0, rank_max), :] = u_near[...].astype(bf16)
        y_copy(0, mine, 0).wait_recv()
        inner = jnp.dot(arrived[...].astype(bf16), v_pair[...], preferred_element_type=f32).astype(bf16)
        low_part[...] = jnp.dot(inner[:, :rank_max], folded[pl.ds(0, rank_max), :], preferred_element_type=f32)
        low_part_copy(col).start()
        own_part[...] = jnp.dot(inner[:, rank_max:], u16[...], preferred_element_type=f32)
        part_copy(col, 1).start()

    @pl.when(is_worker)
    def _():
        y_copy(0, mine, 0).wait_recv()
        inner = inner_of(arrived[...], v_ref[...])
        @pl.when(second)
        def _():
            own_inner[...] = inner
            inner_copy().start()
        @pl.when(sends_part)
        def _():
            own_part[...] = jnp.dot(inner.astype(bf16), u16[...], preferred_element_type=f32)
            part_copy(col, parity).start()

    @pl.when(pair)
    def _():
        finish(result[1], logs_all[1])
    @pl.when(in_row & jnp.logical_not(pair))
    def _():
        finish(result[0], logs_all[0])
    @pl.when(jnp.logical_not(in_row))
    def _():
        logs_copy(0, mine, 0).wait_recv()
        final_copy(0, mine, 0).wait_recv()
        finish(final[...], logs_in[...])

    for owner in range(n):
        @pl.when((col == owner) & jnp.logical_not(first_row | in_row | takes_detour))
        def _():
            block_copy(owner, parity).wait_send()
    @pl.when(takes_detour)
    def _():
        detour_copy(detour_slot).wait_send()
    for owner, third, slot, condition in detours:
        @pl.when(condition & (col == third))
        def _():
            detour_onward(owner, slot).wait_send()
    @pl.when(moved)
    def _():
        rs_copy().wait_send()
        v_copy().wait_send()
        u_copy().wait_send()
    @pl.when(lent)
    def _():
        v_copy().wait_send()
        u_copy().wait_send()
    @pl.when(double)
    def _():
        low_part_copy(col).wait_send()
        part_copy(col, 1).wait_send()
    @pl.when(second)
    def _():
        second_copy().wait_send()
        inner_copy().wait_send()
    @pl.when(by_relay)
    def _():
        for which in range(2):
            relay_copy(which).wait_send()
    @pl.when(is_relay)
    def _():
        for which in range(2):
            onward_copy(which, onto_slot).wait_send()
    @pl.when(jnp.logical_not(in_row))
    def _():
        log_copy(col, parity).wait_send()
    @pl.when(sends_part | (first_row & jnp.logical_not(in_row)))
    def _():
        part_copy(col, parity).wait_send()
    for slot, source, active in served:
        @pl.when(active)
        def _():
            @pl.when(feeds_extra(source))
            def _():
                extra_copy(slot, source).wait_send()
            for step in range(1, n):
                @pl.when(feeds(source, source + step))
                def _():
                    y_copy(slot, source, step).wait_send()
            for target, other in others(source):
                @pl.when(other)
                def _():
                    final_copy(slot, source, target).wait_send()
                    logs_copy(slot, source, target).wait_send()


def outputs(y_ref, log_ref, white_ref, lik_ref):
    y = y_ref[...]
    nrhs, width = y.shape
    lik = -0.5 * jnp.sum(y * y, axis=1, keepdims=True) * (1.0 / width) + log_ref[0:1, 0:1] - 0.5 * math.log(2.0 * math.pi)
    diagonal = lax.broadcasted_iota(jnp.int32, (nrhs, nrhs), 0) == lax.broadcasted_iota(jnp.int32, (nrhs, nrhs), 1)
    lik_ref[...] = jnp.sum(jnp.where(diagonal, lik, 0.0), axis=0, keepdims=True)
    white_ref[...] = y


def local(n, right_side, inverse_t, u_factor, v_factor, ranks):
    nrhs, width = right_side.shape[2:]
    piece = inverse_t.shape[2]
    rank_max = u_factor.shape[4]
    f32, bf16 = jnp.float32, jnp.bfloat16
    vmem = pl.BlockSpec(memory_space=pltpu.VMEM)
    dma = pltpu.SemaphoreType.DMA
    rows = pltpu.VMEM((nrhs, width), f32)
    two_rows = pltpu.VMEM((2, nrhs, width), f32)
    small = pltpu.VMEM((8, LANES), f32)
    factor32 = pltpu.VMEM((rank_max, width), f32)
    factor16 = pltpu.VMEM((rank_max, width), bf16)
    inner = pltpu.VMEM((nrhs, rank_max), f32)
    y, log_mean = pl.pallas_call(
        functools.partial(kernel, n),
        out_shape=(jax.ShapeDtypeStruct((nrhs, width), f32), jax.ShapeDtypeStruct((8, LANES), f32)),
        in_specs=[vmem, vmem, vmem, vmem, pl.BlockSpec(memory_space=pltpu.SMEM)],
        out_specs=(vmem, vmem),
        scratch_shapes=[
            pltpu.VMEM((piece, width), f32),
            pltpu.VMEM((3, piece, width), f32),
            pltpu.VMEM((2, width, width), f32),
            pltpu.VMEM((2, width, width), bf16),
            factor32,
            factor32,
            factor16,
            factor32,
            factor32,
            pltpu.VMEM((width, 2 * rank_max), bf16),
            pltpu.VMEM((width, 2 * rank_max), bf16),
            pltpu.VMEM((width, rank_max), bf16),
            pltpu.VMEM((5 * rank_max, width), bf16),
            pltpu.VMEM((5 * rank_max, width), f32),
            factor32,
            rows,
            pltpu.VMEM((3, 2, rank_max, width), f32),
            pltpu.VMEM((2, rank_max, width), f32),
            pltpu.VMEM((2 * rank_max, width), bf16),
            pltpu.VMEM((3 * rank_max, width), bf16),
            pltpu.VMEM((max(piece, LANES), width), bf16),
            pltpu.VMEM((rank_max + 16, width), bf16),
            pltpu.VMEM((rank_max + 16, width), f32),
            rows,
            rows,
            rows,
            rows,
            pltpu.VMEM((2, n, nrhs, width), f32),
            inner,
            inner,
            two_rows,
            two_rows,
            two_rows,
            rows,
            small,
            pltpu.VMEM((2, n, 8, LANES), f32),
            pltpu.VMEM((2, 8, LANES), f32),
            small,
            dma, dma((2, n)), dma((4,)), dma((4,)), dma, dma, dma((2, n)), dma, dma((2,)), dma,
            dma((2,)), dma((2, n)), dma((2, n)), dma, dma, dma((2, n)), dma((2, n)), dma,
            dma((2,)), dma((2,)), dma((2,)), dma((3, 2)), dma((3,)), dma((3,)),
        ],
        compiler_params=pltpu.CompilerParams(collective_id=0, has_side_effects=True),
    )(
        right_side.reshape(nrhs, width),
        inverse_t.reshape(piece, width),
        u_factor.reshape(rank_max, width),
        v_factor.reshape(rank_max, width),
        ranks.reshape(1, 1),
    )
    white, lik = pl.pallas_call(
        outputs,
        out_shape=(jax.ShapeDtypeStruct((nrhs, width), f32), jax.ShapeDtypeStruct((1, nrhs), f32)),
        in_specs=[vmem, vmem],
        out_specs=(vmem, vmem),
    )(y, log_mean)
    return white.reshape(1, 1, nrhs, width), lik.reshape(1, 1, nrhs)


def solution(mesh):
    return jax.shard_map(
        functools.partial(local, mesh.shape["row"]),
        mesh=mesh,
        in_specs=(
            P(None, "row", None, None),
            P(None, "row", "col", None),
            P(None, "row", None, "col", None, None),
            P(None, "row", None, "col", None, None),
            P(None, "row", None, "col"),
        ),
        out_specs=(P(None, "row", None, None), P(None, "row", None)),
        check_vma=False,
    )
```

```python
import functools
import math

import jax
import jax.numpy as jnp
from jax import lax
from jax.experimental import pallas as pl
from jax.experimental.pallas import tpu as pltpu
from jax.sharding import PartitionSpec as P

MESH = pl.DeviceIdType.MESH
LANES = 128
TILE = 256
SECOND = 4


def first_pair(n):
    return 6 if n == 16 else 2


def lean(base, n):
    return 2 - lax.rem(base // 2, 2) if n == 16 else LEAN


LEAN = 1


def solver_of(row, n):
    parity = lax.rem(row, 2)
    base = row - parity
    paired = row >= first_pair(n)
    return (jnp.where((parity == 0) & (row > 0), row + 1, row),
            jnp.where(paired, base - lean(base, n), jnp.maximum(row - 1, 0)))


def kernel(n, rs_ref, inv_ref, u_ref, v_ref, rank_ref, white_ref, lik_ref,
           block, block_in, whole, whole16, u32, v32, u16, u_near, v_near, v_pair, v_pair2, v_last, factors, sums, u_second, rs_near,
           tiles, relay, folded, folded2, padded, lhs, products,
           arrived, arrived2, own_part, low_part, parts, own_inner, inner_second, held, solved, result, final,
           logs, logs_parts, logs_all, logs_in,
           block_send, block_recv, tile_send, tile_recv, inner_send, inner_recv, y_send, y_recv, extra_send, extra_recv,
           part_send, part_recv, final_send, final_recv, log_send, log_recv, logs_send, logs_recv,
           relay_send, relay_recv, tiles_send, tiles_recv, detour_send, detour_recv):
    row = lax.axis_index("row")
    col = lax.axis_index("col")
    piece, width = inv_ref.shape
    rank_max = u_ref.shape[0]
    nrhs = rs_ref.shape[0]
    f32, bf16 = jnp.float32, jnp.bfloat16
    start_pairs = first_pair(n)
    shift = 4 if n == 16 else LEAN + 1

    parity = lax.rem(row, 2)
    odd = parity == 1
    paired = row >= start_pairs
    single = jnp.logical_not(paired)
    pair_row = row - parity
    own_col = pair_row - lean(pair_row, n)
    other_col = pair_row - 3 + lean(pair_row, n)
    pair = odd & (col == own_col) & paired
    for_odd = odd & (col == row - 1) & single
    for_even = odd & (col == row - 2) & single
    for_first = (row == 0) & (col == 0)
    is_single = for_odd | for_even | for_first
    is_solver = is_single | pair
    mine = jnp.where(for_even | pair, row - 1, row)
    kind = lax.rem(mine, 2)
    served = ((0, mine, is_solver), (1, row, pair))
    solver = solver_of(row, n)
    in_row = for_odd | for_first | pair
    first_row = row == 0
    near = col == row - 1
    moved = jnp.where(paired, col == own_col, near) & jnp.logical_not(odd)
    second = (col == row - 2) & (row >= SECOND) & single
    by_x = paired & odd & near
    by_up = paired & jnp.logical_not(odd) & (col == other_col)
    by_down = paired & odd & (col == other_col)
    by_relay = by_x | by_up | by_down
    far = paired & (col <= pair_row - 3)
    lent = far & jnp.logical_not(odd)
    double = far & odd
    takes_y = jnp.where(paired, double | pair, (col < row) & jnp.logical_not(moved))
    sends_part = single & ((col < row - 2) | ((col == row - 2) & (row < SECOND)))
    is_worker = takes_y & single & jnp.logical_not(is_solver)
    west_row, west_col = (row, lax.rem(own_col + n - shift, n)) if n == 16 else (row - 2, own_col)
    def goes_up(base):
        return (lean(base, n) == 2) | (base > start_pairs)

    z_row = jnp.where(goes_up(pair_row), lax.rem(row + 2, n), row - 2)
    relay_row = jnp.where(by_x, row, jnp.where(by_up, z_row, west_row))
    relay_col = jnp.where(by_x, lax.rem(own_col + shift, n), jnp.where(by_up, own_col, west_col))
    x_relay = paired & odd & (col == lax.rem(own_col + shift, n))
    below_row, above_row = lax.rem(row + n - 2, n), row + 2
    from_below = (below_row >= start_pairs) & goes_up(below_row) & (col == below_row - lean(below_row, n))
    from_above = (
        (above_row < n) & (above_row >= start_pairs) & jnp.logical_not(goes_up(above_row)) & (col == above_row - 1)
    )
    up_relay = jnp.logical_not(odd) & (from_below | from_above)
    up_row = jnp.where(from_below, below_row, above_row)
    if n == 16:
        west_relay = paired & odd & (col == west_col)
        west_from = row
    else:
        west_relay = odd & (row + 2 > start_pairs) & (row + 2 < n) & (col == row + 1 - lean(row + 1, n))
        west_from = row + 2
    is_relay = x_relay | up_relay | west_relay
    from_row = jnp.where(x_relay, row, jnp.where(up_relay, up_row, west_from))
    from_col = jnp.where(
        x_relay, row - 1,
        jnp.where(up_relay, up_row - 3 + lean(up_row, n), west_from - 4 + lean(west_from - 1, n))
    )
    onto_slot = jnp.where(x_relay, 0, jnp.where(up_relay, 1, 2))

    even_out = paired & (lean(pair_row, n) == 2)
    if n == 16:
        detours = [
            (6, 4, 0, row == 1), (7, 4, 1, row == 1),
            (4, 5, 0, row == 2), (6, 5, 1, row == 2),
            (4, 6, 0, row == 3), (5, 6, 1, row == 3),
            (0, 3, 0, even_out), (4, 7, 0, even_out),
            (7, 4, 0, pair_row == start_pairs),
        ]
    else:
        detours = [(2, 1, 0, row == 1), (3, 1, 1, row == 1)]
    takes_detour, detour_col, detour_slot = False, 0, 0
    for owner, third, slot, condition in detours:
        takes = condition & (col == owner)
        takes_detour = takes_detour | takes
        detour_col = jnp.where(takes, third, detour_col)
        detour_slot = jnp.where(takes, slot, detour_slot)

    def feeds(source, target):
        base = target - lax.rem(target, 2)
        early = jnp.logical_not((target == source + 1) & (lax.rem(target, 2) == 0))
        late = ((source <= base - 3) | (source == base - lean(base, n))) & (lax.rem(target, 2) == 1)
        return (target > source) & (target < n) & jnp.where(target >= start_pairs, late, early)

    def next_base(source):
        return source + 2 - lax.rem(source, 2)

    def feeds_extra(source):
        base = next_base(source)
        return (base >= start_pairs) & (base < n) & (source != base - lean(base, n))

    def extra_target(source):
        base = next_base(source)
        return base + 1, base - lean(base, n)

    barrier = pltpu.get_barrier_semaphore()

    def greet(condition, device):
        @pl.when(condition)
        def _():
            pl.semaphore_signal(barrier, inc=1, device_id=device, device_id_type=MESH)
        return condition.astype(jnp.int32)

    waits = 0
    for slot, source, active in served:
        @pl.when(active)
        def _():
            for step in range(n):
                greet(jnp.logical_not((source == row) & (col == step)), (source, step))
            for step in range(1, n):
                greet(feeds(source, source + step), (source + step, source))
            greet(feeds_extra(source), extra_target(source))
        met = n - (source == row).astype(jnp.int32) + feeds_extra(source).astype(jnp.int32)
        for step in range(1, n):
            met = met + feeds(source, source + step).astype(jnp.int32)
        waits = waits + jnp.where(active, met, 0)
    waits = waits + greet(jnp.logical_not(in_row), solver)
    waits = waits + greet(takes_y, solver_of(col, n))
    greet(takes_detour, (row, detour_col))
    waits = waits + takes_detour.astype(jnp.int32)
    for owner, third, slot, condition in detours:
        waits = waits + greet(condition & (col == third), (row, owner))

    @pl.when(paired)
    def _():
        greet(pair, solver_of(other_col, n))
        greet(by_relay, (relay_row, relay_col))
        greet(lent, (row + 1, col))
        greet(double, (row - 1, col))
        greet(pair, (row, lax.rem(own_col + shift, n)))
        greet(pair, (jnp.where(goes_up(pair_row), lax.rem(row + 1, n), row - 3), col))
        greet(pair, (west_row, west_col))
    @pl.when(is_relay)
    def _():
        greet(is_relay, (from_row, from_col))
        greet(is_relay, solver_of(from_row, n))
    for count, condition in ((4, pair), (1, by_relay), (1, lent), (1, double), (2, is_relay)):
        waits = waits + jnp.where(condition, count, 0)

    block[...] = inv_ref[...].astype(f32)
    keep = lax.broadcasted_iota(jnp.int32, u_ref.shape, 0) < rank_ref[0, 0]
    u32[...] = jnp.where(keep, u_ref[...].astype(f32), 0.0)
    u16[...] = u32[...].astype(bf16)
    @pl.when(moved | by_relay | lent)
    def _():
        v32[...] = v_ref[...].astype(f32)

    span = max(piece, LANES)
    base = pl.multiple_of(col * piece // span * span, span)
    offset = col * piece - base
    @pl.when(first_row)
    def _():
        padded[...] = jnp.zeros(padded.shape, bf16)
        padded[pl.ds(pl.multiple_of(offset, piece), piece), :] = inv_ref[...]
        own_part[...] = jnp.dot(rs_ref[:, pl.ds(base, span)].astype(bf16), padded[...], preferred_element_type=f32)

    log_base = pl.multiple_of(col * piece // LANES * LANES, LANES)
    total = jnp.zeros((1, LANES), f32)
    for start in range(0, piece, LANES):
        height = min(LANES, piece - start)
        square = block[pl.ds(start, height), pl.ds(log_base + start, LANES)]
        rows_at = lax.broadcasted_iota(jnp.int32, square.shape, 0) + (col * piece - log_base)
        on_diagonal = rows_at == lax.broadcasted_iota(jnp.int32, square.shape, 1)
        total = total + jnp.sum(jnp.log(jnp.where(on_diagonal, square, 1.0)), axis=0, keepdims=True)
    own_log = jnp.sum(total, axis=1, keepdims=True) * (1.0 / width)
    logs[...] = jnp.broadcast_to(own_log, logs.shape)

    @pl.when(is_solver)
    def _():
        for half in range(2):
            for tile in range(width // TILE):
                whole16[half, pl.ds(tile * TILE + LANES, LANES), pl.ds(tile * TILE, LANES)] = jnp.zeros(
                    (LANES, LANES), bf16
                )

    pl.semaphore_wait(barrier, waits)

    def block_first(owner):
        return owner * piece // LANES * LANES

    def remote(source, target, send, recv, device):
        return pltpu.make_async_remote_copy(
            src_ref=source, dst_ref=target, send_sem=send, recv_sem=recv, device_id=device, device_id_type=MESH
        )

    def block_copy(owner, half):
        first = block_first(owner)
        return remote(
            block.at[:, pl.ds(first, width - first)],
            whole.at[half, pl.ds(owner * piece, piece), pl.ds(first, width - first)],
            block_send, block_recv.at[half, owner], solver,
        )

    tile_device = (jnp.where(lent, row + 1, solver[0]), jnp.where(lent, col, solver[1]))

    def detour_copy(slot):
        return remote(block, block_in.at[slot], block_send, detour_recv.at[slot], (row, detour_col))

    def detour_onward(owner, slot):
        first = block_first(owner)
        return remote(
            block_in.at[slot, :, pl.ds(first, width - first)],
            whole.at[parity, pl.ds(owner * piece, piece), pl.ds(first, width - first)],
            detour_send.at[slot], block_recv.at[parity, owner], solver,
        )

    def u_copy():
        return remote(u32, u_near, tile_send.at[0], tile_recv.at[0], tile_device)

    def v_copy():
        return remote(v32, v_near, tile_send.at[1], tile_recv.at[1], tile_device)

    def rs_copy():
        return remote(rs_ref, rs_near, tile_send.at[2], tile_recv.at[2], solver)

    def second_copy():
        return remote(u32, u_second, tile_send.at[3], tile_recv.at[3], solver)

    def relay_copy(which):
        return remote(
            (u32, v32)[which], relay.at[which], relay_send.at[which], relay_recv.at[which], (relay_row, relay_col)
        )

    def onward_copy(which, slot):
        return remote(
            relay.at[which], tiles.at[slot, which], tiles_send.at[which], tiles_recv.at[slot, which],
            solver_of(from_row, n),
        )

    def inner_copy():
        return remote(own_inner, inner_second, inner_send, inner_recv, solver)

    def y_copy(slot, source, step):
        return remote(result.at[slot], arrived, y_send.at[slot, step], y_recv, (source + step, source))

    def extra_copy(slot, source):
        return remote(result.at[slot], arrived2, extra_send.at[slot], extra_recv, extra_target(source))

    def part_copy(owner, half):
        return remote(own_part, parts.at[half, owner], part_send.at[0], part_recv.at[half, owner], solver)

    def low_part_copy(owner):
        return remote(low_part, parts.at[0, owner], part_send.at[1], part_recv.at[0, owner], solver)

    def log_copy(owner, half):
        return remote(logs, logs_parts.at[half, owner], log_send, log_recv.at[half, owner], solver)

    def final_copy(slot, source, target):
        return remote(result.at[slot], final, final_send.at[slot, target], final_recv, (source, target))

    def logs_copy(slot, source, target):
        return remote(logs_all.at[slot], logs_in, logs_send.at[slot, target], logs_recv, (source, target))

    def inner_of(y, v):
        return lax.dot_general(y.astype(bf16), v, (((1,), (1,)), ((), ())), preferred_element_type=f32)

    def finish(y, log_mean):
        lik_ref[...] = log_mean
        white_ref[...] = y

    def update(inner, depth):
        result[0] = solved[0] - jnp.dot(inner, folded[pl.ds(0, depth), :], preferred_element_type=f32)

    def others(source):
        for target in range(n):
            yield target, jnp.logical_not((source == row) & (col == target))

    def share_logs(slot, source, half):
        logs_all[slot] = jnp.where(source == row, logs[...], 0.0)
        for owner, other in others(source):
            @pl.when(other)
            def _():
                log_copy(owner, half).wait_recv()
                logs_all[slot] = logs_all[slot] + logs_parts[half, owner]
        for target, other in others(source):
            @pl.when(other)
            def _():
                logs_copy(slot, source, target).start()

    def upper(half, left, right):
        return whole16[half, pl.ds(left * TILE, TILE), pl.ds(right * TILE, TILE)]

    def times_upper(lhs, half, right):
        value = jnp.zeros((lhs.shape[0], TILE), f32)
        for left in range(right + 1):
            value = value + jnp.dot(
                lhs[:, left * TILE:(left + 1) * TILE], upper(half, left, right), preferred_element_type=f32
            )
        return value

    def fold(factor, half, into, at):
        for right in range(width // TILE):
            into[pl.ds(at, rank_max), pl.ds(right * TILE, TILE)] = times_upper(factor, half, right).astype(bf16)

    def solve_far(slot, source, half, right_side, needed):
        solved[slot] = right_side
        for owner in range(n - 2):
            @pl.when(needed(owner))
            def _():
                part_copy(owner, half).wait_recv()
                solved[slot] = solved[slot] - parts[half, owner]
        reduced = solved[slot].astype(bf16)
        for right in range(width // TILE):
            solved[slot, :, pl.ds(right * TILE, TILE)] = times_upper(reduced, half, right)

    def take_block(owner, half, own):
        first = block_first(owner)
        rows = pl.ds(owner * piece, piece)
        columns = pl.ds(first, width - first)
        @pl.when(jnp.logical_not(own & (col == owner)))
        def _():
            block_copy(owner, half).wait_recv()
            whole16[half, rows, columns] = whole[half, rows, columns].astype(bf16)
        @pl.when(own & (col == owner))
        def _():
            whole16[half, rows, columns] = inv_ref[:, columns]

    def onward_copy_in(slot, which):
        return remote(relay.at[which], tiles.at[slot, which], tiles_send.at[which], tiles_recv.at[slot, which], solver)

    def send_y(slot, source, without=0):
        for step in range(1, n):
            if step == without:
                continue
            @pl.when(feeds(source, source + step))
            def _():
                y_copy(slot, source, step).start()

    def send_final(slot, source):
        for target, other in others(source):
            @pl.when(other)
            def _():
                final_copy(slot, source, target).start()

    def transposed(value):
        return value.astype(f32).T.astype(bf16)

    @pl.when(first_row & jnp.logical_not(in_row))
    def _():
        part_copy(col, parity).start()
    for owner in range(n):
        @pl.when((col == owner) & jnp.logical_not(first_row | in_row | takes_detour))
        def _():
            block_copy(owner, parity).start()
    @pl.when(takes_detour)
    def _():
        detour_copy(detour_slot).start()
    @pl.when(by_relay)
    def _():
        for which in range(2):
            relay_copy(which).start()
    @pl.when(moved)
    def _():
        rs_copy().start()
        v_copy().start()
        u_copy().start()
    @pl.when(lent)
    def _():
        v_copy().start()
        u_copy().start()
    @pl.when(second)
    def _():
        second_copy().start()
    @pl.when(jnp.logical_not(in_row))
    def _():
        log_copy(col, parity).start()
    for owner, third, slot, condition in detours:
        @pl.when(condition & (col == third))
        def _():
            detour_copy(slot).wait_recv()
            detour_onward(owner, slot).start()
    @pl.when(is_relay)
    def _():
        for which in range(2):
            relay_copy(which).wait_recv()
            onward_copy(which, onto_slot).start()

    @pl.when(is_single)
    def _():
        @pl.when(for_first)
        def _():
            y = own_part[...]
            for owner in range(1, n):
                part_copy(owner, 0).wait_recv()
                y = y + parts[0, owner]
            result[0] = y

        @pl.when(jnp.logical_not(for_first))
        def _():
            @pl.when(for_even)
            def _():
                rs_copy().wait_recv()
                v_copy().wait_recv()
                u_copy().wait_recv()
                u16[...] = u_near[...].astype(bf16)
                v_pair[:, pl.ds(0, rank_max)] = transposed(v_near[...])
                v_pair[:, pl.ds(rank_max, rank_max)] = transposed(v_ref[...])
            @pl.when(for_odd)
            def _():
                rs_near[...] = rs_ref[...]
                v_pair[:, pl.ds(0, rank_max)] = transposed(v_ref[...])
            lhs[pl.ds(0, rank_max), :] = u16[...]
            lhs[pl.ds(rank_max, 16), :] = jnp.concatenate([rs_near[...]] * (16 // nrhs), axis=0).astype(bf16)
            for left in range(width // TILE):
                for owner in range(left * TILE // piece, (left + 1) * TILE // piece):
                    take_block(owner, kind, in_row)
                for right in range(left, width // TILE):
                    value = jnp.dot(lhs[:, pl.ds(left * TILE, TILE)], upper(kind, left, right), preferred_element_type=f32)
                    columns = pl.ds(right * TILE, TILE)
                    if left:
                        value = value + products[:, columns]
                    products[:, columns] = value
            folded[pl.ds(0, rank_max), :] = products[pl.ds(0, rank_max), :].astype(bf16)
            @pl.when(mine >= SECOND)
            def _():
                second_copy().wait_recv()
                u16[...] = u_second[...].astype(bf16)
                fold(u16, kind, folded, rank_max)

            @pl.when(mine == 1)
            def _():
                solved[0] = products[pl.ds(rank_max, nrhs), :]
            @pl.when(mine > 1)
            def _():
                share_logs(0, mine, kind)
                solve_far(0, mine, kind, rs_near[...],
                          lambda owner: (owner < mine - 2) | ((owner < mine - 1) & (mine < SECOND)))

            two = mine >= SECOND
            @pl.when(for_odd & jnp.logical_not(two))
            def _():
                y_copy(0, mine, 0).wait_recv()
                inner = jnp.dot(arrived[...].astype(bf16), v_pair[:, pl.ds(0, rank_max)], preferred_element_type=f32)
                update(inner.astype(bf16), rank_max)
            @pl.when(for_even & jnp.logical_not(two))
            def _():
                y_copy(0, mine, 0).wait_recv()
                inner = jnp.dot(arrived[...].astype(bf16), v_pair[...], preferred_element_type=f32)
                own_inner[...] = inner[:, rank_max:]
                update(inner[:, :rank_max].astype(bf16), rank_max)
            @pl.when(for_odd & two)
            def _():
                y_copy(0, mine, 0).wait_recv()
                inner_copy().wait_recv()
                inner = jnp.dot(arrived[...].astype(bf16), v_pair[:, pl.ds(0, rank_max)], preferred_element_type=f32)
                update(jnp.concatenate([inner, inner_second[...]], axis=1).astype(bf16), 2 * rank_max)
            @pl.when(for_even & two)
            def _():
                y_copy(0, mine, 0).wait_recv()
                inner = jnp.dot(arrived[...].astype(bf16), v_pair[...], preferred_element_type=f32)
                own_inner[...] = inner[:, rank_max:]
                inner_copy().start()
                inner_copy().wait_recv()
                update(jnp.concatenate([inner[:, :rank_max], inner_second[...]], axis=1).astype(bf16), 2 * rank_max)

        @pl.when(feeds_extra(mine))
        def _():
            extra_copy(0, mine).start()
        send_y(0, mine)
        send_final(0, mine)
        @pl.when(for_even & sends_part)
        def _():
            own_part[...] = jnp.dot(own_inner[...].astype(bf16), u32[...].astype(bf16), preferred_element_type=f32)
            part_copy(col, parity).start()
        @pl.when(mine <= 1)
        def _():
            share_logs(0, mine, kind)

    @pl.when(pair)
    def _():
        lower, upper_row = row - 1, row
        rs_copy().wait_recv()
        v_copy().wait_recv()
        v_pair[:, pl.ds(0, rank_max)] = transposed(v_near[...])
        v_pair[:, pl.ds(rank_max, rank_max)] = transposed(v_ref[...])
        u_copy().wait_recv()
        factors[pl.ds(0, rank_max), :] = u_near[...].astype(bf16)
        factors[pl.ds(2 * rank_max, rank_max), :] = u16[...]
        for slot in range(3):
            for which in range(2):
                onward_copy_in(slot, which).wait_recv()
        factors[pl.ds(rank_max, rank_max), :] = tiles[1, 0].astype(bf16)
        factors[pl.ds(3 * rank_max, rank_max), :] = tiles[2, 0].astype(bf16)
        factors[pl.ds(4 * rank_max, rank_max), :] = tiles[0, 0].astype(bf16)
        v_pair2[:, pl.ds(0, rank_max)] = transposed(tiles[1, 1])
        v_pair2[:, pl.ds(rank_max, rank_max)] = transposed(tiles[2, 1])
        v_last[...] = transposed(tiles[0, 1])
        for left in reversed(range(width // TILE)):
            for half, at in ((0, pl.ds(0, 2 * rank_max)), (1, pl.ds(2 * rank_max, 3 * rank_max))):
                for owner in reversed(range(left * TILE // piece, (left + 1) * TILE // piece)):
                    take_block(owner, half, half == 1)
                for right in range(left, width // TILE):
                    columns = pl.ds(right * TILE, TILE)
                    value = jnp.dot(
                        factors[at, pl.ds(left * TILE, TILE)], upper(half, left, right), preferred_element_type=f32
                    )
                    if left < right:
                        value = value + sums[at, columns]
                    if left:
                        sums[at, columns] = value
                    elif half == 0:
                        folded[:, columns] = value.astype(bf16)
                    else:
                        folded2[:, columns] = value.astype(bf16)
        share_logs(0, lower, 0)
        share_logs(1, upper_row, 1)
        solved[0] = rs_near[...]
        solved[1] = rs_ref[...]
        for owner in range(n - 2):
            @pl.when(owner <= row - 6)
            def _():
                for half in range(2):
                    part_copy(owner, half).wait_recv()
                    solved[half] = solved[half] - parts[half, owner]
        own_part_of = pl.ds(0, rank_max)
        other_part_of = pl.ds(rank_max, rank_max)

        def near_products(y, v, part, first):
            inner = jnp.dot(y.astype(bf16), v, preferred_element_type=f32).astype(bf16)
            low = jnp.dot(inner[:, :rank_max], folded[part, :], preferred_element_type=f32)
            high = jnp.dot(inner[:, rank_max:], folded2[part, :], preferred_element_type=f32)
            held[0] = low if first else held[0] + low
            held[1] = high if first else held[1] + high

        @pl.when(lean(lower, n) == 1)
        def _():
            extra_copy(0, 0).wait_recv()
            near_products(arrived2[...], v_pair2[...], other_part_of, True)
            y_copy(0, mine, 0).wait_recv()
            near_products(arrived[...], v_pair[...], own_part_of, False)
        @pl.when(lean(lower, n) == 2)
        def _():
            y_copy(0, mine, 0).wait_recv()
            near_products(arrived[...], v_pair[...], own_part_of, True)
            extra_copy(0, 0).wait_recv()
            near_products(arrived2[...], v_pair2[...], other_part_of, False)
        def last_far(half):
            for owner in (row - 5, row - 4):
                @pl.when(owner >= 0)
                def _():
                    part_copy(owner, half).wait_recv()
                    solved[half] = solved[half] - parts[half, owner]

        last_far(0)
        reduced = solved[0].astype(bf16)
        y_low = jnp.concatenate(
            [times_upper(reduced, 0, right) for right in range(width // TILE)], axis=1
        ) - held[0]
        result[0] = y_low
        @pl.when(feeds_extra(lower))
        def _():
            extra_copy(0, lower).start()
        @pl.when(feeds(lower, lower + 3))
        def _():
            y_copy(0, lower, 3).start()
        last_far(1)
        @pl.when(row == n - 1)
        def _():
            send_final(0, lower)
        last = jnp.dot(y_low.astype(bf16), v_last[...], preferred_element_type=f32).astype(bf16)
        reduced = solved[1].astype(bf16)
        result[1] = (
            jnp.concatenate([times_upper(reduced, 1, right) for right in range(width // TILE)], axis=1)
            - held[1]
            - jnp.dot(last, folded2[pl.ds(2 * rank_max, rank_max), :], preferred_element_type=f32)
        )
        @pl.when(feeds_extra(upper_row))
        def _():
            extra_copy(1, upper_row).start()
        send_y(1, upper_row)
        send_y(0, lower, without=3)
        send_final(1, upper_row)
        @pl.when(row < n - 1)
        def _():
            send_final(0, lower)

    @pl.when(double)
    def _():
        v_copy().wait_recv()
        v_pair[:, pl.ds(0, rank_max)] = transposed(v_near[...])
        v_pair[:, pl.ds(rank_max, rank_max)] = transposed(v_ref[...])
        u_copy().wait_recv()
        folded[pl.ds(0, rank_max), :] = u_near[...].astype(bf16)
        y_copy(0, mine, 0).wait_recv()
        inner = jnp.dot(arrived[...].astype(bf16), v_pair[...], preferred_element_type=f32).astype(bf16)
        low_part[...] = jnp.dot(inner[:, :rank_max], folded[pl.ds(0, rank_max), :], preferred_element_type=f32)
        low_part_copy(col).start()
        own_part[...] = jnp.dot(inner[:, rank_max:], u16[...], preferred_element_type=f32)
        part_copy(col, 1).start()

    @pl.when(is_worker)
    def _():
        y_copy(0, mine, 0).wait_recv()
        inner = inner_of(arrived[...], v_ref[...])
        @pl.when(second)
        def _():
            own_inner[...] = inner
            inner_copy().start()
        @pl.when(sends_part)
        def _():
            own_part[...] = jnp.dot(inner.astype(bf16), u16[...], preferred_element_type=f32)
            part_copy(col, parity).start()

    @pl.when(pair)
    def _():
        finish(result[1], logs_all[1])
    @pl.when(in_row & jnp.logical_not(pair))
    def _():
        finish(result[0], logs_all[0])
    @pl.when(jnp.logical_not(in_row))
    def _():
        logs_copy(0, mine, 0).wait_recv()
        final_copy(0, mine, 0).wait_recv()
        finish(final[...], logs_in[...])

    for owner in range(n):
        @pl.when((col == owner) & jnp.logical_not(first_row | in_row | takes_detour))
        def _():
            block_copy(owner, parity).wait_send()
    @pl.when(takes_detour)
    def _():
        detour_copy(detour_slot).wait_send()
    for owner, third, slot, condition in detours:
        @pl.when(condition & (col == third))
        def _():
            detour_onward(owner, slot).wait_send()
    @pl.when(moved)
    def _():
        rs_copy().wait_send()
        v_copy().wait_send()
        u_copy().wait_send()
    @pl.when(lent)
    def _():
        v_copy().wait_send()
        u_copy().wait_send()
    @pl.when(double)
    def _():
        low_part_copy(col).wait_send()
        part_copy(col, 1).wait_send()
    @pl.when(second)
    def _():
        second_copy().wait_send()
        inner_copy().wait_send()
    @pl.when(by_relay)
    def _():
        for which in range(2):
            relay_copy(which).wait_send()
    @pl.when(is_relay)
    def _():
        for which in range(2):
            onward_copy(which, onto_slot).wait_send()
    @pl.when(jnp.logical_not(in_row))
    def _():
        log_copy(col, parity).wait_send()
    @pl.when(sends_part | (first_row & jnp.logical_not(in_row)))
    def _():
        part_copy(col, parity).wait_send()
    for slot, source, active in served:
        @pl.when(active)
        def _():
            @pl.when(feeds_extra(source))
            def _():
                extra_copy(slot, source).wait_send()
            for step in range(1, n):
                @pl.when(feeds(source, source + step))
                def _():
                    y_copy(slot, source, step).wait_send()
            for target, other in others(source):
                @pl.when(other)
                def _():
                    final_copy(slot, source, target).wait_send()
                    logs_copy(slot, source, target).wait_send()


def outputs(y_ref, log_ref, white_ref, lik_ref):
    y = y_ref[...]
    nrhs, width = y.shape
    lik = -0.5 * jnp.sum(y * y, axis=1, keepdims=True) * (1.0 / width) + log_ref[0:1, 0:1] - 0.5 * math.log(2.0 * math.pi)
    diagonal = lax.broadcasted_iota(jnp.int32, (nrhs, nrhs), 0) == lax.broadcasted_iota(jnp.int32, (nrhs, nrhs), 1)
    lik_ref[...] = jnp.sum(jnp.where(diagonal, lik, 0.0), axis=0, keepdims=True)
    white_ref[...] = y


def local(n, right_side, inverse_t, u_factor, v_factor, ranks):
    nrhs, width = right_side.shape[2:]
    piece = inverse_t.shape[2]
    rank_max = u_factor.shape[4]
    f32, bf16 = jnp.float32, jnp.bfloat16
    vmem = pl.BlockSpec(memory_space=pltpu.VMEM)
    dma = pltpu.SemaphoreType.DMA
    rows = pltpu.VMEM((nrhs, width), f32)
    two_rows = pltpu.VMEM((2, nrhs, width), f32)
    small = pltpu.VMEM((8, LANES), f32)
    factor32 = pltpu.VMEM((rank_max, width), f32)
    factor16 = pltpu.VMEM((rank_max, width), bf16)
    inner = pltpu.VMEM((nrhs, rank_max), f32)
    y, log_mean = pl.pallas_call(
        functools.partial(kernel, n),
        out_shape=(jax.ShapeDtypeStruct((nrhs, width), f32), jax.ShapeDtypeStruct((8, LANES), f32)),
        in_specs=[vmem, vmem, vmem, vmem, pl.BlockSpec(memory_space=pltpu.SMEM)],
        out_specs=(vmem, vmem),
        scratch_shapes=[
            pltpu.VMEM((piece, width), f32),
            pltpu.VMEM((3, piece, width), f32),
            pltpu.VMEM((2, width, width), f32),
            pltpu.VMEM((2, width, width), bf16),
            factor32,
            factor32,
            factor16,
            factor32,
            factor32,
            pltpu.VMEM((width, 2 * rank_max), bf16),
            pltpu.VMEM((width, 2 * rank_max), bf16),
            pltpu.VMEM((width, rank_max), bf16),
            pltpu.VMEM((5 * rank_max, width), bf16),
            pltpu.VMEM((5 * rank_max, width), f32),
            factor32,
            rows,
            pltpu.VMEM((3, 2, rank_max, width), f32),
            pltpu.VMEM((2, rank_max, width), f32),
            pltpu.VMEM((2 * rank_max, width), bf16),
            pltpu.VMEM((3 * rank_max, width), bf16),
            pltpu.VMEM((max(piece, LANES), width), bf16),
            pltpu.VMEM((rank_max + 16, width), bf16),
            pltpu.VMEM((rank_max + 16, width), f32),
            rows,
            rows,
            rows,
            rows,
            pltpu.VMEM((2, n, nrhs, width), f32),
            inner,
            inner,
            two_rows,
            two_rows,
            two_rows,
            rows,
            small,
            pltpu.VMEM((2, n, 8, LANES), f32),
            pltpu.VMEM((2, 8, LANES), f32),
            small,
            dma, dma((2, n)), dma((4,)), dma((4,)), dma, dma, dma((2, n)), dma, dma((2,)), dma,
            dma((2,)), dma((2, n)), dma((2, n)), dma, dma, dma((2, n)), dma((2, n)), dma,
            dma((2,)), dma((2,)), dma((2,)), dma((3, 2)), dma((3,)), dma((3,)),
        ],
        compiler_params=pltpu.CompilerParams(collective_id=0, has_side_effects=True),
    )(
        right_side.reshape(nrhs, width),
        inverse_t.reshape(piece, width),
        u_factor.reshape(rank_max, width),
        v_factor.reshape(rank_max, width),
        ranks.reshape(1, 1),
    )
    white, lik = pl.pallas_call(
        outputs,
        out_shape=(jax.ShapeDtypeStruct((nrhs, width), f32), jax.ShapeDtypeStruct((1, nrhs), f32)),
        in_specs=[vmem, vmem],
        out_specs=(vmem, vmem),
    )(y, log_mean)
    return white.reshape(1, 1, nrhs, width), lik.reshape(1, 1, nrhs)


def solution(mesh):
    return jax.shard_map(
        functools.partial(local, mesh.shape["row"]),
        mesh=mesh,
        in_specs=(
            P(None, "row", None, None),
            P(None, "row", "col", None),
            P(None, "row", None, "col", None, None),
            P(None, "row", None, "col", None, None),
            P(None, "row", None, "col"),
        ),
        out_specs=(P(None, "row", None, None), P(None, "row", None)),
        check_vma=False,
    )
```

```python
import functools
import math

import jax
import jax.numpy as jnp
from jax import lax
from jax.experimental import pallas as pl
from jax.experimental.pallas import tpu as pltpu
from jax.sharding import PartitionSpec as P

MESH = pl.DeviceIdType.MESH
LANES = 128
TILE = 256
SECOND = 4


def first_pair(n):
    return 6 if n == 16 else 2


def lean(base, n):
    return 2 - lax.rem(base // 2, 2) if n == 16 else LEAN


LEAN = 1


def solver_of(row, n):
    parity = lax.rem(row, 2)
    base = row - parity
    paired = row >= first_pair(n)
    return (jnp.where((parity == 0) & (row > 0), row + 1, row),
            jnp.where(paired, base - lean(base, n), jnp.maximum(row - 1, 0)))


def kernel(n, rs_ref, inv_ref, u_ref, v_ref, rank_ref, white_ref, lik_ref,
           block, block_in, whole, whole16, u32, v32, u16, u_near, v_near, v_pair, v_pair2, v_last, factors, sums, u_second, rs_near,
           tiles, relay, folded, folded2, padded, lhs, products,
           arrived, arrived2, own_part, low_part, parts, own_inner, inner_second, held, solved, result, final,
           logs, logs_parts, logs_all, logs_in,
           block_send, block_recv, tile_send, tile_recv, inner_send, inner_recv, y_send, y_recv, extra_send, extra_recv,
           part_send, part_recv, final_send, final_recv, log_send, log_recv, logs_send, logs_recv,
           relay_send, relay_recv, tiles_send, tiles_recv, detour_send, detour_recv):
    row = lax.axis_index("row")
    col = lax.axis_index("col")
    piece, width = inv_ref.shape
    rank_max = u_ref.shape[0]
    nrhs = rs_ref.shape[0]
    f32, bf16 = jnp.float32, jnp.bfloat16
    start_pairs = first_pair(n)
    shift = 4 if n == 16 else LEAN + 1

    parity = lax.rem(row, 2)
    odd = parity == 1
    paired = row >= start_pairs
    single = jnp.logical_not(paired)
    pair_row = row - parity
    own_col = pair_row - lean(pair_row, n)
    other_col = pair_row - 3 + lean(pair_row, n)
    pair = odd & (col == own_col) & paired
    for_odd = odd & (col == row - 1) & single
    for_even = odd & (col == row - 2) & single
    for_first = (row == 0) & (col == 0)
    is_single = for_odd | for_even | for_first
    is_solver = is_single | pair
    mine = jnp.where(for_even | pair, row - 1, row)
    kind = lax.rem(mine, 2)
    served = ((0, mine, is_solver), (1, row, pair))
    solver = solver_of(row, n)
    in_row = for_odd | for_first | pair
    first_row = row == 0
    near = col == row - 1
    moved = jnp.where(paired, col == own_col, near) & jnp.logical_not(odd)
    second = (col == row - 2) & (row >= SECOND) & single
    by_x = paired & odd & near
    by_up = paired & jnp.logical_not(odd) & (col == other_col)
    by_down = paired & odd & (col == other_col)
    by_relay = by_x | by_up | by_down
    far = paired & (col <= pair_row - 3)
    lent = far & jnp.logical_not(odd)
    double = far & odd
    takes_y = jnp.where(paired, double | pair, (col < row) & jnp.logical_not(moved))
    sends_part = single & ((col < row - 2) | ((col == row - 2) & (row < SECOND)))
    is_worker = takes_y & single & jnp.logical_not(is_solver)
    west_row, west_col = (row, lax.rem(own_col + n - shift, n)) if n == 16 else (row - 2, own_col)
    def goes_up(base):
        return (lean(base, n) == 2) | (base > start_pairs)

    z_row = jnp.where(goes_up(pair_row), lax.rem(row + 2, n), row - 2)
    relay_row = jnp.where(by_x, row, jnp.where(by_up, z_row, west_row))
    relay_col = jnp.where(by_x, lax.rem(own_col + shift, n), jnp.where(by_up, own_col, west_col))
    x_relay = paired & odd & (col == lax.rem(own_col + shift, n))
    below_row, above_row = lax.rem(row + n - 2, n), row + 2
    from_below = (below_row >= start_pairs) & goes_up(below_row) & (col == below_row - lean(below_row, n))
    from_above = (
        (above_row < n) & (above_row >= start_pairs) & jnp.logical_not(goes_up(above_row)) & (col == above_row - 1)
    )
    up_relay = jnp.logical_not(odd) & (from_below | from_above)
    up_row = jnp.where(from_below, below_row, above_row)
    if n == 16:
        west_relay = paired & odd & (col == west_col)
        west_from = row
    else:
        west_relay = odd & (row + 2 > start_pairs) & (row + 2 < n) & (col == row + 1 - lean(row + 1, n))
        west_from = row + 2
    is_relay = x_relay | up_relay | west_relay
    from_row = jnp.where(x_relay, row, jnp.where(up_relay, up_row, west_from))
    from_col = jnp.where(
        x_relay, row - 1,
        jnp.where(up_relay, up_row - 3 + lean(up_row, n), west_from - 4 + lean(west_from - 1, n))
    )
    onto_slot = jnp.where(x_relay, 0, jnp.where(up_relay, 1, 2))

    even_out = paired & (lean(pair_row, n) == 2)
    if n == 16:
        detours = [
            (6, 4, 0, row == 1), (7, 4, 1, row == 1),
            (4, 5, 0, row == 2), (6, 5, 1, row == 2),
            (4, 6, 0, row == 3), (5, 6, 1, row == 3),
            (0, 3, 0, even_out), (4, 7, 0, even_out),
            (7, 4, 0, pair_row == start_pairs),
        ]
    else:
        detours = [(2, 1, 0, row == 1), (3, 1, 1, row == 1)]
    takes_detour, detour_col, detour_slot = False, 0, 0
    for owner, third, slot, condition in detours:
        takes = condition & (col == owner)
        takes_detour = takes_detour | takes
        detour_col = jnp.where(takes, third, detour_col)
        detour_slot = jnp.where(takes, slot, detour_slot)

    def feeds(source, target):
        base = target - lax.rem(target, 2)
        early = jnp.logical_not((target == source + 1) & (lax.rem(target, 2) == 0))
        late = ((source <= base - 3) | (source == base - lean(base, n))) & (lax.rem(target, 2) == 1)
        return (target > source) & (target < n) & jnp.where(target >= start_pairs, late, early)

    def next_base(source):
        return source + 2 - lax.rem(source, 2)

    def feeds_extra(source):
        base = next_base(source)
        return (base >= start_pairs) & (base < n) & (source != base - lean(base, n))

    def extra_target(source):
        base = next_base(source)
        return base + 1, base - lean(base, n)

    barrier = pltpu.get_barrier_semaphore()

    def greet(condition, device):
        @pl.when(condition)
        def _():
            pl.semaphore_signal(barrier, inc=1, device_id=device, device_id_type=MESH)
        return condition.astype(jnp.int32)

    waits = 0
    for slot, source, active in served:
        @pl.when(active)
        def _():
            for step in range(n):
                greet(jnp.logical_not((source == row) & (col == step)), (source, step))
            for step in range(1, n):
                greet(feeds(source, source + step), (source + step, source))
            greet(feeds_extra(source), extra_target(source))
        met = n - (source == row).astype(jnp.int32) + feeds_extra(source).astype(jnp.int32)
        for step in range(1, n):
            met = met + feeds(source, source + step).astype(jnp.int32)
        waits = waits + jnp.where(active, met, 0)
    waits = waits + greet(jnp.logical_not(in_row), solver)
    waits = waits + greet(takes_y, solver_of(col, n))
    greet(takes_detour, (row, detour_col))
    waits = waits + takes_detour.astype(jnp.int32)
    for owner, third, slot, condition in detours:
        waits = waits + greet(condition & (col == third), (row, owner))

    @pl.when(paired)
    def _():
        greet(pair, solver_of(other_col, n))
        greet(by_relay, (relay_row, relay_col))
        greet(lent, (row + 1, col))
        greet(double, (row - 1, col))
        greet(pair, (row, lax.rem(own_col + shift, n)))
        greet(pair, (jnp.where(goes_up(pair_row), lax.rem(row + 1, n), row - 3), col))
        greet(pair, (west_row, west_col))
    @pl.when(is_relay)
    def _():
        greet(is_relay, (from_row, from_col))
        greet(is_relay, solver_of(from_row, n))
    for count, condition in ((4, pair), (1, by_relay), (1, lent), (1, double), (2, is_relay)):
        waits = waits + jnp.where(condition, count, 0)

    block[...] = inv_ref[...].astype(f32)
    keep = lax.broadcasted_iota(jnp.int32, u_ref.shape, 0) < rank_ref[0, 0]
    u32[...] = jnp.where(keep, u_ref[...].astype(f32), 0.0)
    u16[...] = u32[...].astype(bf16)
    @pl.when(moved | by_relay | lent)
    def _():
        v32[...] = v_ref[...].astype(f32)

    span = max(piece, LANES)
    base = pl.multiple_of(col * piece // span * span, span)
    offset = col * piece - base
    @pl.when(first_row)
    def _():
        padded[...] = jnp.zeros(padded.shape, bf16)
        padded[pl.ds(pl.multiple_of(offset, piece), piece), :] = inv_ref[...]
        own_part[...] = jnp.dot(rs_ref[:, pl.ds(base, span)].astype(bf16), padded[...], preferred_element_type=f32)

    log_base = pl.multiple_of(col * piece // LANES * LANES, LANES)
    total = jnp.zeros((1, LANES), f32)
    for start in range(0, piece, LANES):
        height = min(LANES, piece - start)
        square = block[pl.ds(start, height), pl.ds(log_base + start, LANES)]
        rows_at = lax.broadcasted_iota(jnp.int32, square.shape, 0) + (col * piece - log_base)
        on_diagonal = rows_at == lax.broadcasted_iota(jnp.int32, square.shape, 1)
        total = total + jnp.sum(jnp.log(jnp.where(on_diagonal, square, 1.0)), axis=0, keepdims=True)
    own_log = jnp.sum(total, axis=1, keepdims=True) * (1.0 / width)
    logs[...] = jnp.broadcast_to(own_log, logs.shape)

    @pl.when(is_solver)
    def _():
        for half in range(2):
            for tile in range(width // TILE):
                whole16[half, pl.ds(tile * TILE + LANES, LANES), pl.ds(tile * TILE, LANES)] = jnp.zeros(
                    (LANES, LANES), bf16
                )

    pl.semaphore_wait(barrier, waits)

    def block_first(owner):
        return owner * piece // LANES * LANES

    def remote(source, target, send, recv, device):
        return pltpu.make_async_remote_copy(
            src_ref=source, dst_ref=target, send_sem=send, recv_sem=recv, device_id=device, device_id_type=MESH
        )

    def block_copy(owner, half):
        first = block_first(owner)
        return remote(
            block.at[:, pl.ds(first, width - first)],
            whole.at[half, pl.ds(owner * piece, piece), pl.ds(first, width - first)],
            block_send, block_recv.at[half, owner], solver,
        )

    tile_device = (jnp.where(lent, row + 1, solver[0]), jnp.where(lent, col, solver[1]))

    def detour_copy(slot):
        return remote(block, block_in.at[slot], block_send, detour_recv.at[slot], (row, detour_col))

    def detour_onward(owner, slot):
        first = block_first(owner)
        return remote(
            block_in.at[slot, :, pl.ds(first, width - first)],
            whole.at[parity, pl.ds(owner * piece, piece), pl.ds(first, width - first)],
            detour_send.at[slot], block_recv.at[parity, owner], solver,
        )

    def u_copy():
        return remote(u32, u_near, tile_send.at[0], tile_recv.at[0], tile_device)

    def v_copy():
        return remote(v32, v_near, tile_send.at[1], tile_recv.at[1], tile_device)

    def rs_copy():
        return remote(rs_ref, rs_near, tile_send.at[2], tile_recv.at[2], solver)

    def second_copy():
        return remote(u32, u_second, tile_send.at[3], tile_recv.at[3], solver)

    def relay_copy(which):
        return remote(
            (u32, v32)[which], relay.at[which], relay_send.at[which], relay_recv.at[which], (relay_row, relay_col)
        )

    def onward_copy(which, slot):
        return remote(
            relay.at[which], tiles.at[slot, which], tiles_send.at[which], tiles_recv.at[slot, which],
            solver_of(from_row, n),
        )

    def inner_copy():
        return remote(own_inner, inner_second, inner_send, inner_recv, solver)

    def y_copy(slot, source, step):
        return remote(result.at[slot], arrived, y_send.at[slot, step], y_recv, (source + step, source))

    def extra_copy(slot, source):
        return remote(result.at[slot], arrived2, extra_send.at[slot], extra_recv, extra_target(source))

    def part_copy(owner, half):
        return remote(own_part, parts.at[half, owner], part_send.at[0], part_recv.at[half, owner], solver)

    def low_part_copy(owner):
        return remote(low_part, parts.at[0, owner], part_send.at[1], part_recv.at[0, owner], solver)

    def log_copy(owner, half):
        return remote(logs, logs_parts.at[half, owner], log_send, log_recv.at[half, owner], solver)

    def final_copy(slot, source, target):
        return remote(result.at[slot], final, final_send.at[slot, target], final_recv, (source, target))

    def logs_copy(slot, source, target):
        return remote(logs_all.at[slot], logs_in, logs_send.at[slot, target], logs_recv, (source, target))

    def inner_of(y, v):
        return lax.dot_general(y.astype(bf16), v, (((1,), (1,)), ((), ())), preferred_element_type=f32)

    def finish(y, log_mean):
        lik_ref[...] = log_mean
        white_ref[...] = y

    def update(inner, depth):
        result[0] = solved[0] - jnp.dot(inner, folded[pl.ds(0, depth), :], preferred_element_type=f32)

    def others(source):
        for target in range(n):
            yield target, jnp.logical_not((source == row) & (col == target))

    def share_logs(slot, source, half):
        logs_all[slot] = jnp.where(source == row, logs[...], 0.0)
        for owner, other in others(source):
            @pl.when(other)
            def _():
                log_copy(owner, half).wait_recv()
                logs_all[slot] = logs_all[slot] + logs_parts[half, owner]
        for target, other in others(source):
            @pl.when(other)
            def _():
                logs_copy(slot, source, target).start()

    def upper(half, left, right):
        return whole16[half, pl.ds(left * TILE, TILE), pl.ds(right * TILE, TILE)]

    def times_upper(lhs, half, right):
        value = jnp.zeros((lhs.shape[0], TILE), f32)
        for left in range(right + 1):
            value = value + jnp.dot(
                lhs[:, left * TILE:(left + 1) * TILE], upper(half, left, right), preferred_element_type=f32
            )
        return value

    def fold(factor, half, into, at):
        for right in range(width // TILE):
            into[pl.ds(at, rank_max), pl.ds(right * TILE, TILE)] = times_upper(factor, half, right).astype(bf16)

    def solve_far(slot, source, half, right_side, needed):
        solved[slot] = right_side
        for owner in range(n - 2):
            @pl.when(needed(owner))
            def _():
                part_copy(owner, half).wait_recv()
                solved[slot] = solved[slot] - parts[half, owner]
        reduced = solved[slot].astype(bf16)
        for right in range(width // TILE):
            solved[slot, :, pl.ds(right * TILE, TILE)] = times_upper(reduced, half, right)

    def take_block(owner, half, own):
        first = block_first(owner)
        rows = pl.ds(owner * piece, piece)
        columns = pl.ds(first, width - first)
        @pl.when(jnp.logical_not(own & (col == owner)))
        def _():
            block_copy(owner, half).wait_recv()
            whole16[half, rows, columns] = whole[half, rows, columns].astype(bf16)
        @pl.when(own & (col == owner))
        def _():
            whole16[half, rows, columns] = inv_ref[:, columns]

    def onward_copy_in(slot, which):
        return remote(relay.at[which], tiles.at[slot, which], tiles_send.at[which], tiles_recv.at[slot, which], solver)

    def send_y(slot, source, without=()):
        for step in range(1, n):
            if step in without:
                continue
            @pl.when(feeds(source, source + step))
            def _():
                y_copy(slot, source, step).start()

    def send_final(slot, source):
        for target, other in others(source):
            @pl.when(other)
            def _():
                final_copy(slot, source, target).start()

    def transposed(value):
        return value.astype(f32).T.astype(bf16)

    @pl.when(first_row & jnp.logical_not(in_row))
    def _():
        part_copy(col, parity).start()
    for owner in range(n):
        @pl.when((col == owner) & jnp.logical_not(first_row | in_row | takes_detour))
        def _():
            block_copy(owner, parity).start()
    @pl.when(takes_detour)
    def _():
        detour_copy(detour_slot).start()
    @pl.when(by_relay)
    def _():
        for which in range(2):
            relay_copy(which).start()
    @pl.when(moved)
    def _():
        rs_copy().start()
        v_copy().start()
        u_copy().start()
    @pl.when(lent)
    def _():
        v_copy().start()
        u_copy().start()
    @pl.when(second)
    def _():
        second_copy().start()
    @pl.when(jnp.logical_not(in_row))
    def _():
        log_copy(col, parity).start()
    for owner, third, slot, condition in detours:
        @pl.when(condition & (col == third))
        def _():
            detour_copy(slot).wait_recv()
            detour_onward(owner, slot).start()
    @pl.when(is_relay)
    def _():
        for which in range(2):
            relay_copy(which).wait_recv()
            onward_copy(which, onto_slot).start()

    @pl.when(is_single)
    def _():
        @pl.when(for_first)
        def _():
            y = own_part[...]
            for owner in range(1, n):
                part_copy(owner, 0).wait_recv()
                y = y + parts[0, owner]
            result[0] = y

        @pl.when(jnp.logical_not(for_first))
        def _():
            @pl.when(for_even)
            def _():
                rs_copy().wait_recv()
                v_copy().wait_recv()
                u_copy().wait_recv()
                u16[...] = u_near[...].astype(bf16)
                v_pair[:, pl.ds(0, rank_max)] = transposed(v_near[...])
                v_pair[:, pl.ds(rank_max, rank_max)] = transposed(v_ref[...])
            @pl.when(for_odd)
            def _():
                rs_near[...] = rs_ref[...]
                v_pair[:, pl.ds(0, rank_max)] = transposed(v_ref[...])
            lhs[pl.ds(0, rank_max), :] = u16[...]
            lhs[pl.ds(rank_max, 16), :] = jnp.concatenate([rs_near[...]] * (16 // nrhs), axis=0).astype(bf16)
            for left in range(width // TILE):
                for owner in range(left * TILE // piece, (left + 1) * TILE // piece):
                    take_block(owner, kind, in_row)
                for right in range(left, width // TILE):
                    value = jnp.dot(lhs[:, pl.ds(left * TILE, TILE)], upper(kind, left, right), preferred_element_type=f32)
                    columns = pl.ds(right * TILE, TILE)
                    if left:
                        value = value + products[:, columns]
                    products[:, columns] = value
            folded[pl.ds(0, rank_max), :] = products[pl.ds(0, rank_max), :].astype(bf16)
            @pl.when(mine >= SECOND)
            def _():
                second_copy().wait_recv()
                u16[...] = u_second[...].astype(bf16)
                fold(u16, kind, folded, rank_max)

            @pl.when(mine == 1)
            def _():
                solved[0] = products[pl.ds(rank_max, nrhs), :]
            @pl.when(mine > 1)
            def _():
                share_logs(0, mine, kind)
                solve_far(0, mine, kind, rs_near[...],
                          lambda owner: (owner < mine - 2) | ((owner < mine - 1) & (mine < SECOND)))

            two = mine >= SECOND
            @pl.when(for_odd & jnp.logical_not(two))
            def _():
                y_copy(0, mine, 0).wait_recv()
                inner = jnp.dot(arrived[...].astype(bf16), v_pair[:, pl.ds(0, rank_max)], preferred_element_type=f32)
                update(inner.astype(bf16), rank_max)
            @pl.when(for_even & jnp.logical_not(two))
            def _():
                y_copy(0, mine, 0).wait_recv()
                inner = jnp.dot(arrived[...].astype(bf16), v_pair[...], preferred_element_type=f32)
                own_inner[...] = inner[:, rank_max:]
                update(inner[:, :rank_max].astype(bf16), rank_max)
            @pl.when(for_odd & two)
            def _():
                y_copy(0, mine, 0).wait_recv()
                inner_copy().wait_recv()
                inner = jnp.dot(arrived[...].astype(bf16), v_pair[:, pl.ds(0, rank_max)], preferred_element_type=f32)
                update(jnp.concatenate([inner, inner_second[...]], axis=1).astype(bf16), 2 * rank_max)
            @pl.when(for_even & two)
            def _():
                y_copy(0, mine, 0).wait_recv()
                inner = jnp.dot(arrived[...].astype(bf16), v_pair[...], preferred_element_type=f32)
                own_inner[...] = inner[:, rank_max:]
                inner_copy().start()
                inner_copy().wait_recv()
                update(jnp.concatenate([inner[:, :rank_max], inner_second[...]], axis=1).astype(bf16), 2 * rank_max)

        @pl.when(feeds_extra(mine))
        def _():
            extra_copy(0, mine).start()
        send_y(0, mine)
        send_final(0, mine)
        @pl.when(for_even & sends_part)
        def _():
            own_part[...] = jnp.dot(own_inner[...].astype(bf16), u32[...].astype(bf16), preferred_element_type=f32)
            part_copy(col, parity).start()
        @pl.when(mine <= 1)
        def _():
            share_logs(0, mine, kind)

    @pl.when(pair)
    def _():
        lower, upper_row = row - 1, row
        rs_copy().wait_recv()
        v_copy().wait_recv()
        v_pair[:, pl.ds(0, rank_max)] = transposed(v_near[...])
        v_pair[:, pl.ds(rank_max, rank_max)] = transposed(v_ref[...])
        u_copy().wait_recv()
        factors[pl.ds(0, rank_max), :] = u_near[...].astype(bf16)
        factors[pl.ds(2 * rank_max, rank_max), :] = u16[...]
        for slot in range(3):
            for which in range(2):
                onward_copy_in(slot, which).wait_recv()
        factors[pl.ds(rank_max, rank_max), :] = tiles[1, 0].astype(bf16)
        factors[pl.ds(3 * rank_max, rank_max), :] = tiles[2, 0].astype(bf16)
        factors[pl.ds(4 * rank_max, rank_max), :] = tiles[0, 0].astype(bf16)
        v_pair2[:, pl.ds(0, rank_max)] = transposed(tiles[1, 1])
        v_pair2[:, pl.ds(rank_max, rank_max)] = transposed(tiles[2, 1])
        v_last[...] = transposed(tiles[0, 1])
        for left in reversed(range(width // TILE)):
            for half, at in ((0, pl.ds(0, 2 * rank_max)), (1, pl.ds(2 * rank_max, 3 * rank_max))):
                for owner in reversed(range(left * TILE // piece, (left + 1) * TILE // piece)):
                    take_block(owner, half, half == 1)
                for right in range(left, width // TILE):
                    columns = pl.ds(right * TILE, TILE)
                    value = jnp.dot(
                        factors[at, pl.ds(left * TILE, TILE)], upper(half, left, right), preferred_element_type=f32
                    )
                    if left < right:
                        value = value + sums[at, columns]
                    if left:
                        sums[at, columns] = value
                    elif half == 0:
                        folded[:, columns] = value.astype(bf16)
                    else:
                        folded2[:, columns] = value.astype(bf16)
        share_logs(0, lower, 0)
        share_logs(1, upper_row, 1)
        solved[0] = rs_near[...]
        solved[1] = rs_ref[...]
        for owner in range(n - 2):
            @pl.when(owner <= row - 6)
            def _():
                for half in range(2):
                    part_copy(owner, half).wait_recv()
                    solved[half] = solved[half] - parts[half, owner]
        own_part_of = pl.ds(0, rank_max)
        other_part_of = pl.ds(rank_max, rank_max)

        def near_products(y, v, part, first):
            inner = jnp.dot(y.astype(bf16), v, preferred_element_type=f32).astype(bf16)
            low = jnp.dot(inner[:, :rank_max], folded[part, :], preferred_element_type=f32)
            high = jnp.dot(inner[:, rank_max:], folded2[part, :], preferred_element_type=f32)
            held[0] = low if first else held[0] + low
            held[1] = high if first else held[1] + high

        @pl.when(lean(lower, n) == 1)
        def _():
            extra_copy(0, 0).wait_recv()
            near_products(arrived2[...], v_pair2[...], other_part_of, True)
            y_copy(0, mine, 0).wait_recv()
            near_products(arrived[...], v_pair[...], own_part_of, False)
        @pl.when(lean(lower, n) == 2)
        def _():
            y_copy(0, mine, 0).wait_recv()
            near_products(arrived[...], v_pair[...], own_part_of, True)
            extra_copy(0, 0).wait_recv()
            near_products(arrived2[...], v_pair2[...], other_part_of, False)
        def last_far(half):
            for owner in (row - 5, row - 4):
                @pl.when(owner >= 0)
                def _():
                    part_copy(owner, half).wait_recv()
                    solved[half] = solved[half] - parts[half, owner]

        last_far(0)
        reduced = solved[0].astype(bf16)
        y_low = jnp.concatenate(
            [times_upper(reduced, 0, right) for right in range(width // TILE)], axis=1
        ) - held[0]
        result[0] = y_low
        @pl.when(feeds_extra(lower))
        def _():
            extra_copy(0, lower).start()
        for step in (3, 5):
            @pl.when(feeds(lower, lower + step))
            def _():
                y_copy(0, lower, step).start()
        last_far(1)
        @pl.when(row == n - 1)
        def _():
            send_final(0, lower)
        last = jnp.dot(y_low.astype(bf16), v_last[...], preferred_element_type=f32).astype(bf16)
        reduced = solved[1].astype(bf16)
        result[1] = (
            jnp.concatenate([times_upper(reduced, 1, right) for right in range(width // TILE)], axis=1)
            - held[1]
            - jnp.dot(last, folded2[pl.ds(2 * rank_max, rank_max), :], preferred_element_type=f32)
        )
        @pl.when(feeds_extra(upper_row))
        def _():
            extra_copy(1, upper_row).start()
        send_y(1, upper_row)
        send_y(0, lower, without=(3, 5))
        send_final(1, upper_row)
        @pl.when(row < n - 1)
        def _():
            send_final(0, lower)

    @pl.when(double)
    def _():
        v_copy().wait_recv()
        v_pair[:, pl.ds(0, rank_max)] = transposed(v_near[...])
        v_pair[:, pl.ds(rank_max, rank_max)] = transposed(v_ref[...])
        u_copy().wait_recv()
        folded[pl.ds(0, rank_max), :] = u_near[...].astype(bf16)
        y_copy(0, mine, 0).wait_recv()
        inner = jnp.dot(arrived[...].astype(bf16), v_pair[...], preferred_element_type=f32).astype(bf16)
        low_part[...] = jnp.dot(inner[:, :rank_max], folded[pl.ds(0, rank_max), :], preferred_element_type=f32)
        low_part_copy(col).start()
        own_part[...] = jnp.dot(inner[:, rank_max:], u16[...], preferred_element_type=f32)
        part_copy(col, 1).start()

    @pl.when(is_worker)
    def _():
        y_copy(0, mine, 0).wait_recv()
        inner = inner_of(arrived[...], v_ref[...])
        @pl.when(second)
        def _():
            own_inner[...] = inner
            inner_copy().start()
        @pl.when(sends_part)
        def _():
            own_part[...] = jnp.dot(inner.astype(bf16), u16[...], preferred_element_type=f32)
            part_copy(col, parity).start()

    @pl.when(pair)
    def _():
        finish(result[1], logs_all[1])
    @pl.when(in_row & jnp.logical_not(pair))
    def _():
        finish(result[0], logs_all[0])
    @pl.when(jnp.logical_not(in_row))
    def _():
        logs_copy(0, mine, 0).wait_recv()
        final_copy(0, mine, 0).wait_recv()
        finish(final[...], logs_in[...])

    for owner in range(n):
        @pl.when((col == owner) & jnp.logical_not(first_row | in_row | takes_detour))
        def _():
            block_copy(owner, parity).wait_send()
    @pl.when(takes_detour)
    def _():
        detour_copy(detour_slot).wait_send()
    for owner, third, slot, condition in detours:
        @pl.when(condition & (col == third))
        def _():
            detour_onward(owner, slot).wait_send()
    @pl.when(moved)
    def _():
        rs_copy().wait_send()
        v_copy().wait_send()
        u_copy().wait_send()
    @pl.when(lent)
    def _():
        v_copy().wait_send()
        u_copy().wait_send()
    @pl.when(double)
    def _():
        low_part_copy(col).wait_send()
        part_copy(col, 1).wait_send()
    @pl.when(second)
    def _():
        second_copy().wait_send()
        inner_copy().wait_send()
    @pl.when(by_relay)
    def _():
        for which in range(2):
            relay_copy(which).wait_send()
    @pl.when(is_relay)
    def _():
        for which in range(2):
            onward_copy(which, onto_slot).wait_send()
    @pl.when(jnp.logical_not(in_row))
    def _():
        log_copy(col, parity).wait_send()
    @pl.when(sends_part | (first_row & jnp.logical_not(in_row)))
    def _():
        part_copy(col, parity).wait_send()
    for slot, source, active in served:
        @pl.when(active)
        def _():
            @pl.when(feeds_extra(source))
            def _():
                extra_copy(slot, source).wait_send()
            for step in range(1, n):
                @pl.when(feeds(source, source + step))
                def _():
                    y_copy(slot, source, step).wait_send()
            for target, other in others(source):
                @pl.when(other)
                def _():
                    final_copy(slot, source, target).wait_send()
                    logs_copy(slot, source, target).wait_send()


def outputs(y_ref, log_ref, white_ref, lik_ref):
    y = y_ref[...]
    nrhs, width = y.shape
    lik = -0.5 * jnp.sum(y * y, axis=1, keepdims=True) * (1.0 / width) + log_ref[0:1, 0:1] - 0.5 * math.log(2.0 * math.pi)
    diagonal = lax.broadcasted_iota(jnp.int32, (nrhs, nrhs), 0) == lax.broadcasted_iota(jnp.int32, (nrhs, nrhs), 1)
    lik_ref[...] = jnp.sum(jnp.where(diagonal, lik, 0.0), axis=0, keepdims=True)
    white_ref[...] = y


def local(n, right_side, inverse_t, u_factor, v_factor, ranks):
    nrhs, width = right_side.shape[2:]
    piece = inverse_t.shape[2]
    rank_max = u_factor.shape[4]
    f32, bf16 = jnp.float32, jnp.bfloat16
    vmem = pl.BlockSpec(memory_space=pltpu.VMEM)
    dma = pltpu.SemaphoreType.DMA
    rows = pltpu.VMEM((nrhs, width), f32)
    two_rows = pltpu.VMEM((2, nrhs, width), f32)
    small = pltpu.VMEM((8, LANES), f32)
    factor32 = pltpu.VMEM((rank_max, width), f32)
    factor16 = pltpu.VMEM((rank_max, width), bf16)
    inner = pltpu.VMEM((nrhs, rank_max), f32)
    y, log_mean = pl.pallas_call(
        functools.partial(kernel, n),
        out_shape=(jax.ShapeDtypeStruct((nrhs, width), f32), jax.ShapeDtypeStruct((8, LANES), f32)),
        in_specs=[vmem, vmem, vmem, vmem, pl.BlockSpec(memory_space=pltpu.SMEM)],
        out_specs=(vmem, vmem),
        scratch_shapes=[
            pltpu.VMEM((piece, width), f32),
            pltpu.VMEM((3, piece, width), f32),
            pltpu.VMEM((2, width, width), f32),
            pltpu.VMEM((2, width, width), bf16),
            factor32,
            factor32,
            factor16,
            factor32,
            factor32,
            pltpu.VMEM((width, 2 * rank_max), bf16),
            pltpu.VMEM((width, 2 * rank_max), bf16),
            pltpu.VMEM((width, rank_max), bf16),
            pltpu.VMEM((5 * rank_max, width), bf16),
            pltpu.VMEM((5 * rank_max, width), f32),
            factor32,
            rows,
            pltpu.VMEM((3, 2, rank_max, width), f32),
            pltpu.VMEM((2, rank_max, width), f32),
            pltpu.VMEM((2 * rank_max, width), bf16),
            pltpu.VMEM((3 * rank_max, width), bf16),
            pltpu.VMEM((max(piece, LANES), width), bf16),
            pltpu.VMEM((rank_max + 16, width), bf16),
            pltpu.VMEM((rank_max + 16, width), f32),
            rows,
            rows,
            rows,
            rows,
            pltpu.VMEM((2, n, nrhs, width), f32),
            inner,
            inner,
            two_rows,
            two_rows,
            two_rows,
            rows,
            small,
            pltpu.VMEM((2, n, 8, LANES), f32),
            pltpu.VMEM((2, 8, LANES), f32),
            small,
            dma, dma((2, n)), dma((4,)), dma((4,)), dma, dma, dma((2, n)), dma, dma((2,)), dma,
            dma((2,)), dma((2, n)), dma((2, n)), dma, dma, dma((2, n)), dma((2, n)), dma,
            dma((2,)), dma((2,)), dma((2,)), dma((3, 2)), dma((3,)), dma((3,)),
        ],
        compiler_params=pltpu.CompilerParams(collective_id=0, has_side_effects=True),
    )(
        right_side.reshape(nrhs, width),
        inverse_t.reshape(piece, width),
        u_factor.reshape(rank_max, width),
        v_factor.reshape(rank_max, width),
        ranks.reshape(1, 1),
    )
    white, lik = pl.pallas_call(
        outputs,
        out_shape=(jax.ShapeDtypeStruct((nrhs, width), f32), jax.ShapeDtypeStruct((1, nrhs), f32)),
        in_specs=[vmem, vmem],
        out_specs=(vmem, vmem),
    )(y, log_mean)
    return white.reshape(1, 1, nrhs, width), lik.reshape(1, 1, nrhs)


def solution(mesh):
    return jax.shard_map(
        functools.partial(local, mesh.shape["row"]),
        mesh=mesh,
        in_specs=(
            P(None, "row", None, None),
            P(None, "row", "col", None),
            P(None, "row", None, "col", None, None),
            P(None, "row", None, "col", None, None),
            P(None, "row", None, "col"),
        ),
        out_specs=(P(None, "row", None, None), P(None, "row", None)),
        check_vma=False,
    )
```
